32 devices in a mesh: part: 1 (over z), tp: 4 (over y), dp: 8 (over x, core).
Axes of the slice: x: 4, y: 4, z: 1, core: 2. Of those that a mesh axis runs over, the one named last changes fastest.
The devices are a block of a 4x4x8 slice.
Arguments:
- x: bfloat16 [2048, 5120], P(('part', 'dp', 'tp'))
- w_gate: bfloat16 [5120, 13824], P(('part', 'dp'), 'tp')
- w_up: bfloat16 [5120, 13824], P(('part', 'dp'), 'tp')
- w_down: bfloat16 [13824, 5120], P(('part', 'tp'), 'dp')
- dy: bfloat16 [2048, 5120], P(('part', 'dp', 'tp'))
Outputs:
- output 1: bfloat16 [2048, 5120], P(('part', 'dp', 'tp'))
- output 2: bfloat16 [2048, 5120], P(('part', 'dp', 'tp'))
- output 3: float32 [5120, 13824], P(('part', 'dp'), 'tp')
- output 4: float32 [5120, 13824], P(('part', 'dp'), 'tp')
- output 5: float32 [13824, 5120], P(('part', 'tp'), 'dp')
All inputs are finite; a program needn't handle non-finite values.
Results may differ from the reference program's by a relative error of at most 0.00104.
Values are sent between devices in bfloat16 or wider.
A program may use at most 768 MiB of HBM per device.

```python
import jax
import jax.numpy as jnp
from jax import lax

D = 5120
FF = 13824
TOKENS_DEV = 64
SHARDS = 32

ROWS = SHARDS * TOKENS_DEV
BLK = min(ROWS, 512)


def setup_inputs(seed: int = 0, part: int = 0) -> dict:
    key = jax.random.fold_in(jax.random.key(seed), part)
    ks = jax.random.split(key, 5)
    x = jax.random.normal(ks[0], (ROWS, D), jnp.float32)
    w_gate = jax.random.normal(ks[1], (D, FF), jnp.float32) * D ** -0.5
    w_up = jax.random.normal(ks[2], (D, FF), jnp.float32) * D ** -0.5
    w_down = jax.random.normal(ks[3], (FF, D), jnp.float32) * FF ** -0.5
    dy = jax.random.normal(ks[4], (ROWS, D), jnp.float32)
    return {'x': x.astype(jnp.bfloat16), 'w_gate': w_gate.astype(jnp.bfloat16), 'w_up': w_up.astype(jnp.bfloat16), 'w_down': w_down.astype(jnp.bfloat16), 'dy': dy.astype(jnp.bfloat16)}


def _block(x, w_gate, w_up, w_down, dy):
    a = jnp.dot(x, w_gate, preferred_element_type=jnp.float32)
    b = jnp.dot(x, w_up, preferred_element_type=jnp.float32)
    sig = jax.nn.sigmoid(a)
    act = a * sig
    h = (act * b).astype(jnp.bfloat16)
    y = (x.astype(jnp.float32) + jnp.dot(h, w_down, preferred_element_type=jnp.float32)).astype(jnp.bfloat16)
    g = jnp.dot(dy, w_down.T, preferred_element_type=jnp.float32)
    da = (g * b * sig * (1.0 + a * (1.0 - sig))).astype(jnp.bfloat16)
    db = (g * act).astype(jnp.bfloat16)
    dx = (dy.astype(jnp.float32) + jnp.dot(da, w_gate.T, preferred_element_type=jnp.float32) + jnp.dot(db, w_up.T, preferred_element_type=jnp.float32)).astype(jnp.bfloat16)
    dw_gate = jnp.dot(x.T, da, preferred_element_type=jnp.float32)
    dw_up = jnp.dot(x.T, db, preferred_element_type=jnp.float32)
    dw_down = jnp.dot(h.T, dy, preferred_element_type=jnp.float32)
    return y, dx, dw_gate, dw_up, dw_down


def reference(x, w_gate, w_up, w_down, dy):
    xb = x.reshape(ROWS // BLK, BLK, D)
    dyb = dy.reshape(ROWS // BLK, BLK, D)

    def step(carry, blk):
        y, dx, dwg, dwu, dwd = _block(blk[0], w_gate, w_up, w_down, blk[1])
        return (carry[0] + dwg, carry[1] + dwu, carry[2] + dwd), (y, dx)

    init = (jnp.zeros((D, FF), jnp.float32), jnp.zeros((D, FF), jnp.float32), jnp.zeros((FF, D), jnp.float32))
    (dwg, dwu, dwd), (y, dx) = lax.scan(step, init, (xb, dyb))
    return (y.reshape(ROWS, D), dx.reshape(ROWS, D), dwg, dwu, dwd)
```

```python
import functools

import jax
import jax.numpy as jnp
from jax import lax
from jax.experimental import pallas as pl
from jax.experimental.pallas import tpu as pltpu
from jax.sharding import PartitionSpec as P

F32, BF16 = jnp.float32, jnp.bfloat16
LANES, ROWS = 128, 16
VMEM_LIMIT = 66_000_000


class Sizes:
    def __init__(self, axes, nx, ny, x, wg):
        self.axes = axes
        self.nc, self.ny = nx // 2, ny
        self.td, self.d = x.shape
        self.dp, self.fc = wg.shape
        self.dc = 2 * self.dp
        tiles = self.fc // LANES
        per = -(-tiles // self.nc)
        self.over = (self.nc * per - tiles) * LANES
        self.ft = per * LANES
        self.nf = self.nc * self.ft
        self.nb = self.nc * ny
        self.nj = self.td // ROWS
        self.mc = self.nb * ROWS

    def first(self, c):
        return c * self.ft - (c // (self.nc - 1)) * self.over


def _dot(a, b, ca, cb):
    return lax.dot_general(a, b, (((ca,), (cb,)), ((), ())), preferred_element_type=F32)


def _kernel(z, x_ref, wg_ref, wu_ref, wd_ref, dy_ref,
            y_ref, dx_ref, dwg_ref, dwu_ref, dwd_ref,
            xh, xp, wgu, wdb, wgup, wdp, ha, dda, rsb,
            xs, xr, ys, yr, ws, wr, ps, pr, es, er, ags, agr, rss, rsr, a2s, a2r, ls):
    nc, ny, nj = z.nc, z.ny, z.nj
    ft, dp, dc, nf, mc, td = z.ft, z.dp, z.dc, z.nf, z.mc, z.td
    half = td // 2
    me = lax.axis_index("dp")
    t = lax.axis_index("tp")
    part = lax.axis_index("part")
    c, k = me // 2, me % 2

    def dev(cc, tt, kk):
        ids = {"part": part, "tp": tt, "dp": 2 * cc + kk}
        return tuple(ids[a] for a in z.axes)

    def cx(i):
        return (c + i + nc) % nc

    def ty(i):
        return (t + i + ny) % ny

    right, left = dev(cx(1), t, k), dev(cx(-1), t, k)
    up, down = dev(c, ty(1), k), dev(c, ty(-1), k)
    mate = dev(c, t, 1 - k)

    def rc(src, dst, s, r, to):
        return pltpu.make_async_remote_copy(
            src_ref=src, dst_ref=dst, send_sem=s, recv_sem=r, device_id=to,
            device_id_type=pl.DeviceIdType.MESH)

    def lane(i, n):
        return pl.ds(pl.multiple_of(i, LANES), n)

    def row(i, n):
        return pl.ds(pl.multiple_of(i, ROWS), n)

    barrier = pltpu.get_barrier_semaphore()
    peers = [dev(cx(i), t, k) for i in range(1, nc)] + [dev(c, ty(i), k) for i in range(1, ny)] + [mate]
    for peer in peers:
        pl.semaphore_signal(barrier, inc=1, device_id=peer, device_id_type=pl.DeviceIdType.MESH)
    pl.semaphore_wait(barrier, len(peers))

    src = (x_ref, dy_ref)
    TOP, BOT = pl.ds(0, half), pl.ds(half, half)

    def blk(tt, cc):
        return tt * nc + cc

    own = blk(t, c)

    def x_send(a):
        for i, to in ((0, right), (1, left)):
            rc(src[a], xh.at[a, own], xs.at[a, i], xr.at[a, i], to).start()

    def x_pass(a):
        for i, cc, rows, to in ((0, cx(-1), TOP, right), (1, cx(1), BOT, left)):
            b = xh.at[a, blk(t, cc)]
            rc(b, b, xs.at[a, i], xr.at[a, i], to).wait_recv()
            v = xh.at[a, blk(t, cc), rows]
            rc(v, v, xs.at[a, 2 + i], xr.at[a, 2 + i], to).start()

    def x_last(a):
        for i, rows in ((2, TOP), (3, BOT)):
            v = xh.at[a, blk(t, cx(2)), rows]
            rc(v, v, xs.at[a, i], xr.at[a, i], right).wait_recv()

    OFFS = (0, -1, 1, 2)

    def y_send(a, o):
        d = xh.at[a, blk(t, cx(OFFS[o]))]
        s = src[a] if o == 0 else d
        for i, to in ((0, up), (1, down)):
            rc(s, d, ys.at[a, o, i], yr.at[a, o, i], to).start()

    def y_pass(a, o):
        for i, tt, rows, to in ((0, ty(-1), TOP, up), (1, ty(1), BOT, down)):
            b = xh.at[a, blk(tt, cx(OFFS[o]))]
            rc(b, b, ys.at[a, o, i], yr.at[a, o, i], to).wait_recv()
            v = xh.at[a, blk(tt, cx(OFFS[o])), rows]
            rc(v, v, ys.at[a, o, 2 + i], yr.at[a, o, 2 + i], to).start()

    def y_last(a, o):
        for i, rows in ((2, TOP), (3, BOT)):
            v = xh.at[a, blk(ty(2), cx(OFFS[o])), rows]
            rc(v, v, ys.at[a, o, i], yr.at[a, o, i], up).wait_recv()

    def e_copy(a):
        return rc(xh.at[a, :, :, lane((2 * c + 1 - k) * dp, dp)], xp.at[a], es.at[a], er.at[a], mate)

    def w_in(w, cc):
        if w == 2:
            return wd_ref.at[row(z.first(cc), ft), :]
        return (wg_ref, wu_ref)[w].at[:, lane(z.first(cc), ft)]

    def w_slot(w, cc, kk):
        return wdb.at[cc, kk] if w == 2 else wgu.at[w, cc, kk]

    def w_send(w):
        for i in (1, 3, 2):
            rc(w_in(w, cx(i)), w_slot(w, c, k), ws.at[w, i - 1], wr.at[w, i - 1], dev(cx(i), t, k)).start()

    def w_mate(w):
        rc(w_in(w, c), w_slot(w, c, k), ps.at[w, 0], pr.at[w, 0], mate).start()

    def w_pass(w, i):
        v = w_slot(w, cx(-i), k)
        rc(v, v, ws.at[w, i - 1], wr.at[w, i - 1], mate).wait_recv()
        rc(v, v, ps.at[w, i], pr.at[w, i], mate).start()

    def w_got(w, i):
        v = w_slot(w, cx(-i), 1 - k)
        rc(v, v, ps.at[w, i], pr.at[w, i], mate).wait_recv()

    def p_copy(w):
        s = (wg_ref, wu_ref, wd_ref)[w]
        d = wdp if w == 2 else wgup.at[w]
        return rc(s, d, es.at[2 + w], er.at[2 + w], mate)

    def local(i):
        if i < 2:
            return pltpu.make_async_copy(src[i], xh.at[i, own], ls.at[i])
        return pltpu.make_async_copy(w_in(i - 2, c), w_slot(i - 2, c, k), ls.at[i])

    def g_buf(q, j, kk, cc):
        return (dda if q else ha).at[j, kk, cc]

    def g_half(q, j, kk, cc, i):
        return dda.at[j, kk, cc, i] if q else ha.at[j, kk, cc, pl.ds(i * (mc // 2), mc // 2)]

    def g_send(q, j):
        s = nj * q + j
        v = g_buf(q, j, k, c)
        for i, to in ((0, right), (1, left), (4, mate)):
            rc(v, v, ags.at[s, i], agr.at[s, i], to).start()

    def g_pass(q, j):
        s = nj * q + j
        for i, cc, to in ((0, cx(-1), right), (1, cx(1), left)):
            v = g_buf(q, j, k, cc)
            rc(v, v, ags.at[s, i], agr.at[s, i], to).wait_recv()
            u = g_half(q, j, k, cc, i)
            rc(u, u, ags.at[s, 2 + i], agr.at[s, 2 + i], to).start()
            rc(v, v, ags.at[s, 5 + i], agr.at[s, 5 + i], mate).start()

    def g_last(q, j):
        s = nj * q + j
        for i in (0, 1):
            u = g_half(q, j, k, cx(2), i)
            rc(u, u, ags.at[s, 2 + i], agr.at[s, 2 + i], right).wait_recv()
            rc(u, u, ags.at[s, 7 + i], agr.at[s, 7 + i], mate).start()

    def g_mate(q, j):
        s = nj * q + j
        for i, cc in ((4, c), (5, cx(-1)), (6, cx(1))):
            v = g_buf(q, j, 1 - k, cc)
            rc(v, v, ags.at[s, i], agr.at[s, i], mate).wait_recv()
        for i in (0, 1):
            u = g_half(q, j, 1 - k, cx(2), i)
            rc(u, u, ags.at[s, 7 + i], agr.at[s, 7 + i], mate).wait_recv()

    def g_sent(q, j):
        s = nj * q + j
        for i in (0, 1, 4, 5, 6):
            v = g_buf(q, j, k, c)
            rc(v, v, ags.at[s, i], agr.at[s, i], mate).wait_send()
        for i in (2, 3, 7, 8):
            u = g_half(q, j, k, c, 0)
            rc(u, u, ags.at[s, i], agr.at[s, i], mate).wait_send()

    x_send(0)
    y_send(0, 0)
    x_send(1)
    for i in range(5):
        local(i).start()
    for w in range(3):
        w_mate(w)
    x_pass(0)
    y_send(0, 1)
    y_send(0, 2)
    x_pass(1)
    for w in range(3):
        p_copy(w).start()
    x_last(0)
    y_send(0, 3)
    for w in range(3):
        w_send(w)
    x_last(1)
    for o in range(4):
        y_send(1, o)
    for o in range(4):
        y_pass(0, o)
    for i in range(5):
        local(i).wait()
    for o in range(4):
        y_last(0, o)
    e_copy(0).start()

    def phase1(acc, xv, wv, wdv, hv, dv, sem):
        def x_load(a, i, slot):
            cols = lane(cx(OFFS[i]) * dc, dc)
            return [pltpu.make_async_copy(xh.at[a, :, pl.ds(j * ROWS, ROWS), cols], xv.at[slot, j], sem.at[slot, j])
                    for j in range(nj)]

        def w_load(w, i, slot):
            cc = cx(OFFS[i])
            if w == 2:
                return [pltpu.make_async_copy(wdb.at[cc, kk], wdv.at[slot, :, pl.ds(kk * dp, dp)], sem.at[slot, nj + kk])
                        for kk in range(2)]
            return [pltpu.make_async_copy(wgu.at[w, cc], wv.at[slot], sem.at[slot, nj])]

        def matmul(w, first, slot):
            @pl.loop(0, nj)
            def _(j):
                rows = row(j * mc, mc)
                lhs = xv[slot, j].reshape(mc, dc)
                if w == 2:
                    r = _dot(lhs, wdv[slot], 1, 1)
                else:
                    r = _dot(lhs, wv[slot].reshape(dc, ft), 1, 0)
                acc[w, rows, :] = r if first else acc[w, rows, :] + r

        def product(w):
            loads = {}
            for i in range(4):
                loads[i] = x_load(w // 2, i, i % 2)
            for cp in loads[0]:
                cp.start()
            for i, off in enumerate(OFFS):
                if off == 0:
                    w_got(w, 0)
                else:
                    w_got(w, -off if off < 0 else nc - off)
                wl = w_load(w, i, i % 2)
                for cp in wl:
                    cp.start()
                if i < 3:
                    for cp in loads[i + 1]:
                        cp.start()
                for cp in loads[i] + wl:
                    cp.wait()
                matmul(w, i == 0, i % 2)

        keep = lax.broadcasted_iota(jnp.int32, (ROWS, ft), 1) >= (c // (nc - 1)) * z.over

        for i in (1, 3, 2):
            w_pass(0, i)
        product(0)
        for o in range(4):
            y_pass(1, o)
        for i in (1, 3, 2):
            w_pass(1, i)
        product(1)

        @pl.loop(0, nj)
        def _(j):
            @pl.loop(0, z.nb)
            def _(b):
                rows = row(j * mc + b * ROWS, ROWS)
                aa = acc[0, rows, :]
                h = aa * jax.nn.sigmoid(aa) * acc[1, rows, :]
                hv[j, row(b * ROWS, ROWS), :] = jnp.where(keep, h, 0.0).astype(BF16)

            pltpu.make_async_copy(hv.at[j], ha.at[j, k, c], sem.at[0, 0]).start()
            pltpu.make_async_copy(hv.at[j], ha.at[j, k, c], sem.at[0, 0]).wait()

        g_send(0, 0)
        g_send(0, 1)
        for o in range(4):
            y_last(1, o)
        e_copy(1).start()
        for i in (1, 3, 2):
            w_pass(2, i)
        product(2)

        @pl.loop(0, nj)
        def _(j):
            @pl.loop(0, z.nb)
            def _(b):
                rows = row(j * mc + b * ROWS, ROWS)
                aa, gg = acc[0, rows, :], acc[2, rows, :]
                sig = jax.nn.sigmoid(aa)
                da = gg * acc[1, rows, :] * sig * (1.0 + aa * (1.0 - sig))
                db = gg * (aa * sig)
                dv[j, 0, row(b * ROWS, ROWS), :] = jnp.where(keep, da, 0.0).astype(BF16)
                dv[j, 1, row(b * ROWS, ROWS), :] = jnp.where(keep, db, 0.0).astype(BF16)

            pltpu.make_async_copy(dv.at[j], dda.at[j, k, c], sem.at[0, 0]).start()
            pltpu.make_async_copy(dv.at[j], dda.at[j, k, c], sem.at[0, 0]).wait()

    pl.run_scoped(
        phase1,
        pltpu.VMEM((3, nj * mc, ft), F32),
        pltpu.VMEM((2, nj, z.nb, ROWS, dc), BF16),
        pltpu.VMEM((2, 2, dp, ft), BF16),
        pltpu.VMEM((2, ft, dc), BF16),
        pltpu.VMEM((nj, mc, ft), BF16),
        pltpu.VMEM((nj, 2, mc, ft), BF16),
        pltpu.SemaphoreType.DMA((2, nj + 2)),
    )

    def cols_of(i):
        return pl.ds(z.first(i), ft), pl.ds(i * ft, ft)

    def tok_load(a, j, tv, sem):
        rows = pl.ds(pl.multiple_of(j * ROWS, ROWS), ROWS)
        return [pltpu.make_async_copy(xh.at[a, :, rows, lane(me * dp, dp)], tv.at[0], sem.at[0]),
                pltpu.make_async_copy(xp.at[a, :, rows, :], tv.at[1], sem.at[1])]

    rpt = nc * ROWS

    def rs_copy(q, j, i, pv, slot):
        s = nj * q + j
        return rc(pv.at[slot, row(ty(i) * rpt, rpt), :], rsb.at[s, i - 1], rss.at[s, i - 1], rsr.at[s, i - 1],
                  dev(c, ty(i), k))

    def out_copy(q, j, i, ov):
        s = nj * q + j
        dst = (dx_ref if q else y_ref).at[row(j * ROWS, ROWS), lane(c * dc, dc)]
        return rc(ov.at[cx(i)], dst, a2s.at[s, i - 1], a2r.at[s, i - 1], dev(cx(i), t, k))

    def out_local(q, j, ov, sem):
        dst = (dx_ref if q else y_ref).at[row(j * ROWS, ROWS), lane(c * dc, dc)]
        return pltpu.make_async_copy(ov.at[c], dst, sem)

    def finish(q, j, slot, pv, rv, xv, ov, sem):
        s = nj * q + j
        for i in range(1, ny):
            rs_copy(q, j, i, pv, slot).wait_recv()
        ld = [pltpu.make_async_copy(rsb.at[s], rv, sem.at[0]),
              pltpu.make_async_copy(xh.at[q, pl.ds(t * nc, nc), row(j * ROWS, ROWS), lane(c * dc, dc)],
                                    xv, sem.at[1])]
        for cp in ld:
            cp.start()

        @pl.when(j > 0)
        def _():
            for i in range(1, nc):
                out_copy(q, j - 1, i, ov).wait_send()
            out_local(q, j - 1, ov, sem.at[2]).wait()
        for cp in ld:
            cp.wait()
        for cc in range(nc):
            mine = pv[slot, row(t * rpt + cc * ROWS, ROWS), :]
            tot = mine
            for i in range(ny - 1):
                tot = tot + rv[i, pl.ds(cc * ROWS, ROWS), :]
            ov[cc] = (xv[cc].astype(F32) + tot).astype(BF16)
        for i in range(1, nc):
            out_copy(q, j, i, ov).start()
        out_local(q, j, ov, sem.at[2]).start()

    def drain(q, j, ov, sem):
        for i in range(1, nc):
            out_copy(q, j, i, ov).wait_send()
        out_local(q, j, ov, sem.at[2]).wait()

    STEP = 512

    def phase2h(acc, wv, hv, tv, pv, rv, xv, ov, sem, fsem):
        loads = []
        for i in range(nc):
            a, b = cols_of(i)
            loads.append(pltpu.make_async_copy(wd_ref.at[a, :], wv.at[b, lane(k * dp, dp)], sem.at[i]))
            loads.append(pltpu.make_async_copy(wdp.at[a, :], wv.at[b, lane((1 - k) * dp, dp)], sem.at[nc + i]))
        p_copy(2).wait_recv()
        for cp in loads:
            cp.start()
        for cp in loads:
            cp.wait()

        @pl.loop(0, nj)
        def _(j):
            slot = j % 2

            @pl.when(j < nj - 1)
            def _():
                g_pass(0, j + 1)

            @pl.when(j == nj - 1)
            def _():
                g_pass(1, 0)

            @pl.when(j < nj - 2)
            def _():
                g_send(0, j + 2)

            @pl.when(j >= nj - 2)
            def _():
                g_send(1, j - (nj - 2))
            g_last(0, j)
            mine = [pltpu.make_async_copy(ha.at[j, k, i], hv.at[pl.ds(0, mc), pl.ds(i * ft, ft)], sem.at[i])
                    for i in range(nc)]
            for cp in mine:
                cp.start()
            tl = tok_load(1, j, tv, fsem.at[1])
            for cp in tl:
                cp.start()
            for cp in mine:
                cp.wait()

            @pl.when(j >= 2)
            def _():
                for i in range(1, ny):
                    rs_copy(0, j - 2, i, pv, slot).wait_send()
            pv[slot] = _dot(hv[pl.ds(0, mc), :], wv[...], 1, 0)
            for i in range(1, ny):
                rs_copy(0, j, i, pv, slot).start()
            g_mate(0, j)
            other = [pltpu.make_async_copy(ha.at[j, 1 - k, i], hv.at[pl.ds(mc, mc), pl.ds(i * ft, ft)], sem.at[i])
                     for i in range(nc)]
            for cp in other:
                cp.start()
            for cp in tl + other:
                cp.wait()

            @pl.loop(0, nf // STEP)
            def _(n):
                r = _dot(hv[:, lane(n * STEP, STEP)], tv[...].reshape(2 * mc, dp), 0, 0)
                rows = row(n * STEP, STEP)

                @pl.when(j == 0)
                def _():
                    acc[rows, :] = r

                @pl.when(j > 0)
                def _():
                    acc[rows, :] += r

            @pl.when(j > 0)
            def _():
                finish(0, j - 1, 1 - slot, pv, rv, xv, ov, fsem.at[0])

        last = (nc - 1) * ft
        outs = [pltpu.make_async_copy(acc.at[pl.ds(0, last), :], dwd_ref.at[pl.ds(0, last), :], sem.at[0]),
                pltpu.make_async_copy(acc.at[pl.ds(last + z.over, ft - z.over), :],
                                      dwd_ref.at[pl.ds(last, ft - z.over), :], sem.at[1])]
        for cp in outs:
            cp.start()
        finish(0, nj - 1, (nj - 1) % 2, pv, rv, xv, ov, fsem.at[0])
        for j in (nj - 2, nj - 1):
            for i in range(1, ny):
                rs_copy(0, j, i, pv, j % 2).wait_send()
        drain(0, nj - 1, ov, fsem.at[0])
        for cp in outs:
            cp.wait()

    g_pass(0, 0)
    e_copy(1).wait_recv()
    e_copy(0).wait_recv()
    small = (
        pltpu.VMEM((2, z.nb, ROWS, dp), BF16),
        pltpu.VMEM((2, mc, dc), F32),
        pltpu.VMEM((ny - 1, rpt, dc), F32),
        pltpu.VMEM((nc, ROWS, dc), BF16),
        pltpu.VMEM((nc, ROWS, dc), BF16),
        pltpu.SemaphoreType.DMA((4 * nc,)),
        pltpu.SemaphoreType.DMA((2, 3)),
    )
    pl.run_scoped(
        phase2h,
        pltpu.VMEM((nf, dp), F32),
        pltpu.VMEM((nf, dc), BF16),
        pltpu.VMEM((2 * mc, nf), BF16),
        *small,
    )

    def phase2d(acc, wv, dv, tv, pv, rv, xv, ov, sem, fsem):
        loads = []
        for w, r in ((0, wg_ref), (1, wu_ref)):
            p_copy(w).wait_recv()
            for i in range(nc):
                a, b = cols_of(i)
                loads.append(pltpu.make_async_copy(r.at[:, a], wv.at[w, row(k * dp, dp), b], sem.at[(2 * w) * nc + i]))
                loads.append(pltpu.make_async_copy(wgup.at[w, :, a], wv.at[w, row((1 - k) * dp, dp), b], sem.at[(2 * w + 1) * nc + i]))
        for cp in loads:
            cp.start()
        for cp in loads:
            cp.wait()

        @pl.loop(0, nj)
        def _(j):
            slot = j % 2

            @pl.when(j < nj - 1)
            def _():
                g_pass(1, j + 1)

            @pl.when(j < nj - 2)
            def _():
                g_send(1, j + 2)
            g_last(1, j)
            mine = [pltpu.make_async_copy(dda.at[j, k, i, q], dv.at[q, pl.ds(0, mc), pl.ds(i * ft, ft)], sem.at[2 * i + q])
                    for i in range(nc) for q in range(2)]
            tl = tok_load(0, j, tv, fsem.at[1])
            for cp in tl:
                cp.start()
            for cp in mine:
                cp.start()
            for cp in mine:
                cp.wait()

            @pl.when(j >= 2)
            def _():
                for i in range(1, ny):
                    rs_copy(1, j - 2, i, pv, slot).wait_send()
            pv[slot] = _dot(dv[0, pl.ds(0, mc), :], wv[0], 1, 1)
            pv[slot] += _dot(dv[1, pl.ds(0, mc), :], wv[1], 1, 1)
            for i in range(1, ny):
                rs_copy(1, j, i, pv, slot).start()
            g_mate(1, j)
            other = [pltpu.make_async_copy(dda.at[j, 1 - k, i, q], dv.at[q, pl.ds(mc, mc), pl.ds(i * ft, ft)], sem.at[2 * i + q])
                     for i in range(nc) for q in range(2)]
            for cp in other:
                cp.start()
            for cp in tl + other:
                cp.wait()

            @pl.loop(0, nf // STEP)
            def _(n):
                cols = lane(n * STEP, STEP)
                for q in range(2):
                    r = _dot(tv[...].reshape(2 * mc, dp), dv[q, :, cols], 0, 0)

                    @pl.when(j == 0)
                    def _():
                        acc[q, :, cols] = r

                    @pl.when(j > 0)
                    def _():
                        acc[q, :, cols] += r

            @pl.when(j > 0)
            def _():
                finish(1, j - 1, 1 - slot, pv, rv, xv, ov, fsem.at[0])

        last = (nc - 1) * ft
        outs = []
        for q, r in ((0, dwg_ref), (1, dwu_ref)):
            outs += [pltpu.make_async_copy(acc.at[q, :, pl.ds(0, last)], r.at[:, pl.ds(0, last)], sem.at[2 * q]),
                     pltpu.make_async_copy(acc.at[q, :, pl.ds(last + z.over, ft - z.over)],
                                           r.at[:, pl.ds(last, ft - z.over)], sem.at[2 * q + 1])]
        for cp in outs:
            cp.start()
        finish(1, nj - 1, (nj - 1) % 2, pv, rv, xv, ov, fsem.at[0])
        for j in (nj - 2, nj - 1):
            for i in range(1, ny):
                rs_copy(1, j, i, pv, j % 2).wait_send()
        for j in range(nj):
            for q in range(2):
                for i in range(1, nc):
                    out_copy(q, j, i, ov).wait_recv()
        drain(1, nj - 1, ov, fsem.at[0])
        for cp in outs:
            cp.wait()

    pl.run_scoped(
        phase2d,
        pltpu.VMEM((2, dp, nf), F32),
        pltpu.VMEM((2, dc, nf), BF16),
        pltpu.VMEM((2, 2 * mc, nf), BF16),
        *small,
    )

    for a in range(2):
        for i in range(2):
            rc(src[a], src[a], xs.at[a, i], xr.at[a, i], right).wait_send()
            v = xh.at[a, own, TOP]
            rc(v, v, xs.at[a, 2 + i], xr.at[a, 2 + i], right).wait_send()
        for o in range(4):
            for i in range(2):
                rc(src[a], src[a], ys.at[a, o, i], yr.at[a, o, i], up).wait_send()
                v = xh.at[a, own, TOP]
                rc(v, v, ys.at[a, o, 2 + i], yr.at[a, o, 2 + i], up).wait_send()
        e_copy(a).wait_send()
    for w in range(3):
        for i in range(4):
            v = w_slot(w, c, k)
            if i:
                rc(v, v, ws.at[w, i - 1], wr.at[w, i - 1], right).wait_send()
            rc(v, v, ps.at[w, i], pr.at[w, i], mate).wait_send()
        p_copy(w).wait_send()
    for q in range(2):
        for j in range(nj):
            g_sent(q, j)


def solution(mesh):
    nx, ny = mesh.shape["dp"], mesh.shape["tp"]
    axes = mesh.axis_names
    row_spec = P(("part", "dp", "tp"), None)
    win_spec = P(("part", "dp"), "tp")
    wout_spec = P(("part", "tp"), "dp")

    def f(x, wg, wu, wd, dy):
        z = Sizes(axes, nx, ny, x, wg)
        steps = 2 * z.nj
        hbm = pl.BlockSpec(memory_space=pltpu.HBM)
        s = jax.ShapeDtypeStruct
        outs = [
            s(x.shape, BF16), s(x.shape, BF16), s(wg.shape, F32), s(wg.shape, F32), s(wd.shape, F32),
            s((2, z.nb, z.td, z.d), BF16),
            s((2, z.nb, z.td, z.dp), BF16),
            s((2, z.nc, 2, z.dp, z.ft), BF16),
            s((z.nc, 2, z.ft, z.dp), BF16),
            s((2, z.dp, z.fc), BF16),
            s((z.fc, z.dp), BF16),
            s((z.nj, 2, z.nc, z.mc, z.ft), BF16),
            s((z.nj, 2, z.nc, 2, z.mc, z.ft), BF16),
            s((steps, ny - 1, z.nc * ROWS, z.dc), F32),
        ]
        sem = pltpu.SemaphoreType.DMA
        scratch = []
        for shape in ((2, 4), (2, 4, 4), (3, 3), (3, 4), (5,), (steps, 9), (steps, ny - 1), (steps, z.nc - 1)):
            scratch += [sem(shape), sem(shape)]
        scratch.append(sem((5,)))
        r = pl.pallas_call(
            functools.partial(_kernel, z),
            out_shape=outs,
            in_specs=[hbm] * 5,
            out_specs=[hbm] * len(outs),
            scratch_shapes=scratch,
            name="mlp",
            compiler_params=pltpu.CompilerParams(
                collective_id=0, has_side_effects=True, vmem_limit_bytes=VMEM_LIMIT),
        )(x, wg, wu, wd, dy)
        return tuple(r[:5])

    return jax.shard_map(f, mesh=mesh, in_specs=(row_spec, win_spec, win_spec, wout_spec, row_spec),
                         out_specs=(row_spec, row_spec, win_spec, win_spec, wout_spec), check_vma=False)
```

```python
import functools

import jax
import jax.numpy as jnp
from jax import lax
from jax.experimental import pallas as pl
from jax.experimental.pallas import tpu as pltpu
from jax.sharding import PartitionSpec as P

F32, BF16 = jnp.float32, jnp.bfloat16
LANES, ROWS = 128, 16
VMEM_LIMIT = 48_000_000
X, DY = PAIR = range(2)
GATE, UP, DOWN = WEIGHTS = range(3)
H, D = range(2)
OWN, RIGHT, LEFT, FAR = CHIPS = range(4)
STEPS = (0, 1, -1, 2)


class Sizes:
    def __init__(self, axes, nx, ny, x, wg):
        self.axes = axes
        self.nc, self.ny = nx // 2, ny
        self.td, self.d = x.shape
        self.dp, self.fc = wg.shape
        self.dc = 2 * self.dp
        self.ft = self.fc // self.nc
        self.nb = self.nc * ny
        self.nj = self.td // ROWS
        self.mc = self.nb * ROWS
        self.hc = self.mc // 2
        starts = [c * self.ft for c in range(self.nc)]
        self.cover = -(-max(s % LANES + self.ft for s in starts) // LANES) * LANES
        self.fp = max(s // LANES * LANES + self.cover for s in starts)
        self.fw = -(-self.fc // (4 * LANES)) * 4 * LANES


def _dot(a, b, ca, cb):
    return lax.dot_general(a, b, (((ca,), (cb,)), ((), ())), preferred_element_type=F32)


def _nn(a, b):
    return _dot(a, b, 1, 0)


def _nt(a, b):
    return _dot(a, b, 1, 1)


def _start(cps):
    for cp in cps:
        cp.start(priority=1)


def _wait(cps):
    for cp in cps:
        cp.wait()


def _lane(i, n):
    return pl.ds(pl.multiple_of(i, LANES), n)


def _row(i, n):
    return pl.ds(pl.multiple_of(i, ROWS), n)


def _head(n):
    return pl.ds(0, n)


def _half(u, n):
    return pl.ds(u * n, n)


def _clear(acc):
    n = 2 * ROWS

    @pl.loop(0, acc.shape[0] // n)
    def _(i):
        acc[_row(i * n, n), :] = jnp.zeros((n, acc.shape[1]), F32)


def _turned(v):
    return v.astype(F32).T.astype(BF16)


def _kernel(z, x_ref, wg_ref, wu_ref, wd_ref, dy_ref,
            y_ref, dx_ref, dw, dwd_ref,
            xh, xp, wt, wdt, wsl, wmt, ha, dda, rsb,
            xs, xr, ys, yr, ws, wr, ps, pr, es, er, ags, agr, rss, rsr, a2s, a2r):
    nc, ny, nj = z.nc, z.ny, z.nj
    ft, fc, dp, dc, mc, hc, td = z.ft, z.fc, z.dp, z.dc, z.mc, z.hc, z.td
    half, hn, last = td // 2, nc // 2, nj - 1
    me = lax.axis_index("dp")
    t = lax.axis_index("tp")
    part = lax.axis_index("part")
    c, k = me // 2, me % 2

    def dev(cc, tt, kk):
        ids = {"part": part, "tp": tt, "dp": 2 * cc + kk}
        return tuple(ids[a] for a in z.axes)

    def cx(i):
        return (c + i + nc) % nc

    def ty(i):
        return (t + i + ny) % ny

    def chip(o):
        return cx(o + o // 2 - 2 * (o // 3))

    right, left = dev(cx(1), t, k), dev(cx(-1), t, k)
    up, down = dev(c, ty(1), k), dev(c, ty(-1), k)
    mate = dev(c, t, 1 - k)
    kinds = (k, 1 - k)

    def rc(src, dst, s, r, to):
        return pltpu.make_async_remote_copy(
            src_ref=src, dst_ref=dst, send_sem=s, recv_sem=r, device_id=to,
            device_id_type=pl.DeviceIdType.MESH)

    def arrived(v, r, i, frm):
        rc(v, v, r.at[i], r.at[i], frm).wait_recv()

    def left_for(v, s):
        rc(v, v, s, s, mate).wait_send()

    barrier = pltpu.get_barrier_semaphore()
    peers = [dev(cx(i), t, k) for i in range(1, nc)] + [dev(c, ty(i), k) for i in range(1, ny)] + [mate]
    for peer in peers:
        pl.semaphore_signal(barrier, device_id=peer, device_id_type=pl.DeviceIdType.MESH)
    pl.semaphore_wait(barrier, len(peers))

    src = (x_ref, dy_ref)
    TOP, BOT = (_half(i, half) for i in PAIR)
    fwd = 2

    def x_send(a):
        for i, to in enumerate((right, left)):
            rc(src[a], xh.at[a, c, t], xs.at[a], xr.at[a, i], to).start()

    def x_pass(a):
        for i, (cc, rows, to) in enumerate(((cx(-1), TOP, right), (cx(1), BOT, left))):
            arrived(xh.at[a, cc, t], xr, (a, i), to)
            v = xh.at[a, cc, t, rows]
            rc(v, v, xs.at[a], xr.at[a, fwd], to).start()

    def x_last(a):
        arrived(xh.at[a, cx(2), t], xr, (a, fwd), right)

    def y_send(a, o):
        d = xh.at[a, cx(STEPS[o]), t]
        s = src[a] if o == OWN else d
        for i, to in enumerate((up, down)):
            rc(s, d, ys.at[a], yr.at[a, o, i], to).start()

    def y_pass(a, o):
        for i, (tt, rows, to) in enumerate(((ty(-1), TOP, up), (ty(1), BOT, down))):
            arrived(xh.at[a, cx(STEPS[o]), tt], yr, (a, o, i), to)
            v = xh.at[a, cx(STEPS[o]), tt, rows]
            rc(v, v, ys.at[a], yr.at[a, o, fwd], to).start()

    def y_last(a, o):
        arrived(xh.at[a, cx(STEPS[o]), ty(2)], yr, (a, o, fwd), up)

    def e_copy(a):
        return rc(xh.at[a, :, :, :, _lane((2 * c + 1 - k) * dp, dp)], xp.at[a], es.at[0], er.at[a], mate)

    def w_in(w, cc):
        return (wd_ref if w == DOWN else wt.at[w]).at[_row(cc * ft, ft), :]

    def w_send(w):
        for o in (RIGHT, LEFT, FAR):
            rc(w_in(w, cx(STEPS[o])), wsl.at[w, c, k], ws.at[w], wr.at[w, o], dev(cx(STEPS[o]), t, k)).start()

    def w_mate(w):
        rc(w_in(w, c), wsl.at[w, c, k], ps.at[w], pr.at[w, OWN], mate).start()

    def w_pass(w, o):
        v = wsl.at[w, cx(STEPS[o]), k]
        arrived(v, wr, (w, {RIGHT: LEFT, LEFT: RIGHT, FAR: FAR}[o]), mate)
        rc(v, v, ps.at[w], pr.at[w, o], mate).start()

    def w_got(w, o):
        arrived(wsl.at[w, cx(STEPS[o]), 1 - k], pr, (w, o), mate)

    def p_copy(w):
        return rc((wg_ref, wu_ref, wdt)[w], wmt.at[w], es.at[1], er.at[len(PAIR) + w], mate)

    def gs(q, j, u):
        return nj * q + j if u is None else nj + last + u

    def gv(q, j, kk, cc, u=None):
        b = (dda if q else ha).at[j, kk, cc]
        return b if u is None else b.at[:, u]

    def g_some(q, j, kk, n, u):
        b = (dda if q else ha).at[j, kk, pl.ds(0, n)]
        return b if u is None else b.at[:, :, u]

    def gp(q, j, kk, cc, i, u=None):
        b = (dda if q else ha).at[j, kk, cc, i]
        return b if u is None else b.at[u]

    HOP, PASSED, MATE_NEAR, MATE_FAR = 0, 2, 3, 4

    def g_send(q, j, u=None):
        s = gs(q, j, u)
        v = gv(q, j, k, c, u)
        for i, to in ((HOP, right), (HOP + 1, left), (MATE_NEAR, mate)):
            rc(v, v, ags.at[s, 0], agr.at[s, i], to).start()

    def g_pass(q, j, u=None):
        s = gs(q, j, u)
        for i, (cc, to) in enumerate(((cx(-1), right), (cx(1), left))):
            v = gv(q, j, k, cc, u)
            arrived(v, agr, (s, HOP + i), to)
            p = gp(q, j, k, cc, i, u)
            rc(p, p, ags.at[s, 1], agr.at[s, PASSED], to).start()
            rc(v, v, ags.at[s, 1], agr.at[s, MATE_NEAR], mate).start()

    def g_last(q, j, u=None):
        s = gs(q, j, u)
        v = gv(q, j, k, cx(2), u)
        arrived(v, agr, (s, PASSED), right)
        rc(v, v, ags.at[s, 0], agr.at[s, MATE_FAR], mate).start()

    def g_mate_near(q, j, u=None):
        arrived(g_some(q, j, 1 - k, nc - 1, u), agr, (gs(q, j, u), MATE_NEAR), mate)

    def g_mate_far(q, j, u=None):
        arrived(gv(q, j, 1 - k, cx(2), u), agr, (gs(q, j, u), MATE_FAR), mate)

    def g_sent(q, j, u=None):
        for i in PAIR:
            left_for(g_some(q, j, k, nc - i, u), ags.at[gs(q, j, u), i])

    def sent_tokens():
        for a in PAIR:
            left_for(xh.at[a, pl.ds(0, nc - 1), 0], xs.at[a])
            left_for(xh.at[a, pl.ds(0, nc - 1)], ys.at[a])
        left_for(xp, es.at[0])

    def sent_weights():
        for w in WEIGHTS:
            left_for(wsl.at[w, pl.ds(0, nc - 1), 0], ws.at[w])
            left_for(wsl.at[w, :, 0], ps.at[w])
        left_for(wmt, es.at[1])

    def phase1(acc, xb, wide, tall, xv, wv, dv, bsem, tsem, sem):
        def x_in(a):
            return pltpu.make_async_copy(src[a], xb.at[a], bsem.at[0, a])

        def x_out(a):
            return pltpu.make_async_copy(xb.at[a], xh.at[a, c, t], bsem.at[1, a])

        def place(w):
            return (tall.at[GATE], wide.at[GATE]) if w == DOWN else (wide.at[w], tall.at[w])

        def s_in(w):
            return pltpu.make_async_copy((wg_ref, wu_ref, wd_ref)[w], place(w)[0], tsem.at[0, w])

        def s_out(w):
            return pltpu.make_async_copy(place(w)[1], wdt if w == DOWN else wt.at[w], tsem.at[1, w])

        def s_own(w):
            s = place(w)[0 if w == DOWN else 1].at[_row(c * ft, ft), :]
            return pltpu.make_async_copy(s, wsl.at[w, c, k], tsem.at[2, w])

        def turned(w):
            a, b = place(w)

            @pl.loop(0, fc // LANES)
            def _(n):
                rows, cols = _row(n * LANES, LANES), _lane(n * LANES, LANES)
                if w == DOWN:
                    b[:, cols] = _turned(a[rows, :])
                else:
                    b[rows, :] = _turned(a[:, cols])
            _start([s_out(w)])
            _start([s_own(w)])

        x_send(X)
        y_send(X, OWN)
        x_send(DY)
        for w in PAIR:
            _start([s_in(w)])
        for a in PAIR:
            _start([x_in(a)])
        for w in PAIR:
            s_in(w).wait()
            turned(w)
        s_out(GATE).wait()
        s_own(GATE).wait()
        _start([s_in(DOWN)])
        for a in PAIR:
            x_in(a).wait()
            _start([x_out(a)])
        s_in(DOWN).wait()
        turned(DOWN)
        x_pass(X)
        y_send(X, RIGHT)
        y_send(X, LEFT)
        for w in WEIGHTS:
            _clear(acc.at[w])
        for w in (UP, DOWN):
            s_out(w).wait()
        for w in WEIGHTS:
            w_mate(w)
        x_pass(DY)
        x_last(X)
        y_send(X, FAR)
        w_send(GATE)
        for w in WEIGHTS:
            p_copy(w).start()
        x_last(DY)
        for w in (UP, DOWN):
            s_own(w).wait()
        for a in PAIR:
            x_out(a).wait()
        for o in CHIPS:
            y_pass(X, o)
        for o in CHIPS:
            y_send(DY, o)
        y_last(X, OWN)
        y_last(X, RIGHT)
        w_send(UP)
        w_pass(GATE, LEFT)
        w_pass(GATE, RIGHT)
        y_last(X, LEFT)
        y_last(X, FAR)

        def x_load(a, o, slot):
            cols = _lane(cx(STEPS[o]) * dc, dc)
            return [pltpu.make_async_copy(xh.at[a, :, :, pl.ds(j * ROWS, ROWS), cols], xv.at[slot, j], sem.at[slot, j])
                    for j in range(nj)]

        def w_load(w, o, slot):
            return [pltpu.make_async_copy(wsl.at[w, cx(STEPS[o]), kk], wv.at[slot, :, _half(kk, dp)], sem.at[slot, nj + kk])
                    for kk in PAIR]

        def matmul(w, slot):
            @pl.loop(0, nj)
            def _(j):
                cols = _lane(j * mc, mc)
                acc[w, :, cols] += _nt(wv[slot], xv[slot, j].reshape(mc, dc))

        n_parts = len(CHIPS)
        parts = [(w, o) for w in WEIGHTS for o in CHIPS]

        def products(before, early, after):
            def tokens(n):
                w, o = parts[n]
                _start(x_load(DY if w == DOWN else X, o, n % 2))

            def read(n):
                before(*parts[n])
                _start(w_load(*parts[n], n % 2))

            tokens(0)
            read(0)

            @pl.loop(0, len(parts))
            def _(n):
                for m, (w, o) in enumerate(parts[:-1]):
                    @pl.when(n == m)
                    def _():
                        if parts[m + 1] != (DOWN, OWN):
                            tokens(m + 1)
                        if parts[m + 1] in early:
                            read(m + 1)
                _wait(w_load(GATE, OWN, n % 2) + x_load(X, OWN, n % 2))
                matmul(n // n_parts, n % 2)
                for m, (w, o) in enumerate(parts[:-1]):
                    @pl.when(n == m)
                    def _():
                        if o == FAR:
                            after(w)
                        if parts[m + 1] == (DOWN, OWN):
                            tokens(m + 1)
                        if parts[m + 1] not in early:
                            read(m + 1)

        def h_out(j):
            return pltpu.make_async_copy(dv.at[j, 0], ha.at[j, k, c], sem.at[0, j])

        def d_out(j):
            return pltpu.make_async_copy(dv.at[j], dda.at[j, k, c], sem.at[0, j])

        step = 2 * ROWS

        def hidden():
            @pl.loop(0, nj)
            def _(j):
                @pl.loop(0, ft // step)
                def _(r):
                    rows, cols = _row(r * step, step), _lane(j * mc, mc)
                    aa = acc[GATE, rows, cols]
                    h = (aa * jax.nn.sigmoid(aa) * acc[UP, rows, cols]).astype(BF16)
                    for u in PAIR:
                        dv[j, 0, u, rows, :] = h[:, u * hc:(u + 1) * hc]
                _start([h_out(j)])
            for j in range(nj):
                h_out(j).wait()

        def grads():
            @pl.loop(0, nj)
            def _(j):
                @pl.loop(0, ft // step)
                def _(r):
                    rows, cols = _row(r * step, step), _lane(j * mc, mc)
                    aa, gg = acc[GATE, rows, cols], acc[DOWN, rows, cols]
                    sig = jax.nn.sigmoid(aa)
                    da = (gg * acc[UP, rows, cols] * sig * (1.0 + aa * (1.0 - sig))).astype(BF16)
                    db = (gg * (aa * sig)).astype(BF16)
                    for q, v in enumerate((da, db)):
                        for u in PAIR:
                            dv[j, q, u, rows, :] = v[:, u * hc:(u + 1) * hc]
                _start([d_out(j)])
            for j in range(nj):
                d_out(j).wait()

        def before(w, o):
            if (w, o) == (UP, FAR):
                y_pass(DY, LEFT)
                w_pass(UP, FAR)
                y_pass(DY, FAR)
            elif o != OWN and (w == UP or o == FAR):
                w_pass(w, o)
            w_got(w, o)

        def after(w):
            if w == GATE:
                y_pass(DY, OWN)
                y_pass(DY, RIGHT)
                w_send(DOWN)
                return
            hidden()
            g_send(H, 0)
            g_send(H, 1)
            e_copy(X).start()
            for o in CHIPS:
                y_last(DY, o)
            w_pass(DOWN, LEFT)
            w_pass(DOWN, RIGHT)

        early = [(GATE, o) for o in CHIPS] + [(UP, LEFT), (DOWN, RIGHT), (DOWN, LEFT)]
        products(before, early, after)
        e_copy(DY).start()
        grads()

    sem = pltpu.SemaphoreType.DMA
    two = len(PAIR)
    pl.run_scoped(
        phase1,
        pltpu.VMEM((len(WEIGHTS), ft, nj * mc), F32),
        pltpu.VMEM((two, td, z.d), BF16),
        pltpu.VMEM((two, dp, fc), BF16),
        pltpu.VMEM((two, fc, dp), BF16),
        pltpu.VMEM((two, nj, nc, ny, ROWS, dc), BF16),
        pltpu.VMEM((two, ft, dc), BF16),
        pltpu.VMEM((nj, two, two, ft, hc), BF16),
        sem((two, two)), sem((3, 3)), sem((two, nj + two)),
    )

    def at_of(q, j):
        return nj * q + j

    def phase2(pt, pv, rv, tv, ov, sb, ssem, fsem, lsem):
        def wide_load(dst, own, other, s):
            return [pltpu.make_async_copy(v, dst.at[_row(kk * dp, dp), _head(fc)], s.at[i])
                    for i, (v, kk) in enumerate(zip((own, other), kinds))]

        def blank(dst):
            dst[:, fc:] = jnp.zeros((dc, z.fp - fc), BF16)

        def share_load(q, j, o, u=None):
            cc, slot = chip(o), o % 2
            at = _row(cc * ft - cc * ft // LANES * LANES, ft)
            cps = []
            for i in range(1 + q):
                for v in PAIR if u is None else (u,):
                    s = dda.at[j, k, cc, i, v] if q else ha.at[j, k, cc, v]
                    cols = _half(v, hc) if u is None else _lane(v * hc, hc)
                    cps.append(pltpu.make_async_copy(s, sb.at[slot, i, at, cols], ssem.at[slot, i, v]))
            return cps

        low = min(z.cover - ft, ft)

        def share_blank(q, slot):
            for i in range(1 + q):
                for a in (0, z.cover - low):
                    sb[slot, i, pl.ds(a, low), :] = jnp.zeros((low, mc), BF16)

        def share_start(q, j, o):
            share_blank(q, o % 2)
            _start(share_load(q, j, o))

        def share(q, j, o, wc, u=None):
            _wait(share_load(q, j, o, u))
            cols = _lane(chip(o) * ft // LANES * LANES, z.cover)
            p = at_of(q, j) % 2
            at = _head(mc) if u is None else _lane(u * hc, hc)
            if q:
                @pl.loop(0, two)
                def _(i):
                    pt[p, :, at] += _nn(wc[i, :, cols], sb[o % 2, i, :, at])
            else:
                pt[p, :, at] += _nn(wc[:, cols], sb[o % 2, 0, :, at])

        def shares(q, j, wc, first, end):
            @pl.loop(first, end)
            def _(o):
                @pl.when(o + 1 < end)
                def _():
                    share_start(q, j, o + 1)
                share(q, j, o, wc)

        def front(q, j, wc):
            _clear(pt.at[at_of(q, j) % 2])
            shares(q, j, wc, OWN, FAR)

        def upright(q, j, u):
            p, s = at_of(q, j) % 2, at_of(q, j) % 3
            wide = 2 * LANES

            @pl.loop(0, dc // wide)
            def _(i):
                v = pt[p, _row(i * wide, wide), _lane(u * hc, hc)].T
                pv[s, pl.ds(u * hn, hn), :, :, _lane(i * wide, wide)] = v.reshape(hn, ny, ROWS, wide)

        def rs_copy(s, u, i):
            r = i - 1
            return rc(pv.at[s % 3, pl.ds(u * hn, hn), ty(i)], rsb.at[s, u, r], rss.at[s], rsr.at[s, u], dev(c, ty(i), k))

        def rs_send(s, u):
            for i in range(1, ny):
                rs_copy(s, u, i).start()

        def rs_free(s):
            left_for(pv.at[s % 3, :, pl.ds(0, ny - 1)], rss.at[s])

        def send_up(q, j):
            @pl.loop(0, two)
            def _(u):
                upright(q, j, u)
                rs_send(at_of(q, j), u)

        def out_rows(q, j):
            return (dx_ref if q else y_ref).at[_row(j * ROWS, ROWS), _lane(c * dc, dc)]

        def out_copy(s, dst, cc):
            return rc(ov.at[s, cc], dst, a2s.at[s], a2r.at[s], dev(cc, t, k))

        def out_local(s, dst):
            return pltpu.make_async_copy(ov.at[s, c], dst, lsem.at[s])

        def out_send(q, j):
            s, dst = at_of(q, j), out_rows(q, j)
            for cc in range(nc):
                @pl.when(cc != c)
                def _():
                    out_copy(s, dst, cc).start()
            _start([out_local(s, dst)])

        def out_done(s):
            v = ov.at[s, pl.ds(0, nc - 1)]
            left_for(v, a2s.at[s])
            arrived(v, a2r, s, mate)
            out_local(s, out_rows(H, 0)).wait()

        def finish_loads(q, j, u):
            rows = pl.ds(u * hn, hn)
            return [pltpu.make_async_copy(rsb.at[at_of(q, j), u], rv.at[u], fsem.at[0, u]),
                    pltpu.make_async_copy(xh.at[q, rows, t, _row(j * ROWS, ROWS), _lane(c * dc, dc)], tv.at[rows],
                                          fsem.at[1, u])]

        def finish_start(q, j):
            @pl.loop(0, two)
            def _(u):
                arrived(rsb.at[at_of(q, j), u], rsr, (at_of(q, j), u), mate)
                _start(finish_loads(q, j, u))

        def finish(q, j):
            s = at_of(q, j)

            @pl.loop(0, two)
            def _(u):
                _wait(finish_loads(q, j, u))
                for i in range(hn):
                    cc = u * hn + i
                    tot = pv[s % 3, cc, t]
                    for m in range(ny - 1):
                        tot = tot + rv[u, m, i]
                    ov[s, cc] = (tv[cc].astype(F32) + tot).astype(BF16)

        def tok_load(a, j, buf, s):
            rows = _row(j * ROWS, ROWS)
            return [pltpu.make_async_copy(xh.at[a, :, :, rows, _lane(me * dp, dp)], buf.at[0], s.at[0]),
                    pltpu.make_async_copy(xp.at[a, :, :, rows, :], buf.at[1], s.at[1])]

        def phase2h(acc, wc, hv, kv, psem, dsem, ksem):
            p_copy(DOWN).wait_recv()
            loads = wide_load(wc, wdt, wmt.at[DOWN], psem)
            _start(loads)
            g_pass(H, 0)
            g_send(H, 2)
            blank(wc)
            _clear(acc)
            for w in PAIR:
                p_copy(w).wait_recv()
                e_copy(w).wait_recv()
            _wait(loads)

            def h_load(j, os, hs=PAIR):
                return [pltpu.make_async_copy(ha.at[j, kinds[i], cx(STEPS[o]), u],
                                              hv.at[_row(cx(STEPS[o]) * ft, ft), pl.ds(i * mc + u * hc, hc)],
                                              dsem.at[i, o, u])
                        for i in hs for o in os for u in PAIR]

            def add_outer(first, end):
                @pl.loop(first, end)
                def _(o):
                    rows = _row(chip(o) * ft, ft)
                    acc[rows, :] += _nn(hv[rows, :], kv[...].reshape(2 * mc, dp))

            near = (OWN, RIGHT, LEFT)
            share_start(H, 0, OWN)

            @pl.loop(0, nj + 1)
            def _(j):
                here, before, two_before = j < nj, j > 0, j > 1

                @pl.when(before & here)
                def _():
                    g_pass(H, j)

                @pl.when(j == nj)
                def _():
                    g_pass(D, 0)
                    g_send(D, 2)

                @pl.when(before & (j < nj - 2))
                def _():
                    g_send(H, j + 2)

                @pl.when((j >= nj - 2) & here)
                def _():
                    g_send(D, j - (nj - 2))

                @pl.when(before)
                def _():
                    g_mate_near(H, j - 1)
                    _start(tok_load(DY, j - 1, kv, ksem))
                    _start(h_load(j - 1, near))

                @pl.when((j >= 3) & here)
                def _():
                    rs_free(j - 3)

                @pl.when(here)
                def _():
                    front(H, j, wc)

                @pl.when(before)
                def _():
                    g_last(H, j - 1)
                    share_start(H, j - 1, FAR)
                    _start(h_load(j - 1, (FAR,), (0,)))

                @pl.when(j < last)
                def _():
                    share_start(H, j + 1, OWN)

                @pl.when(j == last)
                def _():
                    share_start(D, 0, OWN)

                @pl.when(before)
                def _():
                    _wait(tok_load(DY, j - 1, kv, ksem))
                    _wait(h_load(j - 1, near))
                    add_outer(OWN, FAR)
                    shares(H, j - 1, wc, FAR, FAR + 1)
                    g_mate_far(H, j - 1)
                    _start(h_load(j - 1, (FAR,), (1,)))
                    send_up(H, j - 1)

                @pl.when(two_before)
                def _():
                    finish_start(H, j - 2)

                @pl.when(before)
                def _():
                    _wait(h_load(j - 1, (FAR,)))
                    add_outer(FAR, FAR + 1)

                @pl.when(two_before)
                def _():
                    finish(H, j - 2)

            out = pltpu.make_async_copy(acc, dwd_ref, psem.at[0])
            _start([out])
            out.wait()

        pl.run_scoped(
            phase2h,
            pltpu.VMEM((fc, dp), F32),
            pltpu.VMEM((dc, z.fp), BF16),
            pltpu.VMEM((fc, 2 * mc), BF16),
            pltpu.VMEM((two, nc, ny, ROWS, dp), BF16),
            sem((two,)), sem((two, len(CHIPS), two)), sem((two,)),
        )

        def phase2d(wc, dv, kv, kt, wsem, dsem, ksem):
            loads = [cp for w in PAIR for cp in wide_load(wc.at[w], (wg_ref, wu_ref)[w], wmt.at[w], wsem.at[w])]
            _start(loads)
            for w in PAIR:
                blank(wc.at[w])
                _clear(dw.at[w])
            dv[:, fc:] = jnp.zeros((two, z.fw - fc, 2 * mc), BF16)
            _wait(loads)

            def d_load(j, os, hs=PAIR, us=PAIR):
                return [pltpu.make_async_copy(dda.at[j, kinds[i], cx(STEPS[o]), q, u],
                                              dv.at[q, _row(cx(STEPS[o]) * ft, ft), pl.ds(i * mc + u * hc, hc)],
                                              dsem.at[i, o, q, u])
                        for i in hs for o in os for q in PAIR for u in us]

            def add_outer():
                n = z.fw // 2

                @pl.loop(0, 2 * two)
                def _(i):
                    q, cols = i // 2, _lane(i % 2 * n, n)
                    dw[q, :, cols] += _nt(kt[...], dv[q, cols, :])

            def far(j, us=(None,)):
                for u in us:
                    g_mate_far(D, j, u)
                _start(d_load(j, (FAR,), (1,)))
                _wait(tok_load(X, j, kv, ksem))

                @pl.loop(0, dp // LANES)
                def _(i):
                    v = kv[:, :, :, :, _lane(i * LANES, LANES)].reshape(2 * mc, LANES)
                    kt[_row(i * LANES, LANES), :] = _turned(v)

            def back(j):
                g_last(D, j)
                share_start(D, j, FAR)
                _start(d_load(j, (FAR,), (0,)))

            near = (OWN, RIGHT, LEFT)

            def near_start(j):
                g_mate_near(D, j)
                _start(tok_load(X, j, kv, ksem))
                _start(d_load(j, near))

            @pl.loop(0, last)
            def _(j):
                before, first = j > 0, j == 1

                @pl.when(first)
                def _():
                    sent_tokens()
                    sent_weights()

                @pl.when(before)
                def _():
                    g_pass(D, j)

                @pl.when(before & (j < last - 2))
                def _():
                    g_send(D, j + 2)

                @pl.when(j == last - 1)
                def _():
                    for u in PAIR:
                        g_send(D, last, u)
                    for i in range(nj):
                        g_sent(H, i)

                @pl.when(before)
                def _():
                    near_start(j - 1)

                rs_free(nj + j - 3)
                front(D, j, wc)

                @pl.when(before)
                def _():
                    back(j - 1)

                share_start(D, j + 1, OWN)

                @pl.when(before)
                def _():
                    shares(D, j - 1, wc, FAR, FAR + 1)
                    send_up(D, j - 1)

                @pl.when(first)
                def _():
                    finish_start(H, last)

                @pl.when(j > 1)
                def _():
                    finish_start(D, j - 2)

                @pl.when(before)
                def _():
                    far(j - 1)
                    _wait(d_load(j - 1, CHIPS))
                    add_outer()

                @pl.when(first)
                def _():
                    finish(H, last)

                @pl.when(j > 1)
                def _():
                    finish(D, j - 2)

            m = last - 1
            near_start(m)
            back(m)
            rs_free(nj + last - 3)
            _clear(pt.at[at_of(D, last) % 2])
            shares(D, m, wc, FAR, FAR + 1)
            send_up(D, m)
            finish_start(D, m - 1)
            far(m)
            shares(D, last, wc, OWN, RIGHT)
            _wait(d_load(m, CHIPS))
            add_outer()
            finish(D, m - 1)
            for i in range(m):
                g_sent(D, i)
            _start(tok_load(X, last, kv, ksem))
            for u in PAIR:
                g_pass(D, last, u)
            share_start(D, last, RIGHT)
            share_start(D, last, LEFT)
            _start(d_load(last, near, (0,)))
            share(D, last, RIGHT, wc)
            share_blank(D, FAR % 2)

            @pl.loop(0, nj)
            def _(i):
                out_send(H, i)

            @pl.loop(0, m)
            def _(i):
                out_send(D, i)
            g_last(D, last, 0)
            _start(share_load(D, last, FAR, 0))
            share(D, last, LEFT, wc)

            @pl.loop(0, two)
            def _(u):
                @pl.when(u == 1)
                def _():
                    g_last(D, last, 1)
                    _start(share_load(D, last, FAR, 1))
                share(D, last, FAR, wc, u)
                upright(D, last, u)
                rs_send(at_of(D, last), u)

                @pl.when(u == 0)
                def _():
                    finish_start(D, m)
            for u in PAIR:
                g_mate_near(D, last, u)
            _start(d_load(last, near, (1,)))
            _start(d_load(last, (FAR,), (0,)))
            finish(D, m)
            out_send(D, m)
            far(last, PAIR)
            g_sent(D, m)
            for u in PAIR:
                g_sent(D, last, u)
            _wait(d_load(last, CHIPS))
            add_outer()
            finish_start(D, last)
            finish(D, last)
            out_send(D, last)
            for i in range(3):
                rs_free(nj + last - i)

            @pl.loop(0, 2 * nj)
            def _(i):
                out_done(i)

        pl.run_scoped(
            phase2d,
            pltpu.VMEM((two, dc, z.fp), BF16),
            pltpu.VMEM((two, z.fw, 2 * mc), BF16),
            pltpu.VMEM((two, nc, ny, ROWS, dp), BF16),
            pltpu.VMEM((dp, 2 * mc), BF16),
            sem((two, two)), sem((two, len(CHIPS), two, two)), sem((two,)),
        )

    pl.run_scoped(
        phase2,
        pltpu.VMEM((two, dc, mc), F32),
        pltpu.VMEM((3, nc, ny, ROWS, dc), F32),
        pltpu.VMEM((two, ny - 1, hn, ROWS, dc), F32),
        pltpu.VMEM((nc, ROWS, dc), BF16),
        pltpu.VMEM((2 * nj, nc, ROWS, dc), BF16),
        pltpu.VMEM((two, two, z.cover, mc), BF16),
        sem((two, two, two)), sem((two, two)), sem((2 * nj,)),
    )


def _move(pieces, y, dx, dw, dwd, y_out, dx_out, dwg_out, dwu_out, dwd_out, y_buf, dx_buf, dwd_buf, sems):
    small = [(a, b, o, 1) for a, b, o in ((y, y_buf, y_out), (dx, dx_buf, dx_out))]
    moves = []
    for a, b, o, n in [(dwd, dwd_buf, dwd_out, pieces)] + small:
        rows = a.shape[0] // n
        moves += [[x.at[pl.ds(i * rows, rows)] for x in (a, b, o)] for i in range(n)]

    def copy(i, leg):
        return pltpu.make_async_copy(moves[i][leg], moves[i][leg + 1], sems.at[leg, i])

    direct = [pltpu.make_async_copy(dw.at[q, :, _head(o.shape[1])], o, sems.at[0, len(moves) + q])
              for q, o in enumerate((dwg_out, dwu_out))]
    for i in range(len(moves)):
        copy(i, 0).start()
    _start(direct)
    for i in range(len(moves)):
        copy(i, 0).wait()
        copy(i, 1).start()
    for i in range(len(moves)):
        copy(i, 1).wait()
    _wait(direct)


def _results(y, dx, dw, dwd, like, pieces):
    hbm, vmem = (pl.BlockSpec(memory_space=m) for m in (pltpu.HBM, pltpu.VMEM))
    like = jax.ShapeDtypeStruct(like.shape, F32)
    shapes = [jax.ShapeDtypeStruct(a.shape, a.dtype) for a in (y, dx)]
    return pl.pallas_call(
        functools.partial(_move, pieces),
        out_shape=shapes + [like, like, jax.ShapeDtypeStruct(dwd.shape, F32)],
        in_specs=[hbm, hbm, vmem, hbm],
        out_specs=[hbm] * 5,
        scratch_shapes=[pltpu.VMEM(a.shape, a.dtype) for a in (y, dx, dwd)]
        + [pltpu.SemaphoreType.DMA((2, pieces + 4))],
        name="results",
        compiler_params=pltpu.CompilerParams(vmem_limit_bytes=VMEM_LIMIT // 2),
    )(*(pltpu.with_memory_space_constraint(v, m)
        for v, m in ((y, pltpu.HBM), (dx, pltpu.HBM), (dw, pltpu.VMEM), (dwd, pltpu.HBM))))


def solution(mesh):
    nx, ny = mesh.shape["dp"], mesh.shape["tp"]
    axes = mesh.axis_names
    row_spec = P(("part", "dp", "tp"), None)
    win_spec = P(("part", "dp"), "tp")
    wout_spec = P(("part", "tp"), "dp")

    def f(x, wg, wu, wd, dy):
        z = Sizes(axes, nx, ny, x, wg)
        steps, two, kinds = 2 * z.nj, len(PAIR), len(WEIGHTS)
        hbm = pl.BlockSpec(memory_space=pltpu.HBM)
        vmem = pl.BlockSpec(memory_space=pltpu.VMEM)
        bf16 = functools.partial(jax.ShapeDtypeStruct, dtype=BF16)
        f32 = functools.partial(jax.ShapeDtypeStruct, dtype=F32)
        outs = [
            bf16(x.shape), bf16(x.shape), pltpu.VMEM((two, z.dp, z.fw), F32), f32(wd.shape),
            bf16((two, z.nc, ny, z.td, z.d)),
            bf16((two, z.nc, ny, z.td, z.dp)),
            bf16((two, z.fc, z.dp)),
            bf16((z.dp, z.fc)),
            bf16((kinds, z.nc, two, z.ft, z.dp)),
            bf16((kinds, z.dp, z.fc)),
            bf16((z.nj, two, z.nc, two, z.ft, z.hc)),
            bf16((z.nj, two, z.nc, two, two, z.ft, z.hc)),
            f32((steps, two, ny - 1, z.nc // 2, ROWS, z.dc)),
        ]
        specs = [hbm] * len(outs)
        specs[2] = vmem
        sem = pltpu.SemaphoreType.DMA
        chips = len(CHIPS)
        shapes = ((two,), (two, 3), (two,), (two, chips, 3), (kinds,), (kinds, chips), (kinds,), (kinds, chips),
                  (two,), (two + kinds,), (steps + 1, two), (steps + 1, 5), (steps,), (steps, two), (steps,), (steps,))
        r = pl.pallas_call(
            functools.partial(_kernel, z),
            out_shape=outs,
            in_specs=[hbm] * 5,
            out_specs=specs,
            scratch_shapes=[sem(shape) for shape in shapes],
            name="mlp",
            compiler_params=pltpu.CompilerParams(
                collective_id=0, has_side_effects=True, vmem_limit_bytes=VMEM_LIMIT),
        )(x, wg, wu, wd, dy)
        return tuple(_results(*r[:4], wg, 8))

    return jax.shard_map(f, mesh=mesh, in_specs=(row_spec, win_spec, win_spec, wout_spec, row_spec),
                         out_specs=(row_spec, row_spec, win_spec, win_spec, wout_spec), check_vma=False)
```

```python
import functools

import jax
import jax.numpy as jnp
from jax import lax
from jax.experimental import pallas as pl
from jax.experimental.pallas import tpu as pltpu
from jax.sharding import PartitionSpec as P

F32, BF16 = jnp.float32, jnp.bfloat16
LANES, ROWS = 128, 16
VMEM_LIMIT = 48_000_000
X, DY = PAIR = range(2)
GATE, UP, DOWN = WEIGHTS = range(3)
H, D = range(2)
OWN, RIGHT, LEFT, FAR = CHIPS = range(4)
STEPS = (0, 1, -1, 2)


class Sizes:
    def __init__(self, axes, nx, ny, x, wg):
        self.axes = axes
        self.nc, self.ny = nx // 2, ny
        self.td, self.d = x.shape
        self.dp, self.fc = wg.shape
        self.dc = 2 * self.dp
        self.ft = self.fc // self.nc
        self.nb = self.nc * ny
        self.nj = self.td // ROWS
        self.mc = self.nb * ROWS
        self.hc = self.mc // 2
        starts = [c * self.ft for c in range(self.nc)]
        self.cover = -(-max(s % LANES + self.ft for s in starts) // LANES) * LANES
        self.fp = max(s // LANES * LANES + self.cover for s in starts)
        self.fw = -(-self.fc // (4 * LANES)) * 4 * LANES


def _dot(a, b, ca, cb):
    return lax.dot_general(a, b, (((ca,), (cb,)), ((), ())), preferred_element_type=F32)


def _nn(a, b):
    return _dot(a, b, 1, 0)


def _nt(a, b):
    return _dot(a, b, 1, 1)


def _start(cps, urgent=False):
    for cp in cps:
        cp.start(priority=0 if urgent else 1)


def _wait(cps):
    for cp in cps:
        cp.wait()


def _lane(i, n):
    return pl.ds(pl.multiple_of(i, LANES), n)


def _row(i, n):
    return pl.ds(pl.multiple_of(i, ROWS), n)


def _head(n):
    return pl.ds(0, n)


def _half(u, n):
    return pl.ds(u * n, n)


def _clear(acc):
    n = 2 * ROWS

    @pl.loop(0, acc.shape[0] // n)
    def _(i):
        acc[_row(i * n, n), :] = jnp.zeros((n, acc.shape[1]), F32)


def _turned(v):
    return v.astype(F32).T.astype(BF16)


def _kernel(z, x_ref, wg_ref, wu_ref, wd_ref, dy_ref,
            y_ref, dx_ref, dw, dwd_ref,
            xh, xp, wt, wdt, wsl, wmt, ha, dda, rsb,
            xs, xr, ys, yr, ws, wr, ps, pr, es, er, ags, agr, rss, rsr, a2s, a2r, rsv):
    nc, ny, nj = z.nc, z.ny, z.nj
    ft, fc, dp, dc, mc, hc, td = z.ft, z.fc, z.dp, z.dc, z.mc, z.hc, z.td
    half, hn, last = td // 2, nc // 2, nj - 1
    me = lax.axis_index("dp")
    t = lax.axis_index("tp")
    part = lax.axis_index("part")
    c, k = me // 2, me % 2

    def dev(cc, tt, kk):
        ids = {"part": part, "tp": tt, "dp": 2 * cc + kk}
        return tuple(ids[a] for a in z.axes)

    def cx(i):
        return (c + i + nc) % nc

    def ty(i):
        return (t + i + ny) % ny

    def chip(o):
        return cx(o + o // 2 - 2 * (o // 3))

    right, left = dev(cx(1), t, k), dev(cx(-1), t, k)
    up, down = dev(c, ty(1), k), dev(c, ty(-1), k)
    mate = dev(c, t, 1 - k)
    kinds = (k, 1 - k)

    def rc(src, dst, s, r, to):
        return pltpu.make_async_remote_copy(
            src_ref=src, dst_ref=dst, send_sem=s, recv_sem=r, device_id=to,
            device_id_type=pl.DeviceIdType.MESH)

    def arrived(v, r, i, frm):
        rc(v, v, r.at[i], r.at[i], frm).wait_recv()

    def left_for(v, s):
        rc(v, v, s, s, mate).wait_send()

    barrier = pltpu.get_barrier_semaphore()
    peers = [dev(cx(i), t, k) for i in range(1, nc)] + [dev(c, ty(i), k) for i in range(1, ny)] + [mate]
    for peer in peers:
        pl.semaphore_signal(barrier, device_id=peer, device_id_type=pl.DeviceIdType.MESH)
    pl.semaphore_wait(barrier, len(peers))

    src = (x_ref, dy_ref)
    TOP, BOT = (_half(i, half) for i in PAIR)
    fwd = 2

    def x_send(a):
        for i, to in enumerate((right, left)):
            rc(src[a], xh.at[a, c, t], xs.at[a], xr.at[a, i], to).start()

    def x_pass(a):
        for i, (cc, rows, to) in enumerate(((cx(-1), TOP, right), (cx(1), BOT, left))):
            arrived(xh.at[a, cc, t], xr, (a, i), to)
            v = xh.at[a, cc, t, rows]
            rc(v, v, xs.at[a], xr.at[a, fwd], to).start()

    def x_last(a):
        arrived(xh.at[a, cx(2), t], xr, (a, fwd), right)

    def y_send(a, o):
        d = xh.at[a, cx(STEPS[o]), t]
        s = src[a] if o == OWN else d
        for i, to in enumerate((up, down)):
            rc(s, d, ys.at[a], yr.at[a, o, i], to).start()

    def y_pass(a, o):
        for i, (tt, rows, to) in enumerate(((ty(-1), TOP, up), (ty(1), BOT, down))):
            arrived(xh.at[a, cx(STEPS[o]), tt], yr, (a, o, i), to)
            v = xh.at[a, cx(STEPS[o]), tt, rows]
            rc(v, v, ys.at[a], yr.at[a, o, fwd], to).start()

    def y_last(a, o):
        arrived(xh.at[a, cx(STEPS[o]), ty(2)], yr, (a, o, fwd), up)

    def e_copy(a):
        return rc(xh.at[a, :, :, :, _lane((2 * c + 1 - k) * dp, dp)], xp.at[a], es.at[0], er.at[a], mate)

    def w_in(w, cc):
        return (wd_ref if w == DOWN else wt.at[w]).at[_row(cc * ft, ft), :]

    def w_send(w):
        for o in (RIGHT, LEFT, FAR):
            rc(w_in(w, cx(STEPS[o])), wsl.at[w, c, k], ws.at[w], wr.at[w, o], dev(cx(STEPS[o]), t, k)).start()

    def w_mate(w):
        rc(w_in(w, c), wsl.at[w, c, k], ps.at[w], pr.at[w, OWN], mate).start()

    def w_pass(w, o):
        v = wsl.at[w, cx(STEPS[o]), k]
        arrived(v, wr, (w, {RIGHT: LEFT, LEFT: RIGHT, FAR: FAR}[o]), mate)
        rc(v, v, ps.at[w], pr.at[w, o], mate).start()

    def w_got(w, o):
        arrived(wsl.at[w, cx(STEPS[o]), 1 - k], pr, (w, o), mate)

    def p_copy(w):
        return rc((wg_ref, wu_ref, wdt)[w], wmt.at[w], es.at[1], er.at[len(PAIR) + w], mate)

    def gs(q, j, u):
        return nj * q + j if u is None else nj + last + u

    def gv(q, j, kk, cc, u=None):
        b = (dda if q else ha).at[j, kk, cc]
        return b if u is None else b.at[:, u]

    def g_some(q, j, kk, n, u):
        b = (dda if q else ha).at[j, kk, pl.ds(0, n)]
        return b if u is None else b.at[:, :, u]

    def gp(q, j, kk, cc, i, u=None):
        b = (dda if q else ha).at[j, kk, cc, i]
        return b if u is None else b.at[u]

    HOP, PASSED, MATE_NEAR, MATE_FAR = 0, 2, 3, 4

    def g_send(q, j, u=None):
        s = gs(q, j, u)
        v = gv(q, j, k, c, u)
        for i, to in ((HOP, right), (HOP + 1, left), (MATE_NEAR, mate)):
            rc(v, v, ags.at[s, 0], agr.at[s, i], to).start()

    def g_pass(q, j, u=None):
        s = gs(q, j, u)
        for i, (cc, to) in enumerate(((cx(-1), right), (cx(1), left))):
            v = gv(q, j, k, cc, u)
            arrived(v, agr, (s, HOP + i), to)
            p = gp(q, j, k, cc, i, u)
            rc(p, p, ags.at[s, 1], agr.at[s, PASSED], to).start()
            rc(v, v, ags.at[s, 1], agr.at[s, MATE_NEAR], mate).start()

    def g_last(q, j, u=None):
        s = gs(q, j, u)
        v = gv(q, j, k, cx(2), u)
        arrived(v, agr, (s, PASSED), right)
        rc(v, v, ags.at[s, 0], agr.at[s, MATE_FAR], mate).start()

    def g_mate_near(q, j, u=None):
        arrived(g_some(q, j, 1 - k, nc - 1, u), agr, (gs(q, j, u), MATE_NEAR), mate)

    def g_mate_far(q, j, u=None):
        arrived(gv(q, j, 1 - k, cx(2), u), agr, (gs(q, j, u), MATE_FAR), mate)

    def g_sent(q, j, u=None):
        for i in PAIR:
            left_for(g_some(q, j, k, nc - i, u), ags.at[gs(q, j, u), i])

    def sent_tokens():
        for a in PAIR:
            left_for(xh.at[a, pl.ds(0, nc - 1), 0], xs.at[a])
            left_for(xh.at[a, pl.ds(0, nc - 1)], ys.at[a])
        left_for(xp, es.at[0])

    def sent_weights():
        for w in WEIGHTS:
            left_for(wsl.at[w, pl.ds(0, nc - 1), 0], ws.at[w])
            left_for(wsl.at[w, :, 0], ps.at[w])
        left_for(wmt, es.at[1])

    def phase1(acc, xb, wide, tall, xv, wv, dv, bsem, tsem, sem):
        def x_in(a):
            return pltpu.make_async_copy(src[a], xb.at[a], bsem.at[0, a])

        def x_out(a):
            return pltpu.make_async_copy(xb.at[a], xh.at[a, c, t], bsem.at[1, a])

        def place(w):
            return (tall.at[GATE], wide.at[GATE]) if w == DOWN else (wide.at[w], tall.at[w])

        def s_in(w):
            return pltpu.make_async_copy((wg_ref, wu_ref, wd_ref)[w], place(w)[0], tsem.at[0, w])

        def s_out(w):
            return pltpu.make_async_copy(place(w)[1], wdt if w == DOWN else wt.at[w], tsem.at[1, w])

        def s_own(w):
            s = place(w)[0 if w == DOWN else 1].at[_row(c * ft, ft), :]
            return pltpu.make_async_copy(s, wsl.at[w, c, k], tsem.at[2, w])

        def turned(w):
            a, b = place(w)

            @pl.loop(0, fc // LANES)
            def _(n):
                rows, cols = _row(n * LANES, LANES), _lane(n * LANES, LANES)
                if w == DOWN:
                    b[:, cols] = _turned(a[rows, :])
                else:
                    b[rows, :] = _turned(a[:, cols])
            _start([s_out(w)])
            _start([s_own(w)])

        x_send(X)
        y_send(X, OWN)
        x_send(DY)
        for w in PAIR:
            _start([s_in(w)])
        for a in PAIR:
            _start([x_in(a)])
        for w in PAIR:
            s_in(w).wait()
            turned(w)
        s_out(GATE).wait()
        s_own(GATE).wait()
        _start([s_in(DOWN)])
        for a in PAIR:
            x_in(a).wait()
            _start([x_out(a)])
        s_in(DOWN).wait()
        turned(DOWN)
        x_pass(X)
        y_send(X, RIGHT)
        y_send(X, LEFT)
        for w in WEIGHTS:
            _clear(acc.at[w])
        for w in (UP, DOWN):
            s_out(w).wait()
        for w in WEIGHTS:
            w_mate(w)
        x_pass(DY)
        x_last(X)
        y_send(X, FAR)
        w_send(GATE)
        for w in WEIGHTS:
            p_copy(w).start()
        x_last(DY)
        for w in (UP, DOWN):
            s_own(w).wait()
        for a in PAIR:
            x_out(a).wait()
        for o in CHIPS:
            y_pass(X, o)
        for o in CHIPS:
            y_send(DY, o)
        y_last(X, OWN)
        y_last(X, RIGHT)
        w_send(UP)
        w_pass(GATE, LEFT)
        w_pass(GATE, RIGHT)
        y_last(X, LEFT)
        y_last(X, FAR)

        def x_load(a, o, slot):
            cols = _lane(cx(STEPS[o]) * dc, dc)
            return [pltpu.make_async_copy(xh.at[a, :, :, pl.ds(j * ROWS, ROWS), cols], xv.at[slot, j], sem.at[slot, j])
                    for j in range(nj)]

        def w_load(w, o, slot):
            return [pltpu.make_async_copy(wsl.at[w, cx(STEPS[o]), kk], wv.at[slot, :, _half(kk, dp)], sem.at[slot, nj + kk])
                    for kk in PAIR]

        def matmul(w, slot):
            @pl.loop(0, nj)
            def _(j):
                cols = _lane(j * mc, mc)
                acc[w, :, cols] += _nt(wv[slot], xv[slot, j].reshape(mc, dc))

        n_parts = len(CHIPS)
        parts = [(w, o) for w in WEIGHTS for o in CHIPS]

        def products(before, early, after):
            def tokens(n):
                w, o = parts[n]
                _start(x_load(DY if w == DOWN else X, o, n % 2))

            def read(n):
                before(*parts[n])
                _start(w_load(*parts[n], n % 2))

            tokens(0)
            read(0)

            @pl.loop(0, len(parts))
            def _(n):
                for m, (w, o) in enumerate(parts[:-1]):
                    @pl.when(n == m)
                    def _():
                        if parts[m + 1] != (DOWN, OWN):
                            tokens(m + 1)
                        if parts[m + 1] in early:
                            read(m + 1)
                _wait(w_load(GATE, OWN, n % 2) + x_load(X, OWN, n % 2))
                matmul(n // n_parts, n % 2)
                for m, (w, o) in enumerate(parts[:-1]):
                    @pl.when(n == m)
                    def _():
                        if o == FAR:
                            after(w)
                        if parts[m + 1] == (DOWN, OWN):
                            tokens(m + 1)
                        if parts[m + 1] not in early:
                            read(m + 1)

        def h_out(j):
            return pltpu.make_async_copy(dv.at[j, 0], ha.at[j, k, c], sem.at[0, j])

        def d_out(j):
            return pltpu.make_async_copy(dv.at[j], dda.at[j, k, c], sem.at[0, j])

        step = 2 * ROWS

        def hidden():
            @pl.loop(0, nj)
            def _(j):
                @pl.loop(0, ft // step)
                def _(r):
                    rows, cols = _row(r * step, step), _lane(j * mc, mc)
                    aa = acc[GATE, rows, cols]
                    h = (aa * jax.nn.sigmoid(aa) * acc[UP, rows, cols]).astype(BF16)
                    for u in PAIR:
                        dv[j, 0, u, rows, :] = h[:, u * hc:(u + 1) * hc]
                _start([h_out(j)])
            for j in range(nj):
                h_out(j).wait()

        def grads():
            @pl.loop(0, nj)
            def _(j):
                @pl.loop(0, ft // step)
                def _(r):
                    rows, cols = _row(r * step, step), _lane(j * mc, mc)
                    aa, gg = acc[GATE, rows, cols], acc[DOWN, rows, cols]
                    sig = jax.nn.sigmoid(aa)
                    da = (gg * acc[UP, rows, cols] * sig * (1.0 + aa * (1.0 - sig))).astype(BF16)
                    db = (gg * (aa * sig)).astype(BF16)
                    for q, v in enumerate((da, db)):
                        for u in PAIR:
                            dv[j, q, u, rows, :] = v[:, u * hc:(u + 1) * hc]
                _start([d_out(j)])
            for j in range(nj):
                d_out(j).wait()

        def before(w, o):
            if (w, o) == (UP, FAR):
                y_pass(DY, LEFT)
                w_pass(UP, FAR)
                y_pass(DY, FAR)
            elif (w, o) == (DOWN, RIGHT):
                w_pass(DOWN, LEFT)
                w_pass(DOWN, RIGHT)
            elif o != OWN and (w == UP or o == FAR):
                w_pass(w, o)
            w_got(w, o)

        def after(w):
            if w == GATE:
                y_pass(DY, OWN)
                y_pass(DY, RIGHT)
                w_send(DOWN)
                return
            hidden()
            for j in range(3):
                g_send(H, j)
            e_copy(X).start()
            for o in CHIPS:
                y_last(DY, o)

        early = [(GATE, o) for o in CHIPS] + [(UP, LEFT), (DOWN, LEFT)]
        products(before, early, after)
        e_copy(DY).start()
        grads()

    sem = pltpu.SemaphoreType.DMA
    two = len(PAIR)
    pl.run_scoped(
        phase1,
        pltpu.VMEM((len(WEIGHTS), ft, nj * mc), F32),
        pltpu.VMEM((two, td, z.d), BF16),
        pltpu.VMEM((two, dp, fc), BF16),
        pltpu.VMEM((two, fc, dp), BF16),
        pltpu.VMEM((two, nj, nc, ny, ROWS, dc), BF16),
        pltpu.VMEM((two, ft, dc), BF16),
        pltpu.VMEM((nj, two, two, ft, hc), BF16),
        sem((two, two)), sem((3, 3)), sem((two, nj + two)),
    )

    def at_of(q, j):
        return nj * q + j

    def phase2(pt, pv, rv, tv, ov, sb, ssem, fsem, lsem):
        def wide_load(dst, own, other, s):
            return [pltpu.make_async_copy(v, dst.at[_row(kk * dp, dp), _head(fc)], s.at[i])
                    for i, (v, kk) in enumerate(zip((own, other), kinds))]

        def blank(dst):
            dst[:, fc:] = jnp.zeros((dc, z.fp - fc), BF16)

        def share_load(q, j, o, u=None):
            cc, slot = chip(o), o % 2
            at = _row(cc * ft - cc * ft // LANES * LANES, ft)
            cps = []
            for i in range(1 + q):
                for v in PAIR if u is None else (u,):
                    s = dda.at[j, k, cc, i, v] if q else ha.at[j, k, cc, v]
                    cols = _half(v, hc) if u is None else _lane(v * hc, hc)
                    cps.append(pltpu.make_async_copy(s, sb.at[slot, i, at, cols], ssem.at[slot, i, v]))
            return cps

        low = min(z.cover - ft, ft)

        def share_blank(q, slot):
            for i in range(1 + q):
                for a in (0, z.cover - low):
                    sb[slot, i, pl.ds(a, low), :] = jnp.zeros((low, mc), BF16)

        def share_start(q, j, o):
            share_blank(q, o % 2)
            _start(share_load(q, j, o), True)

        def share(q, j, o, wc, u=None):
            _wait(share_load(q, j, o, u))
            cols = _lane(chip(o) * ft // LANES * LANES, z.cover)
            p = at_of(q, j) % 2
            at = _head(mc) if u is None else _lane(u * hc, hc)
            if q:
                @pl.loop(0, two)
                def _(i):
                    pt[p, :, at] += _nn(wc[i, :, cols], sb[o % 2, i, :, at])
            else:
                pt[p, :, at] += _nn(wc[:, cols], sb[o % 2, 0, :, at])

        def shares(q, j, wc, first, end):
            @pl.loop(first, end)
            def _(o):
                @pl.when(o + 1 < end)
                def _():
                    share_start(q, j, o + 1)
                share(q, j, o, wc)

        def front(q, j, wc):
            _clear(pt.at[at_of(q, j) % 2])
            shares(q, j, wc, OWN, FAR)

        def upright(q, j, u):
            p, s = at_of(q, j) % 2, at_of(q, j) % 3
            wide = 2 * LANES

            @pl.loop(0, dc // wide)
            def _(i):
                v = pt[p, _row(i * wide, wide), _lane(u * hc, hc)].T
                pv[s, pl.ds(u * hn, hn), :, :, _lane(i * wide, wide)] = v.reshape(hn, ny, ROWS, wide)

        def rs_send(s, u, dst=None):
            for i in range(1, ny):
                to = rsb.at[s, u, i - 1] if dst is None else dst.at[u, i - 1]
                rc(pv.at[s % 3, pl.ds(u * hn, hn), ty(i)], to, rss.at[s], rsr.at[s, u], dev(c, ty(i), k)).start()

        def rs_free(s):
            left_for(pv.at[s % 3, :, pl.ds(0, ny - 1)], rss.at[s])

        def send_up(q, j):
            @pl.loop(0, two)
            def _(u):
                upright(q, j, u)
                rs_send(at_of(q, j), u)

        def out_rows(q, j):
            return (dx_ref if q else y_ref).at[_row(j * ROWS, ROWS), _lane(c * dc, dc)]

        def out_copy(s, dst, cc):
            return rc(ov.at[s, cc], dst, a2s.at[s], a2r.at[s], dev(cc, t, k))

        def out_local(s, dst):
            return pltpu.make_async_copy(ov.at[s, c], dst, lsem.at[s])

        def out_one(s, dst, cc):
            @pl.when(cc != c)
            def _():
                out_copy(s, dst, cc).start()

            @pl.when(cc == c)
            def _():
                _start([out_local(s, dst)], True)

        def out_send(q, j):
            for cc in range(nc):
                out_one(at_of(q, j), out_rows(q, j), cc)

        def out_done(s):
            v = ov.at[s, pl.ds(0, nc - 1)]
            left_for(v, a2s.at[s])
            arrived(v, a2r, s, mate)
            out_local(s, out_rows(H, 0)).wait()

        def residual(q, j, u):
            rows = pl.ds(u * hn, hn)
            return pltpu.make_async_copy(xh.at[q, rows, t, _row(j * ROWS, ROWS), _lane(c * dc, dc)], tv.at[rows],
                                         fsem.at[1, u])

        def finish_loads(q, j, u):
            return [pltpu.make_async_copy(rsb.at[at_of(q, j), u], rv.at[u], fsem.at[0, u]), residual(q, j, u)]

        def finish_start(q, j):
            @pl.loop(0, two)
            def _(u):
                arrived(rsb.at[at_of(q, j), u], rsr, (at_of(q, j), u), mate)
                _start(finish_loads(q, j, u), True)

        def finish(q, j, late=None):
            s = at_of(q, j)

            @pl.loop(0, two)
            def _(u):
                if late is None:
                    _wait(finish_loads(q, j, u))
                else:
                    arrived(late.at[u], rsr, (s, u), mate)
                    residual(q, j, u).wait()
                for i in range(hn):
                    cc = u * hn + i
                    tot = pv[s % 3, cc, t]
                    for m in range(ny - 1):
                        tot = tot + (rv if late is None else late)[u, m, i]
                    ov[s, cc] = (tv[cc].astype(F32) + tot).astype(BF16)
                    if late is not None:
                        out_one(s, out_rows(q, j), cc)

        def tok_load(a, j, buf, s):
            rows = _row(j * ROWS, ROWS)
            return [pltpu.make_async_copy(xh.at[a, :, :, rows, _lane(me * dp, dp)], buf.at[0], s.at[0]),
                    pltpu.make_async_copy(xp.at[a, :, :, rows, :], buf.at[1], s.at[1])]

        def phase2h(acc, wc, hv, kv, psem, dsem, ksem):
            p_copy(DOWN).wait_recv()
            loads = wide_load(wc, wdt, wmt.at[DOWN], psem)
            _start(loads)
            g_pass(H, 0)
            g_send(H, 3)
            blank(wc)
            _clear(acc)
            for w in PAIR:
                p_copy(w).wait_recv()
                e_copy(w).wait_recv()
            _wait(loads)

            def h_load(j, os, hs=PAIR):
                return [pltpu.make_async_copy(ha.at[j, kinds[i], cx(STEPS[o]), u],
                                              hv.at[_row(cx(STEPS[o]) * ft, ft), pl.ds(i * mc + u * hc, hc)],
                                              dsem.at[i, o, u])
                        for i in hs for o in os for u in PAIR]

            def add_outer(first, end):
                @pl.loop(first, end)
                def _(o):
                    rows = _row(chip(o) * ft, ft)
                    acc[rows, :] += _nn(hv[rows, :], kv[...].reshape(2 * mc, dp))

            near = (OWN, RIGHT, LEFT)
            share_start(H, 0, OWN)

            @pl.loop(0, nj + 1)
            def _(j):
                here, before, two_before = j < nj, j > 0, j > 1

                @pl.when(before & here)
                def _():
                    g_pass(H, j)

                @pl.when(j == nj)
                def _():
                    g_pass(D, 0)
                    g_send(D, 2)

                @pl.when(j == 1)
                def _():
                    g_send(D, 0)

                @pl.when(j == last)
                def _():
                    g_send(D, 1)

                @pl.when(before)
                def _():
                    g_mate_near(H, j - 1)
                    _start(tok_load(DY, j - 1, kv, ksem))
                    _start(h_load(j - 1, near))

                @pl.when((j >= 3) & here)
                def _():
                    rs_free(j - 3)

                @pl.when(here)
                def _():
                    front(H, j, wc)

                @pl.when(before)
                def _():
                    g_last(H, j - 1)
                    share_start(H, j - 1, FAR)
                    _start(h_load(j - 1, (FAR,), (0,)))

                @pl.when(j < last)
                def _():
                    share_start(H, j + 1, OWN)

                @pl.when(j == last)
                def _():
                    share_start(D, 0, OWN)

                @pl.when(before)
                def _():
                    _wait(tok_load(DY, j - 1, kv, ksem))
                    _wait(h_load(j - 1, near))
                    add_outer(OWN, FAR)
                    shares(H, j - 1, wc, FAR, FAR + 1)
                    g_mate_far(H, j - 1)
                    _start(h_load(j - 1, (FAR,), (1,)))
                    send_up(H, j - 1)

                @pl.when(two_before)
                def _():
                    finish_start(H, j - 2)

                @pl.when(before)
                def _():
                    _wait(h_load(j - 1, (FAR,)))
                    add_outer(FAR, FAR + 1)

                @pl.when(two_before)
                def _():
                    finish(H, j - 2)

            out = pltpu.make_async_copy(acc, dwd_ref, psem.at[0])
            _start([out])
            out.wait()

        pl.run_scoped(
            phase2h,
            pltpu.VMEM((fc, dp), F32),
            pltpu.VMEM((dc, z.fp), BF16),
            pltpu.VMEM((fc, 2 * mc), BF16),
            pltpu.VMEM((two, nc, ny, ROWS, dp), BF16),
            sem((two,)), sem((two, len(CHIPS), two)), sem((two,)),
        )

        def phase2d(wc, dv, kv, kt, wsem, dsem, ksem):
            loads = [cp for w in PAIR for cp in wide_load(wc.at[w], (wg_ref, wu_ref)[w], wmt.at[w], wsem.at[w])]
            _start(loads)
            for w in PAIR:
                blank(wc.at[w])
                _clear(dw.at[w])
            dv[:, fc:] = jnp.zeros((two, z.fw - fc, 2 * mc), BF16)
            _wait(loads)

            def d_load(j, os, hs=PAIR, us=PAIR):
                return [pltpu.make_async_copy(dda.at[j, kinds[i], cx(STEPS[o]), q, u],
                                              dv.at[q, _row(cx(STEPS[o]) * ft, ft), pl.ds(i * mc + u * hc, hc)],
                                              dsem.at[i, o, q, u])
                        for i in hs for o in os for q in PAIR for u in us]

            def add_outer():
                n = z.fw // 2

                @pl.loop(0, 2 * two)
                def _(i):
                    q, cols = i // 2, _lane(i % 2 * n, n)
                    dw[q, :, cols] += _nt(kt[...], dv[q, cols, :])

            def far(j, us=(None,)):
                for u in us:
                    g_mate_far(D, j, u)
                _start(d_load(j, (FAR,), (1,)))
                _wait(tok_load(X, j, kv, ksem))

                @pl.loop(0, dp // LANES)
                def _(i):
                    v = kv[:, :, :, :, _lane(i * LANES, LANES)].reshape(2 * mc, LANES)
                    kt[_row(i * LANES, LANES), :] = _turned(v)

            def back(j):
                g_last(D, j)
                share_start(D, j, FAR)
                _start(d_load(j, (FAR,), (0,)))

            near = (OWN, RIGHT, LEFT)

            def near_start(j):
                g_mate_near(D, j)
                _start(tok_load(X, j, kv, ksem))
                _start(d_load(j, near))

            @pl.loop(0, last)
            def _(j):
                before, first = j > 0, j == 1

                @pl.when(first)
                def _():
                    sent_tokens()
                    sent_weights()

                @pl.when(before)
                def _():
                    g_pass(D, j)

                @pl.when(before & (j < last - 2))
                def _():
                    g_send(D, j + 2)

                @pl.when(j == last - 1)
                def _():
                    for u in PAIR:
                        g_send(D, last, u)
                    for i in range(nj):
                        g_sent(H, i)

                @pl.when(before)
                def _():
                    near_start(j - 1)

                rs_free(nj + j - 3)
                front(D, j, wc)

                @pl.when(before)
                def _():
                    back(j - 1)

                share_start(D, j + 1, OWN)

                @pl.when(before)
                def _():
                    shares(D, j - 1, wc, FAR, FAR + 1)
                    send_up(D, j - 1)

                @pl.when(first)
                def _():
                    finish_start(H, last)

                @pl.when(j > 1)
                def _():
                    finish_start(D, j - 2)

                @pl.when(before)
                def _():
                    far(j - 1)
                    _wait(d_load(j - 1, CHIPS))
                    add_outer()

                @pl.when(first)
                def _():
                    finish(H, last)

                @pl.when(j > 1)
                def _():
                    finish(D, j - 2)

            m = last - 1
            near_start(m)
            back(m)
            rs_free(nj + last - 3)
            _clear(pt.at[at_of(D, last) % 2])
            shares(D, m, wc, FAR, FAR + 1)
            send_up(D, m)
            finish_start(D, m - 1)
            far(m)
            shares(D, last, wc, OWN, RIGHT)
            _wait(d_load(m, CHIPS))
            add_outer()
            finish(D, m - 1)
            for i in range(m):
                g_sent(D, i)
            _start(tok_load(X, last, kv, ksem))
            for u in PAIR:
                g_pass(D, last, u)
            share_start(D, last, RIGHT)
            share_start(D, last, LEFT)
            _start(d_load(last, near, (0,)))
            share(D, last, RIGHT, wc)
            share_blank(D, FAR % 2)
            share(D, last, LEFT, wc)
            g_last(D, last, 0)
            _start(share_load(D, last, FAR, 0), True)

            @pl.loop(0, two)
            def _(u):
                @pl.when(u == 1)
                def _():
                    g_last(D, last, 1)
                    _start(share_load(D, last, FAR, 1), True)
                share(D, last, FAR, wc, u)
                upright(D, last, u)
                rs_send(at_of(D, last), u, rsv)

                @pl.when(u == 0)
                def _():
                    finish_start(D, m)

            @pl.loop(0, nj)
            def _(i):
                out_send(H, i)

            @pl.loop(0, m)
            def _(i):
                out_send(D, i)
            for u in PAIR:
                g_mate_near(D, last, u)
            _start(d_load(last, near, (1,)))
            _start(d_load(last, (FAR,), (0,)))
            finish(D, m)
            out_send(D, m)
            far(last, PAIR)
            g_sent(D, m)
            for u in PAIR:
                g_sent(D, last, u)
            _wait(d_load(last, CHIPS))
            _start([residual(D, last, u) for u in PAIR], True)
            add_outer()
            finish(D, last, rsv)
            for i in range(3):
                rs_free(nj + last - i)

            @pl.loop(0, 2 * nj)
            def _(i):
                out_done(i)

        pl.run_scoped(
            phase2d,
            pltpu.VMEM((two, dc, z.fp), BF16),
            pltpu.VMEM((two, z.fw, 2 * mc), BF16),
            pltpu.VMEM((two, nc, ny, ROWS, dp), BF16),
            pltpu.VMEM((dp, 2 * mc), BF16),
            sem((two, two)), sem((two, len(CHIPS), two, two)), sem((two,)),
        )

    pl.run_scoped(
        phase2,
        pltpu.VMEM((two, dc, mc), F32),
        pltpu.VMEM((3, nc, ny, ROWS, dc), F32),
        pltpu.VMEM((two, ny - 1, hn, ROWS, dc), F32),
        pltpu.VMEM((nc, ROWS, dc), BF16),
        pltpu.VMEM((2 * nj, nc, ROWS, dc), BF16),
        pltpu.VMEM((two, two, z.cover, mc), BF16),
        sem((two, two, two)), sem((two, two)), sem((2 * nj,)),
    )


def _move(pieces, y, dx, dw, dwd, y_out, dx_out, dwg_out, dwu_out, dwd_out, y_buf, dx_buf, dwd_buf, sems):
    small = [(a, b, o, 1) for a, b, o in ((y, y_buf, y_out), (dx, dx_buf, dx_out))]
    moves = []
    for a, b, o, n in [(dwd, dwd_buf, dwd_out, pieces)] + small:
        rows = a.shape[0] // n
        moves += [[x.at[pl.ds(i * rows, rows)] for x in (a, b, o)] for i in range(n)]

    def copy(i, leg):
        return pltpu.make_async_copy(moves[i][leg], moves[i][leg + 1], sems.at[leg, i])

    direct = [pltpu.make_async_copy(dw.at[q, :, _head(o.shape[1])], o, sems.at[0, len(moves) + q])
              for q, o in enumerate((dwg_out, dwu_out))]
    for i in range(len(moves)):
        copy(i, 0).start()
    _start(direct)
    for i in range(len(moves)):
        copy(i, 0).wait()
        copy(i, 1).start()
    for i in range(len(moves)):
        copy(i, 1).wait()
    _wait(direct)


def _results(y, dx, dw, dwd, like, pieces):
    hbm, vmem = (pl.BlockSpec(memory_space=m) for m in (pltpu.HBM, pltpu.VMEM))
    like = jax.ShapeDtypeStruct(like.shape, F32)
    shapes = [jax.ShapeDtypeStruct(a.shape, a.dtype) for a in (y, dx)]
    return pl.pallas_call(
        functools.partial(_move, pieces),
        out_shape=shapes + [like, like, jax.ShapeDtypeStruct(dwd.shape, F32)],
        in_specs=[hbm, hbm, vmem, hbm],
        out_specs=[hbm] * 5,
        scratch_shapes=[pltpu.VMEM(a.shape, a.dtype) for a in (y, dx, dwd)]
        + [pltpu.SemaphoreType.DMA((2, pieces + 4))],
        name="results",
        compiler_params=pltpu.CompilerParams(vmem_limit_bytes=VMEM_LIMIT // 2),
    )(*(pltpu.with_memory_space_constraint(v, m)
        for v, m in ((y, pltpu.HBM), (dx, pltpu.HBM), (dw, pltpu.VMEM), (dwd, pltpu.HBM))))


def solution(mesh):
    nx, ny = mesh.shape["dp"], mesh.shape["tp"]
    axes = mesh.axis_names
    row_spec = P(("part", "dp", "tp"), None)
    win_spec = P(("part", "dp"), "tp")
    wout_spec = P(("part", "tp"), "dp")

    def f(x, wg, wu, wd, dy):
        z = Sizes(axes, nx, ny, x, wg)
        steps, two, kinds = 2 * z.nj, len(PAIR), len(WEIGHTS)
        hbm = pl.BlockSpec(memory_space=pltpu.HBM)
        vmem = pl.BlockSpec(memory_space=pltpu.VMEM)
        bf16 = functools.partial(jax.ShapeDtypeStruct, dtype=BF16)
        f32 = functools.partial(jax.ShapeDtypeStruct, dtype=F32)
        outs = [
            bf16(x.shape), bf16(x.shape), pltpu.VMEM((two, z.dp, z.fw), F32), f32(wd.shape),
            bf16((two, z.nc, ny, z.td, z.d)),
            bf16((two, z.nc, ny, z.td, z.dp)),
            bf16((two, z.fc, z.dp)),
            bf16((z.dp, z.fc)),
            bf16((kinds, z.nc, two, z.ft, z.dp)),
            bf16((kinds, z.dp, z.fc)),
            bf16((z.nj, two, z.nc, two, z.ft, z.hc)),
            bf16((z.nj, two, z.nc, two, two, z.ft, z.hc)),
            f32((steps, two, ny - 1, z.nc // 2, ROWS, z.dc)),
        ]
        specs = [hbm] * len(outs)
        specs[2] = vmem
        sem = pltpu.SemaphoreType.DMA
        chips = len(CHIPS)
        shapes = ((two,), (two, 3), (two,), (two, chips, 3), (kinds,), (kinds, chips), (kinds,), (kinds, chips),
                  (two,), (two + kinds,), (steps + 1, two), (steps + 1, 5), (steps,), (steps, two), (steps,), (steps,))
        r = pl.pallas_call(
            functools.partial(_kernel, z),
            out_shape=outs,
            in_specs=[hbm] * 5,
            out_specs=specs,
            scratch_shapes=[sem(shape) for shape in shapes]
            + [pltpu.VMEM((two, ny - 1, z.nc // 2, ROWS, z.dc), F32)],
            name="mlp",
            compiler_params=pltpu.CompilerParams(
                collective_id=0, has_side_effects=True, vmem_limit_bytes=VMEM_LIMIT),
        )(x, wg, wu, wd, dy)
        return tuple(_results(*r[:4], wg, 8))

    return jax.shard_map(f, mesh=mesh, in_specs=(row_spec, win_spec, win_spec, wout_spec, row_spec),
                         out_specs=(row_spec, row_spec, win_spec, win_spec, wout_spec), check_vma=False)
```

```python
import functools

import jax
import jax.numpy as jnp
from jax import lax
from jax.experimental import pallas as pl
from jax.experimental.pallas import tpu as pltpu
from jax.sharding import PartitionSpec as P

F32, BF16 = jnp.float32, jnp.bfloat16
LANES, ROWS = 128, 16
VMEM_LIMIT = 40_420_000
X, DY = PAIR = range(2)
GATE, UP, DOWN = WEIGHTS = range(3)
H, D = range(2)
OWN, RIGHT, LEFT, FAR = CHIPS = range(4)
STEPS = (0, 1, -1, 2)


class Sizes:
    def __init__(self, axes, nx, ny, x, wg):
        self.axes = axes
        self.nc, self.ny = nx // 2, ny
        self.td, self.d = x.shape
        self.dp, self.fc = wg.shape
        self.dc = 2 * self.dp
        self.ft = self.fc // self.nc
        self.nb = self.nc * ny
        self.nj = self.td // ROWS
        self.mc = self.nb * ROWS
        self.hc = self.mc // 2
        starts = [c * self.ft for c in range(self.nc)]
        self.cover = -(-max(s % LANES + self.ft for s in starts) // LANES) * LANES
        self.back = max(s // LANES * LANES for s in starts) + self.cover - self.fc
        tiles = self.fc // LANES
        self.cuts = 3 if tiles % 3 == 0 else tiles

    def under(self, cc):
        return cc * self.ft // LANES * LANES - cc // (self.nc - 1) * self.back


def _dot(a, b, ca, cb):
    return lax.dot_general(a, b, (((ca,), (cb,)), ((), ())), preferred_element_type=F32)


def _nn(a, b):
    return _dot(a, b, 1, 0)


def _nt(a, b):
    return _dot(a, b, 1, 1)


def _start(cps, urgent=False):
    for cp in cps:
        cp.start(priority=0 if urgent else 1)


def _wait(cps):
    for cp in cps:
        cp.wait()


def _lane(i, n):
    return pl.ds(pl.multiple_of(i, LANES), n)


def _row(i, n):
    return pl.ds(pl.multiple_of(i, ROWS), n)


def _head(n):
    return pl.ds(0, n)


def _half(u, n):
    return pl.ds(u * n, n)


def _clear(acc):
    n = 2 * ROWS

    @pl.loop(0, acc.shape[0] // n)
    def _(i):
        acc[_row(i * n, n), :] = jnp.zeros((n, acc.shape[1]), F32)


def _turned(v):
    return v.astype(F32).T.astype(BF16)


def _kernel(z, x_ref, wg_ref, wu_ref, wd_ref, dy_ref,
            y_ref, dx_ref, dw, dwd,
            xh, xp, wt, wdt, wsl, wmt, ha, dda, rsb, ovh,
            xs, xr, ys, yr, ws, wr, ps, pr, es, er, ags, agr, rss, rsr, a2s, a2r, rsv):
    nc, ny, nj = z.nc, z.ny, z.nj
    ft, fc, dp, dc, mc, hc, td = z.ft, z.fc, z.dp, z.dc, z.mc, z.hc, z.td
    half, hn, last = td // 2, nc // 2, nj - 1
    me = lax.axis_index("dp")
    t = lax.axis_index("tp")
    part = lax.axis_index("part")
    c, k = me // 2, me % 2

    def dev(cc, tt, kk):
        ids = {"part": part, "tp": tt, "dp": 2 * cc + kk}
        return tuple(ids[a] for a in z.axes)

    def cx(i):
        return (c + i + nc) % nc

    def ty(i):
        return (t + i + ny) % ny

    def chip(o):
        return cx(o + o // 2 - 2 * (o // 3))

    right, left = dev(cx(1), t, k), dev(cx(-1), t, k)
    up, down = dev(c, ty(1), k), dev(c, ty(-1), k)
    mate = dev(c, t, 1 - k)
    kinds = (k, 1 - k)

    def rc(src, dst, s, r, to):
        return pltpu.make_async_remote_copy(
            src_ref=src, dst_ref=dst, send_sem=s, recv_sem=r, device_id=to,
            device_id_type=pl.DeviceIdType.MESH)

    def arrived(v, r, i, frm):
        rc(v, v, r.at[i], r.at[i], frm).wait_recv()

    def left_for(v, s):
        rc(v, v, s, s, mate).wait_send()

    barrier = pltpu.get_barrier_semaphore()
    peers = [dev(cx(i), t, k) for i in range(1, nc)] + [dev(c, ty(i), k) for i in range(1, ny)] + [mate]
    for peer in peers:
        pl.semaphore_signal(barrier, device_id=peer, device_id_type=pl.DeviceIdType.MESH)
    pl.semaphore_wait(barrier, len(peers))

    src = (x_ref, dy_ref)
    TOP, BOT = (_half(i, half) for i in PAIR)
    fwd = 2

    def x_send(a):
        for i, to in enumerate((right, left)):
            rc(src[a], xh.at[a, c, t], xs.at[a], xr.at[a, i], to).start()

    def x_pass(a):
        for i, (cc, rows, to) in enumerate(((cx(-1), TOP, right), (cx(1), BOT, left))):
            arrived(xh.at[a, cc, t], xr, (a, i), to)
            v = xh.at[a, cc, t, rows]
            rc(v, v, xs.at[a], xr.at[a, fwd], to).start()

    def x_last(a):
        arrived(xh.at[a, cx(2), t], xr, (a, fwd), right)

    def y_send(a, o):
        d = xh.at[a, cx(STEPS[o]), t]
        s = src[a] if o == OWN else d
        for i, to in enumerate((up, down)):
            rc(s, d, ys.at[a], yr.at[a, o, i], to).start()

    def y_pass(a, o):
        for i, (tt, rows, to) in enumerate(((ty(-1), TOP, up), (ty(1), BOT, down))):
            arrived(xh.at[a, cx(STEPS[o]), tt], yr, (a, o, i), to)
            v = xh.at[a, cx(STEPS[o]), tt, rows]
            rc(v, v, ys.at[a], yr.at[a, o, fwd], to).start()

    def y_last(a, o):
        arrived(xh.at[a, cx(STEPS[o]), ty(2)], yr, (a, o, fwd), up)

    def e_copy(a):
        return rc(xh.at[a, :, :, :, _lane((2 * c + 1 - k) * dp, dp)], xp.at[a], es.at[0], er.at[a], mate)

    def w_in(w, cc):
        return (wd_ref if w == DOWN else wt.at[w]).at[_row(cc * ft, ft), :]

    def w_send(w):
        for o in (RIGHT, LEFT, FAR):
            rc(w_in(w, cx(STEPS[o])), wsl.at[w, c, k], ws.at[w], wr.at[w, o], dev(cx(STEPS[o]), t, k)).start()

    def w_mate(w):
        rc(w_in(w, c), wsl.at[w, c, k], ps.at[w], pr.at[w, OWN], mate).start()

    def w_pass(w, o):
        v = wsl.at[w, cx(STEPS[o]), k]
        arrived(v, wr, (w, {RIGHT: LEFT, LEFT: RIGHT, FAR: FAR}[o]), mate)
        rc(v, v, ps.at[w], pr.at[w, o], mate).start()

    def w_got(w, o):
        arrived(wsl.at[w, cx(STEPS[o]), 1 - k], pr, (w, o), mate)

    def p_copy(w):
        return rc((wg_ref, wu_ref, wdt)[w], wmt.at[w], es.at[1], er.at[len(PAIR) + w], mate)

    def gs(q, j, u):
        return nj * q + j if u is None else nj + last + u

    def gv(q, j, kk, cc, u=None):
        b = (dda if q else ha).at[j, kk, cc]
        return b if u is None else b.at[:, u]

    def g_some(q, j, kk, n, u):
        b = (dda if q else ha).at[j, kk, pl.ds(0, n)]
        return b if u is None else b.at[:, :, u]

    def gp(q, j, kk, cc, i, u=None):
        b = (dda if q else ha).at[j, kk, cc, i]
        return b if u is None else b.at[u]

    HOP, PASSED, MATE_NEAR, MATE_FAR = 0, 2, 3, 4

    def g_send(q, j, u=None):
        s = gs(q, j, u)
        v = gv(q, j, k, c, u)
        for i, to in ((HOP, right), (HOP + 1, left), (MATE_NEAR, mate)):
            rc(v, v, ags.at[s, 0], agr.at[s, i], to).start()

    def g_pass(q, j, u=None):
        s = gs(q, j, u)
        for i, (cc, to) in enumerate(((cx(-1), right), (cx(1), left))):
            v = gv(q, j, k, cc, u)
            arrived(v, agr, (s, HOP + i), to)
            p = gp(q, j, k, cc, i, u)
            rc(p, p, ags.at[s, 1], agr.at[s, PASSED], to).start()
            rc(v, v, ags.at[s, 1], agr.at[s, MATE_NEAR], mate).start()

    def g_last(q, j, u=None):
        s = gs(q, j, u)
        v = gv(q, j, k, cx(2), u)
        arrived(v, agr, (s, PASSED), right)
        rc(v, v, ags.at[s, 0], agr.at[s, MATE_FAR], mate).start()

    def g_mate_near(q, j, u=None):
        arrived(g_some(q, j, 1 - k, nc - 1, u), agr, (gs(q, j, u), MATE_NEAR), mate)

    def g_mate_far(q, j, u=None):
        arrived(gv(q, j, 1 - k, cx(2), u), agr, (gs(q, j, u), MATE_FAR), mate)

    def g_sent(q, j, u=None):
        for i in PAIR:
            left_for(g_some(q, j, k, nc - i, u), ags.at[gs(q, j, u), i])

    def sent_tokens():
        for a in PAIR:
            left_for(xh.at[a, pl.ds(0, nc - 1), 0], xs.at[a])
            left_for(xh.at[a, pl.ds(0, nc - 1)], ys.at[a])
        left_for(xp, es.at[0])

    def sent_weights():
        for w in WEIGHTS:
            left_for(wsl.at[w, pl.ds(0, nc - 1), 0], ws.at[w])
            left_for(wsl.at[w, :, 0], ps.at[w])
        left_for(wmt, es.at[1])

    def phase1(acc, xb, wide, tall, xv, wv, dv, bsem, tsem, sem):
        def x_in(a):
            return pltpu.make_async_copy(src[a], xb.at[a], bsem.at[0, a])

        def x_out(a):
            return pltpu.make_async_copy(xb.at[a], xh.at[a, c, t], bsem.at[1, a])

        def place(w):
            return (tall, wide) if w == DOWN else (wide, tall)

        def s_in(w):
            return pltpu.make_async_copy((wg_ref, wu_ref, wd_ref)[w], place(w)[0], tsem.at[0, w])

        def s_out(w):
            return pltpu.make_async_copy(place(w)[1], wdt if w == DOWN else wt.at[w], tsem.at[1, w])

        def s_own(w):
            s = place(w)[0 if w == DOWN else 1].at[_row(c * ft, ft), :]
            return pltpu.make_async_copy(s, wsl.at[w, c, k], tsem.at[2, w])

        def turned(w):
            a, b = place(w)

            @pl.loop(0, fc // LANES)
            def _(n):
                rows, cols = _row(n * LANES, LANES), _lane(n * LANES, LANES)
                if w == DOWN:
                    b[:, cols] = _turned(a[rows, :])
                else:
                    b[rows, :] = _turned(a[:, cols])
            _start([s_out(w)])
            _start([s_own(w)])

        x_send(X)
        y_send(X, OWN)
        x_send(DY)
        _start([s_in(GATE)] + [x_in(a) for a in PAIR])
        s_in(GATE).wait()
        turned(GATE)
        _start([s_in(UP)])
        for a in PAIR:
            x_in(a).wait()
            _start([x_out(a)])
        _wait([s_in(UP), s_out(GATE), s_own(GATE)])
        turned(UP)
        for w in WEIGHTS:
            _clear(acc.at[w])
        _wait([s_out(UP), s_own(UP)])
        _start([s_in(DOWN)])
        x_pass(X)
        y_send(X, RIGHT)
        y_send(X, LEFT)
        for w in WEIGHTS:
            w_mate(w)
        s_in(DOWN).wait()
        turned(DOWN)
        s_out(DOWN).wait()
        x_pass(DY)
        x_last(X)
        y_send(X, FAR)
        w_send(GATE)
        for w in WEIGHTS:
            p_copy(w).start()
        x_last(DY)
        s_own(DOWN).wait()
        for a in PAIR:
            x_out(a).wait()
        for o in CHIPS:
            y_pass(X, o)
        for o in CHIPS:
            y_send(DY, o)
        y_last(X, OWN)
        y_last(X, RIGHT)
        w_send(UP)
        w_pass(GATE, LEFT)
        w_pass(GATE, RIGHT)
        y_last(X, LEFT)
        y_last(X, FAR)

        def x_load(a, o, slot):
            cols = _lane(cx(STEPS[o]) * dc, dc)
            return [pltpu.make_async_copy(xh.at[a, :, :, pl.ds(j * ROWS, ROWS), cols], xv.at[slot, j], sem.at[slot, j])
                    for j in range(nj)]

        def w_load(w, o, slot):
            return [pltpu.make_async_copy(wsl.at[w, cx(STEPS[o]), kk], wv.at[slot, :, _half(kk, dp)], sem.at[slot, nj + kk])
                    for kk in PAIR]

        def matmul(w, slot):
            @pl.loop(0, nj)
            def _(j):
                cols = _lane(j * mc, mc)
                acc[w, :, cols] += _nt(wv[slot], xv[slot, j].reshape(mc, dc))

        n_parts = len(CHIPS)
        parts = [(w, o) for w in WEIGHTS for o in CHIPS]

        def products(before, early, after):
            def tokens(n):
                w, o = parts[n]
                _start(x_load(DY if w == DOWN else X, o, n % 2))

            def read(n):
                before(*parts[n])
                _start(w_load(*parts[n], n % 2))

            tokens(0)
            read(0)

            @pl.loop(0, len(parts))
            def _(n):
                for m, (w, o) in enumerate(parts[:-1]):
                    @pl.when(n == m)
                    def _():
                        if parts[m + 1] != (DOWN, OWN):
                            tokens(m + 1)
                        if parts[m + 1] in early:
                            read(m + 1)
                _wait(w_load(GATE, OWN, n % 2) + x_load(X, OWN, n % 2))
                matmul(n // n_parts, n % 2)
                for m, (w, o) in enumerate(parts[:-1]):
                    @pl.when(n == m)
                    def _():
                        if o == FAR:
                            after(w)
                        if parts[m + 1] == (DOWN, OWN):
                            tokens(m + 1)
                        if parts[m + 1] not in early:
                            read(m + 1)

        def h_out(j):
            return pltpu.make_async_copy(dv.at[j, 0], ha.at[j, k, c], sem.at[0, j])

        def d_out(j):
            return pltpu.make_async_copy(dv.at[j], dda.at[j, k, c], sem.at[0, j])

        step = 2 * ROWS

        def hidden():
            @pl.loop(0, nj)
            def _(j):
                @pl.loop(0, ft // step)
                def _(r):
                    rows, cols = _row(r * step, step), _lane(j * mc, mc)
                    aa = acc[GATE, rows, cols]
                    h = (aa * jax.nn.sigmoid(aa) * acc[UP, rows, cols]).astype(BF16)
                    for u in PAIR:
                        dv[j, 0, u, rows, :] = h[:, u * hc:(u + 1) * hc]
                _start([h_out(j)])
            for j in range(nj):
                h_out(j).wait()

        def grads():
            @pl.loop(0, nj)
            def _(j):
                @pl.loop(0, ft // step)
                def _(r):
                    rows, cols = _row(r * step, step), _lane(j * mc, mc)
                    aa, gg = acc[GATE, rows, cols], acc[DOWN, rows, cols]
                    sig = jax.nn.sigmoid(aa)
                    da = (gg * acc[UP, rows, cols] * sig * (1.0 + aa * (1.0 - sig))).astype(BF16)
                    db = (gg * (aa * sig)).astype(BF16)
                    for q, v in enumerate((da, db)):
                        for u in PAIR:
                            dv[j, q, u, rows, :] = v[:, u * hc:(u + 1) * hc]
                _start([d_out(j)])
            for j in range(nj):
                d_out(j).wait()

        def before(w, o):
            if (w, o) == (UP, FAR):
                y_pass(DY, LEFT)
                w_pass(UP, FAR)
                y_pass(DY, FAR)
            elif (w, o) == (DOWN, RIGHT):
                w_pass(DOWN, LEFT)
                w_pass(DOWN, RIGHT)
            elif o != OWN and (w == UP or o == FAR):
                w_pass(w, o)
            w_got(w, o)

        def after(w):
            if w == GATE:
                y_pass(DY, OWN)
                y_pass(DY, RIGHT)
                w_send(DOWN)
                return
            hidden()
            for j in range(3):
                g_send(H, j)
            e_copy(X).start()
            for o in CHIPS:
                y_last(DY, o)

        early = [(GATE, o) for o in CHIPS] + [(UP, LEFT), (DOWN, LEFT)]
        products(before, early, after)
        e_copy(DY).start()
        grads()

    sem = pltpu.SemaphoreType.DMA
    two = len(PAIR)
    pl.run_scoped(
        phase1,
        pltpu.VMEM((len(WEIGHTS), ft, nj * mc), F32),
        pltpu.VMEM((two, td, z.d), BF16),
        pltpu.VMEM((dp, fc), BF16),
        pltpu.VMEM((fc, dp), BF16),
        pltpu.VMEM((two, nj, nc, ny, ROWS, dc), BF16),
        pltpu.VMEM((two, ft, dc), BF16),
        pltpu.VMEM((nj, two, two, ft, hc), BF16),
        sem((two, two)), sem((3, 3)), sem((two, nj + two)),
    )

    def at_of(q, j):
        return nj * q + j

    def phase2(pt, pv, rv, tv, ov, sb, ssem, fsem, lsem, osem):
        def wide_load(dst, own, other, s):
            return [pltpu.make_async_copy(v, dst.at[_row(kk * dp, dp), :], s.at[i])
                    for i, (v, kk) in enumerate(zip((own, other), kinds))]

        def share_load(q, j, o, u=None):
            cc, slot = chip(o), o % 2
            at = _row(cc * ft - z.under(cc), ft)
            cps = []
            for i in range(1 + q):
                for v in PAIR if u is None else (u,):
                    s = dda.at[j, k, cc, i, v] if q else ha.at[j, k, cc, v]
                    cols = _half(v, hc) if u is None else _lane(v * hc, hc)
                    cps.append(pltpu.make_async_copy(s, sb.at[slot, i, at, cols], ssem.at[slot, i, v]))
            return cps

        low = min(z.cover - ft, ft)

        def share_blank(q, slot):
            for i in range(1 + q):
                for a in (0, z.cover - low):
                    sb[slot, i, pl.ds(a, low), :] = jnp.zeros((low, mc), BF16)

        def share_start(q, j, o):
            share_blank(q, o % 2)
            _start(share_load(q, j, o), True)

        def share(q, j, o, wc, u=None):
            _wait(share_load(q, j, o, u))
            cols = _lane(z.under(chip(o)), z.cover)
            p = at_of(q, j) % 2
            at = _head(mc) if u is None else _lane(u * hc, hc)
            if q:
                @pl.loop(0, two)
                def _(i):
                    pt[p, :, at] += _nn(wc[i, :, cols], sb[o % 2, i, :, at])
            else:
                pt[p, :, at] += _nn(wc[:, cols], sb[o % 2, 0, :, at])

        def shares(q, j, wc, first, end):
            @pl.loop(first, end)
            def _(o):
                @pl.when(o + 1 < end)
                def _():
                    share_start(q, j, o + 1)
                share(q, j, o, wc)

        def front(q, j, wc):
            _clear(pt.at[at_of(q, j) % 2])
            shares(q, j, wc, OWN, FAR)

        def upright(q, j, u):
            p = s = at_of(q, j) % 2
            wide = 2 * LANES

            @pl.loop(0, dc // wide)
            def _(i):
                v = pt[p, _row(i * wide, wide), _lane(u * hc, hc)].T
                pv[s, pl.ds(u * hn, hn), :, :, _lane(i * wide, wide)] = v.reshape(hn, ny, ROWS, wide)

        def rs_send(s, u, dst=None):
            for i in range(1, ny):
                to = rsb.at[s, u, i - 1] if dst is None else dst.at[u, i - 1]
                rc(pv.at[s % 2, pl.ds(u * hn, hn), ty(i)], to, rss.at[s], rsr.at[s, u], dev(c, ty(i), k)).start()

        def rs_free(s):
            left_for(pv.at[s % 2, :, pl.ds(0, ny - 1)], rss.at[s])

        def send_up(q, j):
            if q:
                rs_free(at_of(q, j) - 2)
            else:
                @pl.when(j > 1)
                def _():
                    rs_free(j - 2)

            @pl.loop(0, two)
            def _(u):
                upright(q, j, u)
                rs_send(at_of(q, j), u)

        def out_rows(q, j):
            return (dx_ref if q else y_ref).at[_row(j * ROWS, ROWS), _lane(c * dc, dc)]

        def out_one(s, rows, dst, cc):
            @pl.when(cc != c)
            def _():
                rc(rows.at[cc], dst, a2s.at[s], a2r.at[s], dev(cc, t, k)).start()

            @pl.when(cc == c)
            def _():
                _start([pltpu.make_async_copy(rows.at[cc], dst, lsem.at[s])], True)

        def out_send(q, j):
            s = at_of(q, j)
            for cc in range(nc):
                out_one(s, ovh.at[s], out_rows(q, j), cc)

        def out_done(s):
            v = ovh.at[s, _head(nc - 1)]
            left_for(v, a2s.at[s])
            arrived(v, a2r, s, mate)
            pltpu.make_async_copy(ovh.at[s, c], out_rows(H, 0), lsem.at[s]).wait()

        def stored(s):
            return pltpu.make_async_copy(ov.at[s % 2], ovh.at[s], osem.at[s % 2])

        def residual(q, j, u):
            rows = pl.ds(u * hn, hn)
            return pltpu.make_async_copy(xh.at[q, rows, t, _row(j * ROWS, ROWS), _lane(c * dc, dc)], tv.at[rows],
                                         fsem.at[1, u])

        def finish_loads(q, j, u):
            return [pltpu.make_async_copy(rsb.at[at_of(q, j), u], rv.at[u], fsem.at[0, u]), residual(q, j, u)]

        def finish_start(q, j):
            @pl.loop(0, two)
            def _(u):
                arrived(rsb.at[at_of(q, j), u], rsr, (at_of(q, j), u), mate)
                _start(finish_loads(q, j, u), True)

        def finish(q, j, late=None):
            s = at_of(q, j)

            @pl.loop(0, two)
            def _(u):
                if late is None:
                    _wait(finish_loads(q, j, u))
                else:
                    arrived(late.at[u], rsr, (s, u), mate)
                    residual(q, j, u).wait()
                for i in range(hn):
                    cc = u * hn + i
                    tot = pv[s % 2, cc, t]
                    for m in range(ny - 1):
                        tot = tot + (rv if late is None else late)[u, m, i]
                    ov[s % 2, cc] = (tv[cc].astype(F32) + tot).astype(BF16)
                    if late is not None:
                        out_one(s, ov.at[s % 2], out_rows(q, j), cc)

            if late is None:
                _start([stored(s)])

        def tok_load(a, j, buf, s):
            rows = _row(j * ROWS, ROWS)
            return [pltpu.make_async_copy(xh.at[a, :, :, rows, _lane(me * dp, dp)], buf.at[0], s.at[0]),
                    pltpu.make_async_copy(xp.at[a, :, :, rows, :], buf.at[1], s.at[1])]

        def phase2h(wc, hv, kv, psem, dsem, ksem):
            p_copy(DOWN).wait_recv()
            loads = wide_load(wc, wdt, wmt.at[DOWN], psem)
            _start(loads)
            g_pass(H, 0)
            g_send(H, 3)
            _clear(dwd)
            for w in PAIR:
                p_copy(w).wait_recv()
                e_copy(w).wait_recv()
            _wait(loads)

            def h_load(j, os, hs=PAIR):
                return [pltpu.make_async_copy(ha.at[j, kinds[i], cx(STEPS[o]), u],
                                              hv.at[_row(cx(STEPS[o]) * ft, ft), pl.ds(i * mc + u * hc, hc)],
                                              dsem.at[i, o, u])
                        for i in hs for o in os for u in PAIR]

            def add_outer(first, end):
                @pl.loop(first, end)
                def _(o):
                    rows = _row(chip(o) * ft, ft)
                    dwd[rows, :] += _nn(hv[rows, :], kv[...].reshape(2 * mc, dp))

            near = (OWN, RIGHT, LEFT)
            share_start(H, 0, OWN)

            @pl.loop(0, nj + 1)
            def _(j):
                here, before, two_before = j < nj, j > 0, j > 1

                @pl.when(before & here)
                def _():
                    g_pass(H, j)

                @pl.when(j == nj)
                def _():
                    g_pass(D, 0)
                    g_send(D, 2)

                @pl.when(j == 1)
                def _():
                    g_send(D, 0)

                @pl.when(j == last)
                def _():
                    g_send(D, 1)

                @pl.when(before)
                def _():
                    g_mate_near(H, j - 1)
                    _start(tok_load(DY, j - 1, kv, ksem))
                    _start(h_load(j - 1, near))

                @pl.when(here)
                def _():
                    front(H, j, wc)

                @pl.when(before)
                def _():
                    g_last(H, j - 1)
                    share_start(H, j - 1, FAR)
                    _start(h_load(j - 1, (FAR,), (0,)))

                @pl.when(j < last)
                def _():
                    share_start(H, j + 1, OWN)

                @pl.when(j == last)
                def _():
                    share_start(D, 0, OWN)

                @pl.when(before)
                def _():
                    _wait(tok_load(DY, j - 1, kv, ksem))
                    _wait(h_load(j - 1, near))
                    add_outer(OWN, FAR)
                    shares(H, j - 1, wc, FAR, FAR + 1)
                    g_mate_far(H, j - 1)
                    _start(h_load(j - 1, (FAR,), (1,)))
                    send_up(H, j - 1)

                @pl.when(two_before)
                def _():
                    finish_start(H, j - 2)

                @pl.when(before)
                def _():
                    _wait(h_load(j - 1, (FAR,)))
                    add_outer(FAR, FAR + 1)

                @pl.when(j > 3)
                def _():
                    stored(j - 4).wait()

                @pl.when(two_before)
                def _():
                    finish(H, j - 2)

        pl.run_scoped(
            phase2h,
            pltpu.VMEM((dc, fc), BF16),
            pltpu.VMEM((fc, 2 * mc), BF16),
            pltpu.VMEM((two, nc, ny, ROWS, dp), BF16),
            sem((two,)), sem((two, len(CHIPS), two)), sem((two,)),
        )

        def phase2d(wc, dv, kv, kt, wsem, dsem, ksem):
            loads = [cp for w in PAIR for cp in wide_load(wc.at[w], (wg_ref, wu_ref)[w], wmt.at[w], wsem.at[w])]
            _start(loads)
            for w in PAIR:
                _clear(dw.at[w])
            _wait(loads)

            def d_load(j, os, hs=PAIR, us=PAIR):
                return [pltpu.make_async_copy(dda.at[j, kinds[i], cx(STEPS[o]), q, u],
                                              dv.at[q, _row(cx(STEPS[o]) * ft, ft), pl.ds(i * mc + u * hc, hc)],
                                              dsem.at[i, o, q, u])
                        for i in hs for o in os for q in PAIR for u in us]

            def add_outer():
                n = fc // z.cuts

                @pl.loop(0, z.cuts * two)
                def _(i):
                    q, cols = i // z.cuts, _lane(i % z.cuts * n, n)
                    dw[q, :, cols] += _nt(kt[...], dv[q, cols, :])

            def far(j, us=(None,)):
                for u in us:
                    g_mate_far(D, j, u)
                _start(d_load(j, (FAR,), (1,)))
                _wait(tok_load(X, j, kv, ksem))

                @pl.loop(0, dp // LANES)
                def _(i):
                    v = kv[:, :, :, :, _lane(i * LANES, LANES)].reshape(2 * mc, LANES)
                    kt[_row(i * LANES, LANES), :] = _turned(v)

            def back(j):
                g_last(D, j)
                share_start(D, j, FAR)
                _start(d_load(j, (FAR,), (0,)))

            near = (OWN, RIGHT, LEFT)

            def near_start(j):
                g_mate_near(D, j)
                _start(tok_load(X, j, kv, ksem))
                _start(d_load(j, near))

            @pl.loop(0, last)
            def _(j):
                before, first = j > 0, j == 1

                @pl.when(first)
                def _():
                    sent_tokens()
                    sent_weights()

                @pl.when(before)
                def _():
                    g_pass(D, j)

                @pl.when(before & (j < last - 2))
                def _():
                    g_send(D, j + 2)

                @pl.when(j == last - 1)
                def _():
                    for u in PAIR:
                        g_send(D, last, u)
                    for i in range(nj):
                        g_sent(H, i)

                @pl.when(before)
                def _():
                    near_start(j - 1)

                front(D, j, wc)

                @pl.when(before)
                def _():
                    back(j - 1)

                share_start(D, j + 1, OWN)

                @pl.when(before)
                def _():
                    shares(D, j - 1, wc, FAR, FAR + 1)
                    send_up(D, j - 1)

                @pl.when(first)
                def _():
                    finish_start(H, last)

                @pl.when(j > 1)
                def _():
                    finish_start(D, j - 2)

                @pl.when(before)
                def _():
                    far(j - 1)
                    _wait(d_load(j - 1, CHIPS))
                    add_outer()

                @pl.when(before)
                def _():
                    stored(nj + j - 4).wait()

                @pl.when(first)
                def _():
                    finish(H, last)

                @pl.when(j > 1)
                def _():
                    finish(D, j - 2)

            m = last - 1
            near_start(m)
            back(m)
            _clear(pt.at[at_of(D, last) % 2])
            shares(D, m, wc, FAR, FAR + 1)
            send_up(D, m)
            finish_start(D, m - 1)
            far(m)
            shares(D, last, wc, OWN, RIGHT)
            g_pass(D, last, 0)
            _wait(d_load(m, CHIPS))
            add_outer()
            stored(nj + m - 3).wait()
            finish(D, m - 1)
            for i in range(m):
                g_sent(D, i)
            _start(tok_load(X, last, kv, ksem))
            g_pass(D, last, 1)
            share_start(D, last, RIGHT)
            share_start(D, last, LEFT)
            _start(d_load(last, near, (0,)))
            share(D, last, RIGHT, wc)
            share_blank(D, FAR % 2)
            rs_free(at_of(D, last) - 2)
            share(D, last, LEFT, wc)
            g_last(D, last, 0)
            _start(share_load(D, last, FAR, 0), True)

            @pl.loop(0, two)
            def _(u):
                @pl.when(u == 1)
                def _():
                    g_last(D, last, 1)
                    _start(share_load(D, last, FAR, 1), True)
                    for i in PAIR:
                        stored(nj + m - 2 + i).wait()

                    @pl.loop(0, nj)
                    def _(i):
                        out_send(H, i)

                    @pl.loop(0, m)
                    def _(i):
                        out_send(D, i)
                share(D, last, FAR, wc, u)
                upright(D, last, u)
                rs_send(at_of(D, last), u, rsv)

                @pl.when(u == 0)
                def _():
                    finish_start(D, m)
            for u in PAIR:
                g_mate_near(D, last, u)
            _start(d_load(last, near, (1,)))
            _start(d_load(last, (FAR,), (0,)))
            finish(D, m)
            far(last, PAIR)
            g_sent(D, m)
            for u in PAIR:
                g_sent(D, last, u)
            _wait(d_load(last, CHIPS))
            _start([residual(D, last, u) for u in PAIR], True)
            add_outer()
            stored(nj + m).wait()
            out_send(D, m)
            finish(D, last, rsv)
            for i in PAIR:
                rs_free(nj + last - i)

            @pl.loop(0, 2 * nj)
            def _(i):
                out_done(i)

        pl.run_scoped(
            phase2d,
            pltpu.VMEM((two, dc, fc), BF16),
            pltpu.VMEM((two, fc, 2 * mc), BF16),
            pltpu.VMEM((two, nc, ny, ROWS, dp), BF16),
            pltpu.VMEM((dp, 2 * mc), BF16),
            sem((two, two)), sem((two, len(CHIPS), two, two)), sem((two,)),
        )

    pl.run_scoped(
        phase2,
        pltpu.VMEM((two, dc, mc), F32),
        pltpu.VMEM((two, nc, ny, ROWS, dc), F32),
        pltpu.VMEM((two, ny - 1, hn, ROWS, dc), F32),
        pltpu.VMEM((nc, ROWS, dc), BF16),
        pltpu.VMEM((two, nc, ROWS, dc), BF16),
        pltpu.VMEM((two, two, z.cover, mc), BF16),
        sem((two, two, two)), sem((two, two)), sem((2 * nj,)), sem((two,)),
    )


def _move(y, dx, dw, dwd, y_out, dx_out, dwg_out, dwu_out, dwd_out, bufs, sems):
    rows = [(y, bufs.at[0], y_out), (dx, bufs.at[1], dx_out)]
    grads = [(dwd, dwd_out)] + [(dw.at[q], o) for q, o in enumerate((dwg_out, dwu_out))]
    read = [pltpu.make_async_copy(a, b, sems.at[i]) for i, (a, b, _) in enumerate(rows)]
    write = [pltpu.make_async_copy(b, o, sems.at[i]) for i, (_, b, o) in enumerate(rows)]
    out = [pltpu.make_async_copy(a, o, sems.at[len(rows) + i]) for i, (a, o) in enumerate(grads)]
    _start(read, True)
    _start(out)
    for a, b in zip(read, write):
        a.wait()
        _start([b], True)
    _wait(write + out)


def _results(y, dx, dw, dwd, like):
    hbm, vmem = pltpu.HBM, pltpu.VMEM
    spaces = (hbm, hbm, vmem, vmem)
    like = jax.ShapeDtypeStruct(like.shape, F32)
    rows = [jax.ShapeDtypeStruct(a.shape, a.dtype) for a in (y, dx)]
    outs = rows + [like, like, jax.ShapeDtypeStruct(dwd.shape, F32)]
    return pl.pallas_call(
        _move,
        out_shape=outs,
        in_specs=[pl.BlockSpec(memory_space=m) for m in spaces],
        out_specs=[pl.BlockSpec(memory_space=hbm)] * len(outs),
        scratch_shapes=[vmem((len(rows), *y.shape), y.dtype), pltpu.SemaphoreType.DMA((len(outs),))],
        name="results",
        compiler_params=pltpu.CompilerParams(vmem_limit_bytes=VMEM_LIMIT // 10),
    )(*(pltpu.with_memory_space_constraint(v, m) for v, m in zip((y, dx, dw, dwd), spaces)))


def solution(mesh):
    nx, ny = mesh.shape["dp"], mesh.shape["tp"]
    axes = mesh.axis_names
    row_spec = P(("part", "dp", "tp"), None)
    win_spec = P(("part", "dp"), "tp")
    wout_spec = P(("part", "tp"), "dp")

    def f(x, wg, wu, wd, dy):
        z = Sizes(axes, nx, ny, x, wg)
        steps, two, kinds = 2 * z.nj, len(PAIR), len(WEIGHTS)
        hbm = pl.BlockSpec(memory_space=pltpu.HBM)
        vmem = pl.BlockSpec(memory_space=pltpu.VMEM)
        bf16 = functools.partial(jax.ShapeDtypeStruct, dtype=BF16)
        f32 = functools.partial(jax.ShapeDtypeStruct, dtype=F32)
        outs = [
            bf16(x.shape), bf16(x.shape), pltpu.VMEM((two, z.dp, z.fc), F32), pltpu.VMEM(wd.shape, F32),
            bf16((two, z.nc, ny, z.td, z.d)),
            bf16((two, z.nc, ny, z.td, z.dp)),
            bf16((two, z.fc, z.dp)),
            bf16((z.dp, z.fc)),
            bf16((kinds, z.nc, two, z.ft, z.dp)),
            bf16((kinds, z.dp, z.fc)),
            bf16((z.nj, two, z.nc, two, z.ft, z.hc)),
            bf16((z.nj, two, z.nc, two, two, z.ft, z.hc)),
            f32((steps, two, ny - 1, z.nc // 2, ROWS, z.dc)),
            bf16((steps, z.nc, ROWS, z.dc)),
        ]
        specs = [hbm] * len(outs)
        specs[2:4] = [vmem] * 2
        sem = pltpu.SemaphoreType.DMA
        chips = len(CHIPS)
        shapes = ((two,), (two, 3), (two,), (two, chips, 3), (kinds,), (kinds, chips), (kinds,), (kinds, chips),
                  (two,), (two + kinds,), (steps + 1, two), (steps + 1, 5), (steps,), (steps, two), (steps,), (steps,))
        r = pl.pallas_call(
            functools.partial(_kernel, z),
            out_shape=outs,
            in_specs=[hbm] * 5,
            out_specs=specs,
            scratch_shapes=[sem(shape) for shape in shapes]
            + [pltpu.VMEM((two, ny - 1, z.nc // 2, ROWS, z.dc), F32)],
            name="mlp",
            compiler_params=pltpu.CompilerParams(
                collective_id=0, has_side_effects=True, vmem_limit_bytes=VMEM_LIMIT),
        )(x, wg, wu, wd, dy)
        return tuple(_results(*r[:4], wg))

    return jax.shard_map(f, mesh=mesh, in_specs=(row_spec, win_spec, win_spec, wout_spec, row_spec),
                         out_specs=(row_spec, row_spec, win_spec, win_spec, wout_spec), check_vma=False)
```

```python
import functools

import jax
import jax.numpy as jnp
from jax import lax
from jax.experimental import pallas as pl
from jax.experimental.pallas import tpu as pltpu
from jax.sharding import PartitionSpec as P

F32, BF16 = jnp.float32, jnp.bfloat16
LANES, ROWS = 128, 16
VMEM_LIMIT = 40_420_000
X, DY = PAIR = range(2)
GATE, UP, DOWN = WEIGHTS = range(3)
H, D = range(2)
OWN, RIGHT, LEFT, FAR = CHIPS = range(4)
STEPS = (0, 1, -1, 2)


class Sizes:
    def __init__(self, axes, nx, ny, x, wg):
        self.axes = axes
        self.nc, self.ny = nx // 2, ny
        self.td, self.d = x.shape
        self.dp, self.fc = wg.shape
        self.dc = 2 * self.dp
        self.ft = self.fc // self.nc
        self.nb = self.nc * ny
        self.nj = self.td // ROWS
        self.mc = self.nb * ROWS
        self.hc = self.mc // 2
        starts = [c * self.ft for c in range(self.nc)]
        self.cover = -(-max(s % LANES + self.ft for s in starts) // LANES) * LANES
        self.back = max(s // LANES * LANES for s in starts) + self.cover - self.fc
        tiles = self.fc // LANES
        self.cuts = 3 if tiles % 3 == 0 else tiles

    def under(self, cc):
        return cc * self.ft // LANES * LANES - cc // (self.nc - 1) * self.back


def _dot(a, b, ca, cb):
    return lax.dot_general(a, b, (((ca,), (cb,)), ((), ())), preferred_element_type=F32)


def _nn(a, b):
    return _dot(a, b, 1, 0)


def _nt(a, b):
    return _dot(a, b, 1, 1)


def _start(cps, urgent=False):
    for cp in cps:
        cp.start(priority=0 if urgent else 1)


def _wait(cps):
    for cp in cps:
        cp.wait()


def _lane(i, n):
    return pl.ds(pl.multiple_of(i, LANES), n)


def _row(i, n):
    return pl.ds(pl.multiple_of(i, ROWS), n)


def _head(n):
    return pl.ds(0, n)


def _half(u, n):
    return pl.ds(u * n, n)


def _clear(acc):
    n = 2 * ROWS

    @pl.loop(0, acc.shape[0] // n)
    def _(i):
        acc[_row(i * n, n), :] = jnp.zeros((n, acc.shape[1]), F32)


def _turned(v):
    return v.astype(F32).T.astype(BF16)


def _kernel(z, x_ref, wg_ref, wu_ref, wd_ref, dy_ref,
            y_ref, dx_ref, dw, dwd,
            xh, xp, wt, wdt, wsl, wmt, ha, dda, rsb, ovh,
            xs, xr, ys, yr, ws, wr, ps, pr, es, er, ags, agr, rss, rsr, a2s, a2r, rsv):
    nc, ny, nj = z.nc, z.ny, z.nj
    ft, fc, dp, dc, mc, hc, td = z.ft, z.fc, z.dp, z.dc, z.mc, z.hc, z.td
    half, hn, last = td // 2, nc // 2, nj - 1
    me = lax.axis_index("dp")
    t = lax.axis_index("tp")
    part = lax.axis_index("part")
    c, k = me // 2, me % 2

    def dev(cc, tt, kk):
        ids = {"part": part, "tp": tt, "dp": 2 * cc + kk}
        return tuple(ids[a] for a in z.axes)

    def cx(i):
        return (c + i + nc) % nc

    def ty(i):
        return (t + i + ny) % ny

    def chip(o):
        return cx(o + o // 2 - 2 * (o // 3))

    right, left = dev(cx(1), t, k), dev(cx(-1), t, k)
    up, down = dev(c, ty(1), k), dev(c, ty(-1), k)
    mate = dev(c, t, 1 - k)
    kinds = (k, 1 - k)

    def rc(src, dst, s, r, to):
        return pltpu.make_async_remote_copy(
            src_ref=src, dst_ref=dst, send_sem=s, recv_sem=r, device_id=to,
            device_id_type=pl.DeviceIdType.MESH)

    def arrived(v, r, i, frm):
        rc(v, v, r.at[i], r.at[i], frm).wait_recv()

    def left_for(v, s):
        rc(v, v, s, s, mate).wait_send()

    barrier = pltpu.get_barrier_semaphore()
    peers = [dev(cx(i), t, k) for i in range(1, nc)] + [dev(c, ty(i), k) for i in range(1, ny)] + [mate]
    for peer in peers:
        pl.semaphore_signal(barrier, device_id=peer, device_id_type=pl.DeviceIdType.MESH)
    pl.semaphore_wait(barrier, len(peers))

    src = (x_ref, dy_ref)
    TOP, BOT = (_half(i, half) for i in PAIR)
    fwd = 2

    def x_send(a):
        for i, to in enumerate((right, left)):
            rc(src[a], xh.at[a, c, t], xs.at[a], xr.at[a, i], to).start()

    def x_pass(a):
        for i, (cc, rows, to) in enumerate(((cx(-1), TOP, right), (cx(1), BOT, left))):
            arrived(xh.at[a, cc, t], xr, (a, i), to)
            v = xh.at[a, cc, t, rows]
            rc(v, v, xs.at[a], xr.at[a, fwd], to).start()

    def x_last(a):
        arrived(xh.at[a, cx(2), t], xr, (a, fwd), right)

    def y_send(a, o):
        d = xh.at[a, cx(STEPS[o]), t]
        s = src[a] if o == OWN else d
        for i, to in enumerate((up, down)):
            rc(s, d, ys.at[a], yr.at[a, o, i], to).start()

    def y_pass(a, o):
        for i, (tt, rows, to) in enumerate(((ty(-1), TOP, up), (ty(1), BOT, down))):
            arrived(xh.at[a, cx(STEPS[o]), tt], yr, (a, o, i), to)
            v = xh.at[a, cx(STEPS[o]), tt, rows]
            rc(v, v, ys.at[a], yr.at[a, o, fwd], to).start()

    def y_last(a, o):
        arrived(xh.at[a, cx(STEPS[o]), ty(2)], yr, (a, o, fwd), up)

    def e_copy(a):
        return rc(xh.at[a, :, :, :, _lane((2 * c + 1 - k) * dp, dp)], xp.at[a], es.at[0], er.at[a], mate)

    def w_in(w, cc):
        return (wd_ref if w == DOWN else wt.at[w]).at[_row(cc * ft, ft), :]

    def w_send(w):
        for o in (RIGHT, LEFT, FAR):
            rc(w_in(w, cx(STEPS[o])), wsl.at[w, c, k], ws.at[w], wr.at[w, o], dev(cx(STEPS[o]), t, k)).start()

    def w_mate(w):
        rc(w_in(w, c), wsl.at[w, c, k], ps.at[w], pr.at[w, OWN], mate).start()

    def w_pass(w, o):
        v = wsl.at[w, cx(STEPS[o]), k]
        arrived(v, wr, (w, {RIGHT: LEFT, LEFT: RIGHT, FAR: FAR}[o]), mate)
        rc(v, v, ps.at[w], pr.at[w, o], mate).start()

    def w_got(w, o):
        arrived(wsl.at[w, cx(STEPS[o]), 1 - k], pr, (w, o), mate)

    def p_copy(w):
        return rc((wg_ref, wu_ref, wdt)[w], wmt.at[w], es.at[1], er.at[len(PAIR) + w], mate)

    def gs(q, j, u):
        return nj * q + j if u is None else nj + last + u

    def gv(q, j, kk, cc, u=None):
        b = (dda if q else ha).at[j, kk, cc]
        return b if u is None else b.at[:, u]

    def g_some(q, j, kk, n, u):
        b = (dda if q else ha).at[j, kk, pl.ds(0, n)]
        return b if u is None else b.at[:, :, u]

    def gp(q, j, kk, cc, i, u=None):
        b = (dda if q else ha).at[j, kk, cc, i]
        return b if u is None else b.at[u]

    HOP, PASSED, MATE_NEAR, MATE_FAR = 0, 2, 3, 4

    def g_send(q, j, u=None):
        s = gs(q, j, u)
        v = gv(q, j, k, c, u)
        for i, to in ((HOP, right), (HOP + 1, left), (MATE_NEAR, mate)):
            rc(v, v, ags.at[s, 0], agr.at[s, i], to).start()

    def g_pass(q, j, u=None):
        s = gs(q, j, u)
        for i, (cc, to) in enumerate(((cx(-1), right), (cx(1), left))):
            v = gv(q, j, k, cc, u)
            arrived(v, agr, (s, HOP + i), to)
            p = gp(q, j, k, cc, i, u)
            rc(p, p, ags.at[s, 1], agr.at[s, PASSED], to).start()
            rc(v, v, ags.at[s, 1], agr.at[s, MATE_NEAR], mate).start()

    def g_last(q, j, u=None):
        s = gs(q, j, u)
        v = gv(q, j, k, cx(2), u)
        arrived(v, agr, (s, PASSED), right)
        rc(v, v, ags.at[s, 0], agr.at[s, MATE_FAR], mate).start()

    def g_mate_near(q, j, u=None):
        arrived(g_some(q, j, 1 - k, nc - 1, u), agr, (gs(q, j, u), MATE_NEAR), mate)

    def g_mate_far(q, j, u=None):
        arrived(gv(q, j, 1 - k, cx(2), u), agr, (gs(q, j, u), MATE_FAR), mate)

    def g_sent(q, j, u=None):
        for i in PAIR:
            left_for(g_some(q, j, k, nc - i, u), ags.at[gs(q, j, u), i])

    def sent_tokens():
        for a in PAIR:
            left_for(xh.at[a, pl.ds(0, nc - 1), 0], xs.at[a])
            left_for(xh.at[a, pl.ds(0, nc - 1)], ys.at[a])
        left_for(xp, es.at[0])

    def sent_weights():
        for w in WEIGHTS:
            left_for(wsl.at[w, pl.ds(0, nc - 1), 0], ws.at[w])
            left_for(wsl.at[w, :, 0], ps.at[w])
        left_for(wmt, es.at[1])

    def phase1(acc, xb, wide, tall, xv, wv, dv, bsem, tsem, sem):
        def x_in(a):
            return pltpu.make_async_copy(src[a], xb.at[a], bsem.at[0, a])

        def x_out(a):
            return pltpu.make_async_copy(xb.at[a], xh.at[a, c, t], bsem.at[1, a])

        def place(w):
            return (tall, wide) if w == DOWN else (wide, tall)

        def s_in(w):
            return pltpu.make_async_copy((wg_ref, wu_ref, wd_ref)[w], place(w)[0], tsem.at[0, w])

        def s_out(w):
            return pltpu.make_async_copy(place(w)[1], wdt if w == DOWN else wt.at[w], tsem.at[1, w])

        def s_own(w):
            s = place(w)[0 if w == DOWN else 1].at[_row(c * ft, ft), :]
            return pltpu.make_async_copy(s, wsl.at[w, c, k], tsem.at[2, w])

        def turned(w):
            a, b = place(w)

            @pl.loop(0, fc // LANES)
            def _(n):
                rows, cols = _row(n * LANES, LANES), _lane(n * LANES, LANES)
                if w == DOWN:
                    b[:, cols] = _turned(a[rows, :])
                else:
                    b[rows, :] = _turned(a[:, cols])
            _start([s_out(w)])
            _start([s_own(w)])

        x_send(X)
        y_send(X, OWN)
        x_send(DY)
        _start([s_in(GATE)] + [x_in(a) for a in PAIR])
        s_in(GATE).wait()
        turned(GATE)
        _start([s_in(UP)])
        for a in PAIR:
            x_in(a).wait()
            _start([x_out(a)])
        _wait([s_in(UP), s_out(GATE), s_own(GATE)])
        turned(UP)
        for w in WEIGHTS:
            _clear(acc.at[w])
        _wait([s_out(UP), s_own(UP)])
        _start([s_in(DOWN)])
        x_pass(X)
        y_send(X, RIGHT)
        y_send(X, LEFT)
        for w in WEIGHTS:
            w_mate(w)
        s_in(DOWN).wait()
        turned(DOWN)
        s_out(DOWN).wait()
        x_pass(DY)
        x_last(X)
        y_send(X, FAR)
        w_send(GATE)
        for w in WEIGHTS:
            p_copy(w).start()
        x_last(DY)
        s_own(DOWN).wait()
        for a in PAIR:
            x_out(a).wait()
        for o in CHIPS:
            y_pass(X, o)
        for o in CHIPS:
            y_send(DY, o)
        y_last(X, OWN)
        y_last(X, RIGHT)
        w_send(UP)
        w_pass(GATE, LEFT)
        w_pass(GATE, RIGHT)
        y_last(X, LEFT)
        y_last(X, FAR)

        def x_load(a, o, slot):
            cols = _lane(cx(STEPS[o]) * dc, dc)
            return [pltpu.make_async_copy(xh.at[a, :, :, pl.ds(j * ROWS, ROWS), cols], xv.at[slot, j], sem.at[slot, j])
                    for j in range(nj)]

        def w_load(w, o, slot):
            return [pltpu.make_async_copy(wsl.at[w, cx(STEPS[o]), kk], wv.at[slot, :, _half(kk, dp)], sem.at[slot, nj + kk])
                    for kk in PAIR]

        def matmul(w, slot):
            @pl.loop(0, nj)
            def _(j):
                cols = _lane(j * mc, mc)
                acc[w, :, cols] += _nt(wv[slot], xv[slot, j].reshape(mc, dc))

        n_parts = len(CHIPS)
        parts = [(w, o) for w in WEIGHTS for o in CHIPS]

        def products(before, early, after):
            def tokens(n):
                w, o = parts[n]
                _start(x_load(DY if w == DOWN else X, o, n % 2))

            def read(n):
                before(*parts[n])
                _start(w_load(*parts[n], n % 2))

            tokens(0)
            read(0)

            @pl.loop(0, len(parts))
            def _(n):
                for m, (w, o) in enumerate(parts[:-1]):
                    @pl.when(n == m)
                    def _():
                        if parts[m + 1] != (DOWN, OWN):
                            tokens(m + 1)
                        if parts[m + 1] in early:
                            read(m + 1)
                _wait(w_load(GATE, OWN, n % 2) + x_load(X, OWN, n % 2))
                matmul(n // n_parts, n % 2)
                for m, (w, o) in enumerate(parts[:-1]):
                    @pl.when(n == m)
                    def _():
                        if o == FAR:
                            after(w)
                        if parts[m + 1] == (DOWN, OWN):
                            tokens(m + 1)
                        if parts[m + 1] not in early:
                            read(m + 1)

        def h_out(j):
            return pltpu.make_async_copy(dv.at[j, 0], ha.at[j, k, c], sem.at[0, j])

        def d_out(j):
            return pltpu.make_async_copy(dv.at[j], dda.at[j, k, c], sem.at[0, j])

        step = 2 * ROWS

        def hidden():
            @pl.loop(0, nj)
            def _(j):
                @pl.loop(0, ft // step)
                def _(r):
                    rows, cols = _row(r * step, step), _lane(j * mc, mc)
                    aa = acc[GATE, rows, cols]
                    h = (aa * jax.nn.sigmoid(aa) * acc[UP, rows, cols]).astype(BF16)
                    for u in PAIR:
                        dv[j, 0, u, rows, :] = h[:, u * hc:(u + 1) * hc]
                _start([h_out(j)])
            for j in range(nj):
                h_out(j).wait()

        def grads():
            @pl.loop(0, nj)
            def _(j):
                @pl.loop(0, ft // step)
                def _(r):
                    rows, cols = _row(r * step, step), _lane(j * mc, mc)
                    aa, gg = acc[GATE, rows, cols], acc[DOWN, rows, cols]
                    sig = jax.nn.sigmoid(aa)
                    da = (gg * acc[UP, rows, cols] * sig * (1.0 + aa * (1.0 - sig))).astype(BF16)
                    db = (gg * (aa * sig)).astype(BF16)
                    for q, v in enumerate((da, db)):
                        for u in PAIR:
                            dv[j, q, u, rows, :] = v[:, u * hc:(u + 1) * hc]
                _start([d_out(j)])
            for j in range(nj):
                d_out(j).wait()

        def before(w, o):
            if (w, o) == (UP, FAR):
                y_pass(DY, LEFT)
                w_pass(UP, FAR)
                y_pass(DY, FAR)
            elif (w, o) == (DOWN, RIGHT):
                w_pass(DOWN, LEFT)
                w_pass(DOWN, RIGHT)
            elif o != OWN and (w == UP or o == FAR):
                w_pass(w, o)
            w_got(w, o)

        def after(w):
            if w == GATE:
                y_pass(DY, OWN)
                y_pass(DY, RIGHT)
                w_send(DOWN)
                return
            hidden()
            for j in range(3):
                g_send(H, j)
            e_copy(X).start()
            for o in CHIPS:
                y_last(DY, o)

        early = [(GATE, o) for o in CHIPS] + [(UP, LEFT), (DOWN, LEFT)]
        products(before, early, after)
        e_copy(DY).start()
        grads()

    sem = pltpu.SemaphoreType.DMA
    two = len(PAIR)
    pl.run_scoped(
        phase1,
        pltpu.VMEM((len(WEIGHTS), ft, nj * mc), F32),
        pltpu.VMEM((two, td, z.d), BF16),
        pltpu.VMEM((dp, fc), BF16),
        pltpu.VMEM((fc, dp), BF16),
        pltpu.VMEM((two, nj, nc, ny, ROWS, dc), BF16),
        pltpu.VMEM((two, ft, dc), BF16),
        pltpu.VMEM((nj, two, two, ft, hc), BF16),
        sem((two, two)), sem((3, 3)), sem((two, nj + two)),
    )

    def at_of(q, j):
        return nj * q + j

    def phase2(pt, pv, rv, tv, ov, sb, ssem, fsem, lsem, osem):
        def wide_load(dst, own, other, s):
            return [pltpu.make_async_copy(v, dst.at[_row(kk * dp, dp), :], s.at[i])
                    for i, (v, kk) in enumerate(zip((own, other), kinds))]

        def share_load(q, j, o, u=None):
            cc, slot = chip(o), o % 2
            at = _row(cc * ft - z.under(cc), ft)
            cps = []
            for i in range(1 + q):
                for v in PAIR if u is None else (u,):
                    s = dda.at[j, k, cc, i, v] if q else ha.at[j, k, cc, v]
                    cols = _half(v, hc) if u is None else _lane(v * hc, hc)
                    cps.append(pltpu.make_async_copy(s, sb.at[slot, i, at, cols], ssem.at[slot, i, v]))
            return cps

        low = min(z.cover - ft, ft)

        def share_blank(q, slot):
            for i in range(1 + q):
                for a in (0, z.cover - low):
                    sb[slot, i, pl.ds(a, low), :] = jnp.zeros((low, mc), BF16)

        def share_start(q, j, o):
            share_blank(q, o % 2)
            _start(share_load(q, j, o), True)

        def share(q, j, o, wc, u=None):
            _wait(share_load(q, j, o, u))
            cols = _lane(z.under(chip(o)), z.cover)
            p = at_of(q, j) % 2
            at = _head(mc) if u is None else _lane(u * hc, hc)
            if q:
                @pl.loop(0, two)
                def _(i):
                    pt[p, :, at] += _nn(wc[i, :, cols], sb[o % 2, i, :, at])
            else:
                pt[p, :, at] += _nn(wc[:, cols], sb[o % 2, 0, :, at])

        def shares(q, j, wc, first, end):
            @pl.loop(first, end)
            def _(o):
                @pl.when(o + 1 < end)
                def _():
                    share_start(q, j, o + 1)
                share(q, j, o, wc)

        def front(q, j, wc):
            _clear(pt.at[at_of(q, j) % 2])
            shares(q, j, wc, OWN, FAR)

        def upright(q, j, u):
            p = s = at_of(q, j) % 2
            wide = 2 * LANES

            @pl.loop(0, dc // wide)
            def _(i):
                v = pt[p, _row(i * wide, wide), _lane(u * hc, hc)].T
                pv[s, pl.ds(u * hn, hn), :, :, _lane(i * wide, wide)] = v.reshape(hn, ny, ROWS, wide)

        def rs_send(s, u, dst=None):
            near_first = list(range(1, ny))
            far_first = sorted(near_first, key=lambda i: -min(i, ny - i))
            for i in near_first if dst is None else far_first:
                to = rsb.at[s, u, i - 1] if dst is None else dst.at[u, i - 1]
                rc(pv.at[s % 2, pl.ds(u * hn, hn), ty(i)], to, rss.at[s], rsr.at[s, u], dev(c, ty(i), k)).start()

        def rs_free(s):
            left_for(pv.at[s % 2, :, pl.ds(0, ny - 1)], rss.at[s])

        def send_up(q, j):
            if q:
                rs_free(at_of(q, j) - 2)
            else:
                @pl.when(j > 1)
                def _():
                    rs_free(j - 2)

            @pl.loop(0, two)
            def _(u):
                upright(q, j, u)
                rs_send(at_of(q, j), u)

        def out_rows(q, j):
            return (dx_ref if q else y_ref).at[_row(j * ROWS, ROWS), _lane(c * dc, dc)]

        def out_one(s, rows, dst, cc):
            @pl.when(cc != c)
            def _():
                rc(rows.at[cc], dst, a2s.at[s], a2r.at[s], dev(cc, t, k)).start()

            @pl.when(cc == c)
            def _():
                _start([pltpu.make_async_copy(rows.at[cc], dst, lsem.at[s])], True)

        def out_send(q, j):
            s = at_of(q, j)
            for cc in range(nc):
                out_one(s, ovh.at[s], out_rows(q, j), cc)

        def out_done(s):
            v = ovh.at[s, _head(nc - 1)]
            left_for(v, a2s.at[s])
            arrived(v, a2r, s, mate)
            pltpu.make_async_copy(ovh.at[s, c], out_rows(H, 0), lsem.at[s]).wait()

        def stored(s):
            return pltpu.make_async_copy(ov.at[s % 2], ovh.at[s], osem.at[s % 2])

        def residual(q, j, u):
            rows = pl.ds(u * hn, hn)
            return pltpu.make_async_copy(xh.at[q, rows, t, _row(j * ROWS, ROWS), _lane(c * dc, dc)], tv.at[rows],
                                         fsem.at[1, u])

        def finish_loads(q, j, u):
            return [pltpu.make_async_copy(rsb.at[at_of(q, j), u], rv.at[u], fsem.at[0, u]), residual(q, j, u)]

        def finish_start(q, j):
            @pl.loop(0, two)
            def _(u):
                arrived(rsb.at[at_of(q, j), u], rsr, (at_of(q, j), u), mate)
                _start(finish_loads(q, j, u), True)

        def finish(q, j, late=None):
            s = at_of(q, j)

            @pl.loop(0, two)
            def _(u):
                if late is None:
                    _wait(finish_loads(q, j, u))
                else:
                    arrived(late.at[u], rsr, (s, u), mate)
                    residual(q, j, u).wait()
                for i in range(hn):
                    cc = u * hn + i
                    tot = pv[s % 2, cc, t]
                    for m in range(ny - 1):
                        tot = tot + (rv if late is None else late)[u, m, i]
                    ov[s % 2, cc] = (tv[cc].astype(F32) + tot).astype(BF16)
                    if late is not None:
                        out_one(s, ov.at[s % 2], out_rows(q, j), cc)

            if late is None:
                _start([stored(s)])

        def tok_load(a, j, buf, s):
            rows = _row(j * ROWS, ROWS)
            return [pltpu.make_async_copy(xh.at[a, :, :, rows, _lane(me * dp, dp)], buf.at[0], s.at[0]),
                    pltpu.make_async_copy(xp.at[a, :, :, rows, :], buf.at[1], s.at[1])]

        def phase2h(wc, hv, kv, psem, dsem, ksem):
            p_copy(DOWN).wait_recv()
            loads = wide_load(wc, wdt, wmt.at[DOWN], psem)
            _start(loads)
            g_pass(H, 0)
            g_send(H, 3)
            _clear(dwd)
            for w in PAIR:
                p_copy(w).wait_recv()
                e_copy(w).wait_recv()
            _wait(loads)

            def h_load(j, os, hs=PAIR):
                return [pltpu.make_async_copy(ha.at[j, kinds[i], cx(STEPS[o]), u],
                                              hv.at[_row(cx(STEPS[o]) * ft, ft), pl.ds(i * mc + u * hc, hc)],
                                              dsem.at[i, o, u])
                        for i in hs for o in os for u in PAIR]

            def add_outer(first, end):
                @pl.loop(first, end)
                def _(o):
                    rows = _row(chip(o) * ft, ft)
                    dwd[rows, :] += _nn(hv[rows, :], kv[...].reshape(2 * mc, dp))

            near = (OWN, RIGHT, LEFT)
            share_start(H, 0, OWN)

            @pl.loop(0, nj + 1)
            def _(j):
                here, before, two_before = j < nj, j > 0, j > 1

                @pl.when(before & here)
                def _():
                    g_pass(H, j)

                @pl.when(j == nj)
                def _():
                    g_pass(D, 0)
                    g_send(D, 2)

                @pl.when(j == 1)
                def _():
                    g_send(D, 0)

                @pl.when(j == last)
                def _():
                    g_send(D, 1)

                @pl.when(before)
                def _():
                    g_mate_near(H, j - 1)
                    _start(tok_load(DY, j - 1, kv, ksem))
                    _start(h_load(j - 1, near))

                @pl.when(here)
                def _():
                    front(H, j, wc)

                @pl.when(before)
                def _():
                    g_last(H, j - 1)
                    share_start(H, j - 1, FAR)
                    _start(h_load(j - 1, (FAR,), (0,)))

                @pl.when(j < last)
                def _():
                    share_start(H, j + 1, OWN)

                @pl.when(j == last)
                def _():
                    share_start(D, 0, OWN)

                @pl.when(before)
                def _():
                    _wait(tok_load(DY, j - 1, kv, ksem))
                    _wait(h_load(j - 1, near))
                    add_outer(OWN, FAR)
                    shares(H, j - 1, wc, FAR, FAR + 1)
                    g_mate_far(H, j - 1)
                    _start(h_load(j - 1, (FAR,), (1,)))
                    send_up(H, j - 1)

                @pl.when(two_before)
                def _():
                    finish_start(H, j - 2)

                @pl.when(before)
                def _():
                    _wait(h_load(j - 1, (FAR,)))
                    add_outer(FAR, FAR + 1)

                @pl.when(j > 3)
                def _():
                    stored(j - 4).wait()

                @pl.when(two_before)
                def _():
                    finish(H, j - 2)

        pl.run_scoped(
            phase2h,
            pltpu.VMEM((dc, fc), BF16),
            pltpu.VMEM((fc, 2 * mc), BF16),
            pltpu.VMEM((two, nc, ny, ROWS, dp), BF16),
            sem((two,)), sem((two, len(CHIPS), two)), sem((two,)),
        )

        def phase2d(wc, dv, kv, kt, wsem, dsem, ksem):
            loads = [cp for w in PAIR for cp in wide_load(wc.at[w], (wg_ref, wu_ref)[w], wmt.at[w], wsem.at[w])]
            _start(loads)
            for w in PAIR:
                _clear(dw.at[w])
            _wait(loads)

            def d_load(j, os, hs=PAIR, us=PAIR):
                return [pltpu.make_async_copy(dda.at[j, kinds[i], cx(STEPS[o]), q, u],
                                              dv.at[q, _row(cx(STEPS[o]) * ft, ft), pl.ds(i * mc + u * hc, hc)],
                                              dsem.at[i, o, q, u])
                        for i in hs for o in os for q in PAIR for u in us]

            def add_outer():
                n = fc // z.cuts

                @pl.loop(0, z.cuts * two)
                def _(i):
                    q, cols = i // z.cuts, _lane(i % z.cuts * n, n)
                    dw[q, :, cols] += _nt(kt[...], dv[q, cols, :])

            def far(j, us=(None,)):
                for u in us:
                    g_mate_far(D, j, u)
                _start(d_load(j, (FAR,), (1,)))
                _wait(tok_load(X, j, kv, ksem))

                @pl.loop(0, dp // LANES)
                def _(i):
                    v = kv[:, :, :, :, _lane(i * LANES, LANES)].reshape(2 * mc, LANES)
                    kt[_row(i * LANES, LANES), :] = _turned(v)

            def back(j):
                g_last(D, j)
                share_start(D, j, FAR)
                _start(d_load(j, (FAR,), (0,)))

            near = (OWN, RIGHT, LEFT)

            def near_start(j):
                g_mate_near(D, j)
                _start(tok_load(X, j, kv, ksem))
                _start(d_load(j, near))

            @pl.loop(0, last)
            def _(j):
                before, first = j > 0, j == 1

                @pl.when(first)
                def _():
                    sent_tokens()
                    sent_weights()

                @pl.when(before)
                def _():
                    g_pass(D, j)

                @pl.when(before & (j < last - 2))
                def _():
                    g_send(D, j + 2)

                @pl.when(j == last - 1)
                def _():
                    for u in PAIR:
                        g_send(D, last, u)
                    for i in range(nj):
                        g_sent(H, i)

                @pl.when(before)
                def _():
                    near_start(j - 1)

                front(D, j, wc)

                @pl.when(before)
                def _():
                    back(j - 1)

                share_start(D, j + 1, OWN)

                @pl.when(before)
                def _():
                    shares(D, j - 1, wc, FAR, FAR + 1)
                    send_up(D, j - 1)

                @pl.when(first)
                def _():
                    finish_start(H, last)

                @pl.when(j > 1)
                def _():
                    finish_start(D, j - 2)

                @pl.when(before)
                def _():
                    far(j - 1)
                    _wait(d_load(j - 1, CHIPS))
                    add_outer()

                @pl.when(before)
                def _():
                    stored(nj + j - 4).wait()

                @pl.when(first)
                def _():
                    finish(H, last)

                @pl.when(j > 1)
                def _():
                    finish(D, j - 2)

            m = last - 1
            near_start(m)
            back(m)
            _clear(pt.at[at_of(D, last) % 2])
            shares(D, m, wc, FAR, FAR + 1)
            send_up(D, m)
            far(m)
            shares(D, last, wc, OWN, RIGHT)
            g_pass(D, last, 0)
            _wait(d_load(m, CHIPS))
            add_outer()
            finish_start(D, m - 1)
            stored(nj + m - 3).wait()
            finish(D, m - 1)
            for i in range(m):
                g_sent(D, i)
            _start(tok_load(X, last, kv, ksem))
            g_pass(D, last, 1)
            share_start(D, last, RIGHT)
            share_start(D, last, LEFT)
            _start(d_load(last, near, (0,)))
            share(D, last, RIGHT, wc)
            share_blank(D, FAR % 2)
            rs_free(at_of(D, last) - 2)
            share(D, last, LEFT, wc)
            g_last(D, last, 0)
            _start(share_load(D, last, FAR, 0), True)

            @pl.loop(0, two)
            def _(u):
                @pl.when(u == 1)
                def _():
                    g_last(D, last, 1)
                    _start(share_load(D, last, FAR, 1), True)
                    for i in PAIR:
                        stored(nj + m - 2 + i).wait()

                    @pl.loop(0, nj)
                    def _(i):
                        out_send(H, i)

                    @pl.loop(0, m)
                    def _(i):
                        out_send(D, i)
                share(D, last, FAR, wc, u)
                upright(D, last, u)
                rs_send(at_of(D, last), u, rsv)

                @pl.when(u == 0)
                def _():
                    finish_start(D, m)
            for u in PAIR:
                g_mate_near(D, last, u)
            _start(d_load(last, near, (1,)))
            _start(d_load(last, (FAR,), (0,)))
            finish(D, m)
            far(last, PAIR)
            g_sent(D, m)
            for u in PAIR:
                g_sent(D, last, u)
            _wait(d_load(last, CHIPS))
            _start([residual(D, last, u) for u in PAIR], True)
            add_outer()
            stored(nj + m).wait()
            out_send(D, m)
            finish(D, last, rsv)
            for i in PAIR:
                rs_free(nj + last - i)

            @pl.loop(0, 2 * nj)
            def _(i):
                out_done(i)

        pl.run_scoped(
            phase2d,
            pltpu.VMEM((two, dc, fc), BF16),
            pltpu.VMEM((two, fc, 2 * mc), BF16),
            pltpu.VMEM((two, nc, ny, ROWS, dp), BF16),
            pltpu.VMEM((dp, 2 * mc), BF16),
            sem((two, two)), sem((two, len(CHIPS), two, two)), sem((two,)),
        )

    pl.run_scoped(
        phase2,
        pltpu.VMEM((two, dc, mc), F32),
        pltpu.VMEM((two, nc, ny, ROWS, dc), F32),
        pltpu.VMEM((two, ny - 1, hn, ROWS, dc), F32),
        pltpu.VMEM((nc, ROWS, dc), BF16),
        pltpu.VMEM((two, nc, ROWS, dc), BF16),
        pltpu.VMEM((two, two, z.cover, mc), BF16),
        sem((two, two, two)), sem((two, two)), sem((2 * nj,)), sem((two,)),
    )


def _move(cuts, y, dx, dw, dwd, y_out, dx_out, dwg_out, dwu_out, dwd_out, bufs, sems):
    rows = [(y, bufs.at[0], y_out), (dx, bufs.at[1], dx_out)]
    grads = [(dwd, dwd_out)] + [(dw.at[q], o) for q, o in enumerate((dwg_out, dwu_out))]
    read = [pltpu.make_async_copy(a, b, sems.at[i]) for i, (a, b, _) in enumerate(rows)]
    write = [pltpu.make_async_copy(b, o, sems.at[i]) for i, (_, b, o) in enumerate(rows)]
    out = []
    for r in range(cuts):
        for a, o in grads:
            n = a.shape[0] // cuts
            out.append(pltpu.make_async_copy(a.at[_half(r, n)], o.at[_half(r, n)], sems.at[len(rows) + len(out)]))
    _start(read, True)
    for i in PAIR:
        _start(out[i::2], i == 1)
    for a, b in zip(read, write):
        a.wait()
        _start([b], True)
    _wait(write + out)


def _results(y, dx, dw, dwd, like, cuts):
    hbm, vmem = pltpu.HBM, pltpu.VMEM
    spaces = (hbm, hbm, vmem, vmem)
    like = jax.ShapeDtypeStruct(like.shape, F32)
    rows = [jax.ShapeDtypeStruct(a.shape, a.dtype) for a in (y, dx)]
    outs = rows + [like, like, jax.ShapeDtypeStruct(dwd.shape, F32)]
    return pl.pallas_call(
        functools.partial(_move, cuts),
        out_shape=outs,
        in_specs=[pl.BlockSpec(memory_space=m) for m in spaces],
        out_specs=[pl.BlockSpec(memory_space=hbm)] * len(outs),
        scratch_shapes=[vmem((len(rows), *y.shape), y.dtype), pltpu.SemaphoreType.DMA((len(rows) + 3 * cuts,))],
        name="results",
        compiler_params=pltpu.CompilerParams(vmem_limit_bytes=VMEM_LIMIT // 10),
    )(*(pltpu.with_memory_space_constraint(v, m) for v, m in zip((y, dx, dw, dwd), spaces)))


def solution(mesh):
    nx, ny = mesh.shape["dp"], mesh.shape["tp"]
    axes = mesh.axis_names
    row_spec = P(("part", "dp", "tp"), None)
    win_spec = P(("part", "dp"), "tp")
    wout_spec = P(("part", "tp"), "dp")

    def f(x, wg, wu, wd, dy):
        z = Sizes(axes, nx, ny, x, wg)
        steps, two, kinds = 2 * z.nj, len(PAIR), len(WEIGHTS)
        hbm = pl.BlockSpec(memory_space=pltpu.HBM)
        vmem = pl.BlockSpec(memory_space=pltpu.VMEM)
        bf16 = functools.partial(jax.ShapeDtypeStruct, dtype=BF16)
        f32 = functools.partial(jax.ShapeDtypeStruct, dtype=F32)
        outs = [
            bf16(x.shape), bf16(x.shape), pltpu.VMEM((two, z.dp, z.fc), F32), pltpu.VMEM(wd.shape, F32),
            bf16((two, z.nc, ny, z.td, z.d)),
            bf16((two, z.nc, ny, z.td, z.dp)),
            bf16((two, z.fc, z.dp)),
            bf16((z.dp, z.fc)),
            bf16((kinds, z.nc, two, z.ft, z.dp)),
            bf16((kinds, z.dp, z.fc)),
            bf16((z.nj, two, z.nc, two, z.ft, z.hc)),
            bf16((z.nj, two, z.nc, two, two, z.ft, z.hc)),
            f32((steps, two, ny - 1, z.nc // 2, ROWS, z.dc)),
            bf16((steps, z.nc, ROWS, z.dc)),
        ]
        specs = [hbm] * len(outs)
        specs[2:4] = [vmem] * 2
        sem = pltpu.SemaphoreType.DMA
        chips = len(CHIPS)
        shapes = ((two,), (two, 3), (two,), (two, chips, 3), (kinds,), (kinds, chips), (kinds,), (kinds, chips),
                  (two,), (two + kinds,), (steps + 1, two), (steps + 1, 5), (steps,), (steps, two), (steps,), (steps,))
        r = pl.pallas_call(
            functools.partial(_kernel, z),
            out_shape=outs,
            in_specs=[hbm] * 5,
            out_specs=specs,
            scratch_shapes=[sem(shape) for shape in shapes]
            + [pltpu.VMEM((two, ny - 1, z.nc // 2, ROWS, z.dc), F32)],
            name="mlp",
            compiler_params=pltpu.CompilerParams(
                collective_id=0, has_side_effects=True, vmem_limit_bytes=VMEM_LIMIT),
        )(x, wg, wu, wd, dy)
        return tuple(_results(*r[:4], wg, 4))

    return jax.shard_map(f, mesh=mesh, in_specs=(row_spec, win_spec, win_spec, wout_spec, row_spec),
                         out_specs=(row_spec, row_spec, win_spec, win_spec, wout_spec), check_vma=False)
```

```python
import functools

import jax
import jax.numpy as jnp
from jax import lax
from jax.experimental import pallas as pl
from jax.experimental.pallas import tpu as pltpu
from jax.sharding import PartitionSpec as P

F32, BF16 = jnp.float32, jnp.bfloat16
LANES, ROWS = 128, 16
VMEM_LIMIT = 40_420_000
X, DY = PAIR = range(2)
GATE, UP, DOWN = WEIGHTS = range(3)
H, D = range(2)
OWN, RIGHT, LEFT, FAR = CHIPS = range(4)
STEPS = (0, 1, -1, 2)


class Sizes:
    def __init__(self, axes, nx, ny, x, wg):
        self.axes = axes
        self.nc, self.ny = nx // 2, ny
        self.td, self.d = x.shape
        self.dp, self.fc = wg.shape
        self.dc = 2 * self.dp
        self.ft = self.fc // self.nc
        self.nb = self.nc * ny
        self.nj = self.td // ROWS
        self.mc = self.nb * ROWS
        self.hc = self.mc // 2
        starts = [c * self.ft for c in range(self.nc)]
        self.cover = -(-max(s % LANES + self.ft for s in starts) // LANES) * LANES
        self.back = max(s // LANES * LANES for s in starts) + self.cover - self.fc
        tiles = self.fc // LANES
        self.cuts = 3 if tiles % 3 == 0 else tiles

    def under(self, cc):
        return cc * self.ft // LANES * LANES - cc // (self.nc - 1) * self.back


def _dot(a, b, ca, cb):
    return lax.dot_general(a, b, (((ca,), (cb,)), ((), ())), preferred_element_type=F32)


def _nn(a, b):
    return _dot(a, b, 1, 0)


def _nt(a, b):
    return _dot(a, b, 1, 1)


def _start(cps, urgent=False):
    for cp in cps:
        cp.start(priority=0 if urgent else 1)


def _wait(cps):
    for cp in cps:
        cp.wait()


def _lane(i, n):
    return pl.ds(pl.multiple_of(i, LANES), n)


def _row(i, n):
    return pl.ds(pl.multiple_of(i, ROWS), n)


def _head(n):
    return pl.ds(0, n)


def _half(u, n):
    return pl.ds(u * n, n)


def _clear(acc):
    n = 2 * ROWS

    @pl.loop(0, acc.shape[0] // n)
    def _(i):
        acc[_row(i * n, n), :] = jnp.zeros((n, acc.shape[1]), F32)


def _turned(v):
    return v.astype(F32).T.astype(BF16)


def _kernel(z, x_ref, wg_ref, wu_ref, wd_ref, dy_ref,
            y_ref, dx_ref, dw, dwd,
            xh, xp, wt, wdt, wsl, wmt, ha, dda, rsb, ovh,
            xs, xr, ys, yr, ws, wr, ps, pr, es, er, ags, agr, rss, rsr, a2s, a2r, rsv):
    nc, ny, nj = z.nc, z.ny, z.nj
    ft, fc, dp, dc, mc, hc, td = z.ft, z.fc, z.dp, z.dc, z.mc, z.hc, z.td
    half, hn, last = td // 2, nc // 2, nj - 1
    me = lax.axis_index("dp")
    t = lax.axis_index("tp")
    part = lax.axis_index("part")
    c, k = me // 2, me % 2

    def dev(cc, tt, kk):
        ids = {"part": part, "tp": tt, "dp": 2 * cc + kk}
        return tuple(ids[a] for a in z.axes)

    def cx(i):
        return (c + i + nc) % nc

    def ty(i):
        return (t + i + ny) % ny

    def chip(o):
        return cx(o + o // 2 - 2 * (o // 3))

    right, left = dev(cx(1), t, k), dev(cx(-1), t, k)
    up, down = dev(c, ty(1), k), dev(c, ty(-1), k)
    mate = dev(c, t, 1 - k)
    kinds = (k, 1 - k)

    def rc(src, dst, s, r, to):
        return pltpu.make_async_remote_copy(
            src_ref=src, dst_ref=dst, send_sem=s, recv_sem=r, device_id=to,
            device_id_type=pl.DeviceIdType.MESH)

    def arrived(v, r, i, frm):
        rc(v, v, r.at[i], r.at[i], frm).wait_recv()

    def left_for(v, s):
        rc(v, v, s, s, mate).wait_send()

    barrier = pltpu.get_barrier_semaphore()
    peers = [dev(cx(i), t, k) for i in range(1, nc)] + [dev(c, ty(i), k) for i in range(1, ny)] + [mate]
    for peer in peers:
        pl.semaphore_signal(barrier, device_id=peer, device_id_type=pl.DeviceIdType.MESH)
    pl.semaphore_wait(barrier, len(peers))

    src = (x_ref, dy_ref)
    TOP, BOT = (_half(i, half) for i in PAIR)
    fwd = 2

    def x_send(a):
        for i, to in enumerate((right, left)):
            rc(src[a], xh.at[a, c, t], xs.at[a], xr.at[a, i], to).start()

    def x_pass(a):
        for i, (cc, rows, to) in enumerate(((cx(-1), TOP, right), (cx(1), BOT, left))):
            arrived(xh.at[a, cc, t], xr, (a, i), to)
            v = xh.at[a, cc, t, rows]
            rc(v, v, xs.at[a], xr.at[a, fwd], to).start()

    def x_last(a):
        arrived(xh.at[a, cx(2), t], xr, (a, fwd), right)

    def y_send(a, o):
        d = xh.at[a, cx(STEPS[o]), t]
        s = src[a] if o == OWN else d
        for i, to in enumerate((up, down)):
            rc(s, d, ys.at[a], yr.at[a, o, i], to).start()

    def y_pass(a, o):
        for i, (tt, rows, to) in enumerate(((ty(-1), TOP, up), (ty(1), BOT, down))):
            arrived(xh.at[a, cx(STEPS[o]), tt], yr, (a, o, i), to)
            v = xh.at[a, cx(STEPS[o]), tt, rows]
            rc(v, v, ys.at[a], yr.at[a, o, fwd], to).start()

    def y_last(a, o):
        arrived(xh.at[a, cx(STEPS[o]), ty(2)], yr, (a, o, fwd), up)

    def e_copy(a):
        return rc(xh.at[a, :, :, :, _lane((2 * c + 1 - k) * dp, dp)], xp.at[a], es.at[0], er.at[a], mate)

    def w_in(w, cc):
        return (wd_ref if w == DOWN else wt.at[w]).at[_row(cc * ft, ft), :]

    def w_send(w):
        for o in (RIGHT, LEFT, FAR):
            rc(w_in(w, cx(STEPS[o])), wsl.at[w, c, k], ws.at[w], wr.at[w, o], dev(cx(STEPS[o]), t, k)).start()

    def w_mate(w):
        rc(w_in(w, c), wsl.at[w, c, k], ps.at[w], pr.at[w, OWN], mate).start()

    def w_pass(w, o):
        v = wsl.at[w, cx(STEPS[o]), k]
        arrived(v, wr, (w, {RIGHT: LEFT, LEFT: RIGHT, FAR: FAR}[o]), mate)
        rc(v, v, ps.at[w], pr.at[w, o], mate).start()

    def w_got(w, o):
        arrived(wsl.at[w, cx(STEPS[o]), 1 - k], pr, (w, o), mate)

    def p_copy(w):
        return rc((wg_ref, wu_ref, wdt)[w], wmt.at[w], es.at[1], er.at[len(PAIR) + w], mate)

    def gs(q, j, u):
        return nj * q + j if u is None else nj + last + u

    def gv(q, j, kk, cc, u=None):
        b = (dda if q else ha).at[j, kk, cc]
        return b if u is None else b.at[:, u]

    def g_some(q, j, kk, n, u):
        b = (dda if q else ha).at[j, kk, pl.ds(0, n)]
        return b if u is None else b.at[:, :, u]

    def gp(q, j, kk, cc, i, u=None):
        b = (dda if q else ha).at[j, kk, cc, i]
        return b if u is None else b.at[u]

    HOP, PASSED, MATE_NEAR, MATE_FAR = 0, 2, 3, 4

    def g_send(q, j, u=None):
        s = gs(q, j, u)
        v = gv(q, j, k, c, u)
        for i, to in ((HOP, right), (HOP + 1, left), (MATE_NEAR, mate)):
            rc(v, v, ags.at[s, 0], agr.at[s, i], to).start()

    def g_pass(q, j, u=None):
        s = gs(q, j, u)
        for i, (cc, to) in enumerate(((cx(-1), right), (cx(1), left))):
            v = gv(q, j, k, cc, u)
            arrived(v, agr, (s, HOP + i), to)
            p = gp(q, j, k, cc, i, u)
            rc(p, p, ags.at[s, 1], agr.at[s, PASSED], to).start()
            rc(v, v, ags.at[s, 1], agr.at[s, MATE_NEAR], mate).start()

    def g_last(q, j, u=None):
        s = gs(q, j, u)
        v = gv(q, j, k, cx(2), u)
        arrived(v, agr, (s, PASSED), right)
        rc(v, v, ags.at[s, 0], agr.at[s, MATE_FAR], mate).start()

    def g_mate_near(q, j, u=None):
        arrived(g_some(q, j, 1 - k, nc - 1, u), agr, (gs(q, j, u), MATE_NEAR), mate)

    def g_mate_far(q, j, u=None):
        arrived(gv(q, j, 1 - k, cx(2), u), agr, (gs(q, j, u), MATE_FAR), mate)

    def g_sent(q, j, u=None):
        for i in PAIR:
            left_for(g_some(q, j, k, nc - i, u), ags.at[gs(q, j, u), i])

    def sent_tokens():
        for a in PAIR:
            left_for(xh.at[a, pl.ds(0, nc - 1), 0], xs.at[a])
            left_for(xh.at[a, pl.ds(0, nc - 1)], ys.at[a])
        left_for(xp, es.at[0])

    def sent_weights():
        for w in WEIGHTS:
            left_for(wsl.at[w, pl.ds(0, nc - 1), 0], ws.at[w])
            left_for(wsl.at[w, :, 0], ps.at[w])
        left_for(wmt, es.at[1])

    def phase1(acc, xb, wide, tall, xv, wv, dv, bsem, tsem, sem):
        def x_in(a):
            return pltpu.make_async_copy(src[a], xb.at[a], bsem.at[0, a])

        def x_out(a):
            return pltpu.make_async_copy(xb.at[a], xh.at[a, c, t], bsem.at[1, a])

        def place(w):
            return (tall, wide) if w == DOWN else (wide, tall)

        def s_in(w):
            return pltpu.make_async_copy((wg_ref, wu_ref, wd_ref)[w], place(w)[0], tsem.at[0, w])

        def s_out(w):
            return pltpu.make_async_copy(place(w)[1], wdt if w == DOWN else wt.at[w], tsem.at[1, w])

        def s_own(w):
            s = place(w)[0 if w == DOWN else 1].at[_row(c * ft, ft), :]
            return pltpu.make_async_copy(s, wsl.at[w, c, k], tsem.at[2, w])

        def turned(w):
            a, b = place(w)

            @pl.loop(0, fc // LANES)
            def _(n):
                rows, cols = _row(n * LANES, LANES), _lane(n * LANES, LANES)
                if w == DOWN:
                    b[:, cols] = _turned(a[rows, :])
                else:
                    b[rows, :] = _turned(a[:, cols])
            _start([s_out(w)])
            _start([s_own(w)])

        x_send(X)
        y_send(X, OWN)
        x_send(DY)
        _start([s_in(GATE)] + [x_in(a) for a in PAIR])
        s_in(GATE).wait()
        turned(GATE)
        _start([s_in(UP)])
        for a in PAIR:
            x_in(a).wait()
            _start([x_out(a)])
        _wait([s_in(UP), s_out(GATE), s_own(GATE)])
        turned(UP)
        for w in WEIGHTS:
            _clear(acc.at[w])
        _wait([s_out(UP), s_own(UP)])
        _start([s_in(DOWN)])
        x_pass(X)
        y_send(X, RIGHT)
        y_send(X, LEFT)
        for w in WEIGHTS:
            w_mate(w)
        s_in(DOWN).wait()
        turned(DOWN)
        s_out(DOWN).wait()
        x_pass(DY)
        x_last(X)
        y_send(X, FAR)
        w_send(GATE)
        for w in WEIGHTS:
            p_copy(w).start()
        x_last(DY)
        s_own(DOWN).wait()
        for a in PAIR:
            x_out(a).wait()
        for o in CHIPS:
            y_pass(X, o)
        for o in CHIPS:
            y_send(DY, o)
        y_last(X, OWN)
        y_last(X, RIGHT)
        w_send(UP)
        w_pass(GATE, LEFT)
        w_pass(GATE, RIGHT)
        y_last(X, LEFT)
        y_last(X, FAR)

        def x_load(a, o, slot):
            cols = _lane(cx(STEPS[o]) * dc, dc)
            return [pltpu.make_async_copy(xh.at[a, :, :, pl.ds(j * ROWS, ROWS), cols], xv.at[slot, j], sem.at[slot, j])
                    for j in range(nj)]

        def w_load(w, o, slot):
            return [pltpu.make_async_copy(wsl.at[w, cx(STEPS[o]), kk], wv.at[slot, :, _half(kk, dp)], sem.at[slot, nj + kk])
                    for kk in PAIR]

        def matmul(w, slot):
            @pl.loop(0, nj)
            def _(j):
                cols = _lane(j * mc, mc)
                acc[w, :, cols] += _nt(wv[slot], xv[slot, j].reshape(mc, dc))

        n_parts = len(CHIPS)
        parts = [(w, o) for w in WEIGHTS for o in CHIPS]

        def products(before, early, after):
            def tokens(n):
                w, o = parts[n]
                _start(x_load(DY if w == DOWN else X, o, n % 2))

            def read(n):
                before(*parts[n])
                _start(w_load(*parts[n], n % 2))

            tokens(0)
            read(0)

            @pl.loop(0, len(parts))
            def _(n):
                for m, (w, o) in enumerate(parts[:-1]):
                    @pl.when(n == m)
                    def _():
                        if parts[m + 1] != (DOWN, OWN):
                            tokens(m + 1)
                        if parts[m + 1] in early:
                            read(m + 1)
                _wait(w_load(GATE, OWN, n % 2) + x_load(X, OWN, n % 2))
                matmul(n // n_parts, n % 2)
                for m, (w, o) in enumerate(parts[:-1]):
                    @pl.when(n == m)
                    def _():
                        if o == FAR:
                            after(w)
                        if parts[m + 1] == (DOWN, OWN):
                            tokens(m + 1)
                        if parts[m + 1] not in early:
                            read(m + 1)

        def h_out(j):
            return pltpu.make_async_copy(dv.at[j, 0], ha.at[j, k, c], sem.at[0, j])

        def d_out(j):
            return pltpu.make_async_copy(dv.at[j], dda.at[j, k, c], sem.at[0, j])

        step = 2 * ROWS

        def hidden():
            @pl.loop(0, nj)
            def _(j):
                @pl.loop(0, ft // step)
                def _(r):
                    rows, cols = _row(r * step, step), _lane(j * mc, mc)
                    aa = acc[GATE, rows, cols]
                    h = (aa * jax.nn.sigmoid(aa) * acc[UP, rows, cols]).astype(BF16)
                    for u in PAIR:
                        dv[j, 0, u, rows, :] = h[:, u * hc:(u + 1) * hc]
                _start([h_out(j)])
            for j in range(nj):
                h_out(j).wait()

        def grads():
            @pl.loop(0, nj)
            def _(j):
                @pl.loop(0, ft // step)
                def _(r):
                    rows, cols = _row(r * step, step), _lane(j * mc, mc)
                    aa, gg = acc[GATE, rows, cols], acc[DOWN, rows, cols]
                    sig = jax.nn.sigmoid(aa)
                    da = (gg * acc[UP, rows, cols] * sig * (1.0 + aa * (1.0 - sig))).astype(BF16)
                    db = (gg * (aa * sig)).astype(BF16)
                    for q, v in enumerate((da, db)):
                        for u in PAIR:
                            dv[j, q, u, rows, :] = v[:, u * hc:(u + 1) * hc]
                _start([d_out(j)])
            for j in range(nj):
                d_out(j).wait()

        def before(w, o):
            if (w, o) == (UP, FAR):
                y_pass(DY, LEFT)
                w_pass(UP, FAR)
                y_pass(DY, FAR)
            elif (w, o) == (DOWN, RIGHT):
                w_pass(DOWN, LEFT)
                w_pass(DOWN, RIGHT)
            elif o != OWN and (w == UP or o == FAR):
                w_pass(w, o)
            w_got(w, o)

        def after(w):
            if w == GATE:
                y_pass(DY, OWN)
                y_pass(DY, RIGHT)
                w_send(DOWN)
                return
            hidden()
            for j in range(3):
                g_send(H, j)
            e_copy(X).start()
            for o in CHIPS:
                y_last(DY, o)

        early = [(GATE, o) for o in CHIPS] + [(UP, LEFT), (DOWN, LEFT)]
        products(before, early, after)
        e_copy(DY).start()
        grads()

    sem = pltpu.SemaphoreType.DMA
    two = len(PAIR)
    pl.run_scoped(
        phase1,
        pltpu.VMEM((len(WEIGHTS), ft, nj * mc), F32),
        pltpu.VMEM((two, td, z.d), BF16),
        pltpu.VMEM((dp, fc), BF16),
        pltpu.VMEM((fc, dp), BF16),
        pltpu.VMEM((two, nj, nc, ny, ROWS, dc), BF16),
        pltpu.VMEM((two, ft, dc), BF16),
        pltpu.VMEM((nj, two, two, ft, hc), BF16),
        sem((two, two)), sem((3, 3)), sem((two, nj + two)),
    )

    def at_of(q, j):
        return nj * q + j

    def phase2(pt, pv, rv, tv, ov, sb, ssem, fsem, lsem, osem):
        def wide_load(dst, own, other, s):
            return [pltpu.make_async_copy(v, dst.at[_row(kk * dp, dp), :], s.at[i])
                    for i, (v, kk) in enumerate(zip((own, other), kinds))]

        def share_load(q, j, o, u=None):
            cc, slot = chip(o), o % 2
            at = _row(cc * ft - z.under(cc), ft)
            cps = []
            for i in range(1 + q):
                for v in PAIR if u is None else (u,):
                    s = dda.at[j, k, cc, i, v] if q else ha.at[j, k, cc, v]
                    cols = _half(v, hc) if u is None else _lane(v * hc, hc)
                    cps.append(pltpu.make_async_copy(s, sb.at[slot, i, at, cols], ssem.at[slot, i, v]))
            return cps

        low = min(z.cover - ft, ft)

        def share_blank(q, slot):
            for i in range(1 + q):
                for a in (0, z.cover - low):
                    sb[slot, i, pl.ds(a, low), :] = jnp.zeros((low, mc), BF16)

        def share_start(q, j, o):
            share_blank(q, o % 2)
            _start(share_load(q, j, o), True)

        def share(q, j, o, wc, u=None):
            _wait(share_load(q, j, o, u))
            cols = _lane(z.under(chip(o)), z.cover)
            p = at_of(q, j) % 2
            at = _head(mc) if u is None else _lane(u * hc, hc)
            if q:
                @pl.loop(0, two)
                def _(i):
                    pt[p, :, at] += _nn(wc[i, :, cols], sb[o % 2, i, :, at])
            else:
                pt[p, :, at] += _nn(wc[:, cols], sb[o % 2, 0, :, at])

        def shares(q, j, wc, first, end):
            @pl.loop(first, end)
            def _(o):
                @pl.when(o + 1 < end)
                def _():
                    share_start(q, j, o + 1)
                share(q, j, o, wc)

        def front(q, j, wc):
            _clear(pt.at[at_of(q, j) % 2])
            shares(q, j, wc, OWN, FAR)

        def upright(q, j, u):
            p = s = at_of(q, j) % 2
            wide = 2 * LANES

            @pl.loop(0, dc // wide)
            def _(i):
                v = pt[p, _row(i * wide, wide), _lane(u * hc, hc)].T
                pv[s, pl.ds(u * hn, hn), :, :, _lane(i * wide, wide)] = v.reshape(hn, ny, ROWS, wide)

        def rs_send(s, u, dst=None):
            near_first = list(range(1, ny))
            far_first = sorted(near_first, key=lambda i: -min(i, ny - i))
            for i in near_first if dst is None else far_first:
                to = rsb.at[s, u, i - 1] if dst is None else dst.at[u, i - 1]
                rc(pv.at[s % 2, pl.ds(u * hn, hn), ty(i)], to, rss.at[s % 2], rsr.at[s, u], dev(c, ty(i), k)).start()

        def rs_free(s):
            left_for(pv.at[s % 2, :, pl.ds(0, ny - 1)], rss.at[s % 2])

        def send_up(q, j):
            if q:
                rs_free(at_of(q, j) - 2)
            else:
                @pl.when(j > 1)
                def _():
                    rs_free(j - 2)

            @pl.loop(0, two)
            def _(u):
                upright(q, j, u)
                rs_send(at_of(q, j), u)

        def out_rows(q, j):
            return (dx_ref if q else y_ref).at[_row(j * ROWS, ROWS), _lane(c * dc, dc)]

        def out_one(s, rows, dst, cc):
            @pl.when(cc != c)
            def _():
                rc(rows.at[cc], dst, a2s.at[0], a2r.at[0], dev(cc, t, k)).start()

            @pl.when(cc == c)
            def _():
                _start([pltpu.make_async_copy(rows.at[cc], dst, lsem.at[s])], True)

        def out_send(q, j):
            s = at_of(q, j)
            for cc in range(nc):
                out_one(s, ovh.at[s], out_rows(q, j), cc)

        def out_done(s):
            pltpu.make_async_copy(ovh.at[s, c], out_rows(H, 0), lsem.at[s]).wait()

        def stored(s):
            return pltpu.make_async_copy(ov.at[s % 2], ovh.at[s], osem.at[s % 2])

        def residual(q, j, u):
            rows = pl.ds(u * hn, hn)
            return pltpu.make_async_copy(xh.at[q, rows, t, _row(j * ROWS, ROWS), _lane(c * dc, dc)], tv.at[rows],
                                         fsem.at[1, u])

        def finish_loads(q, j, u):
            return [pltpu.make_async_copy(rsb.at[at_of(q, j), u], rv.at[u], fsem.at[0, u]), residual(q, j, u)]

        def finish_start(q, j):
            @pl.loop(0, two)
            def _(u):
                arrived(rsb.at[at_of(q, j), u], rsr, (at_of(q, j), u), mate)
                _start(finish_loads(q, j, u), True)

        def finish(q, j, late=None):
            s = at_of(q, j)

            @pl.loop(0, two)
            def _(u):
                if late is None:
                    _wait(finish_loads(q, j, u))
                else:
                    arrived(late.at[u], rsr, (s, u), mate)
                    residual(q, j, u).wait()
                for i in range(hn):
                    cc = u * hn + i
                    tot = pv[s % 2, cc, t]
                    for m in range(ny - 1):
                        tot = tot + (rv if late is None else late)[u, m, i]
                    ov[s % 2, cc] = (tv[cc].astype(F32) + tot).astype(BF16)
                    if late is not None:
                        out_one(s, ov.at[s % 2], out_rows(q, j), cc)

            if late is None:
                _start([stored(s)])

        def tok_load(a, j, buf, s):
            rows = _row(j * ROWS, ROWS)
            return [pltpu.make_async_copy(xh.at[a, :, :, rows, _lane(me * dp, dp)], buf.at[0], s.at[0]),
                    pltpu.make_async_copy(xp.at[a, :, :, rows, :], buf.at[1], s.at[1])]

        def phase2h(wc, hv, kv, psem, dsem, ksem):
            p_copy(DOWN).wait_recv()
            loads = wide_load(wc, wdt, wmt.at[DOWN], psem)
            _start(loads)
            g_pass(H, 0)
            g_send(H, 3)
            _clear(dwd)
            for w in PAIR:
                p_copy(w).wait_recv()
                e_copy(w).wait_recv()
            _wait(loads)

            def h_load(j, os, hs=PAIR):
                return [pltpu.make_async_copy(ha.at[j, kinds[i], cx(STEPS[o]), u],
                                              hv.at[_row(cx(STEPS[o]) * ft, ft), pl.ds(i * mc + u * hc, hc)],
                                              dsem.at[o // FAR])
                        for i in hs for o in os for u in PAIR]

            def add_outer(first, end):
                @pl.loop(first, end)
                def _(o):
                    rows = _row(chip(o) * ft, ft)
                    dwd[rows, :] += _nn(hv[rows, :], kv[...].reshape(2 * mc, dp))

            def all_read(j, first, n):
                v = ha.at[j, :, _head(n)]
                pltpu.make_async_copy(v, v, dsem.at[first // FAR]).wait()

            near = (OWN, RIGHT, LEFT)
            share_start(H, 0, OWN)

            @pl.loop(0, nj + 1)
            def _(j):
                here, before, two_before = j < nj, j > 0, j > 1

                @pl.when(before & here)
                def _():
                    g_pass(H, j)

                @pl.when(j == nj)
                def _():
                    g_pass(D, 0)
                    g_send(D, 2)

                @pl.when(j == 1)
                def _():
                    g_send(D, 0)

                @pl.when(j == last)
                def _():
                    g_send(D, 1)

                @pl.when(before)
                def _():
                    g_mate_near(H, j - 1)
                    _start(tok_load(DY, j - 1, kv, ksem))
                    _start(h_load(j - 1, near))

                @pl.when(here)
                def _():
                    front(H, j, wc)

                @pl.when(before)
                def _():
                    g_last(H, j - 1)
                    share_start(H, j - 1, FAR)
                    _start(h_load(j - 1, (FAR,), (0,)))

                @pl.when(j < last)
                def _():
                    share_start(H, j + 1, OWN)

                @pl.when(j == last)
                def _():
                    share_start(D, 0, OWN)

                @pl.when(before)
                def _():
                    _wait(tok_load(DY, j - 1, kv, ksem))
                    all_read(j - 1, OWN, FAR)
                    add_outer(OWN, FAR)
                    shares(H, j - 1, wc, FAR, FAR + 1)
                    g_mate_far(H, j - 1)
                    _start(h_load(j - 1, (FAR,), (1,)))
                    send_up(H, j - 1)

                @pl.when(two_before)
                def _():
                    finish_start(H, j - 2)

                @pl.when(before)
                def _():
                    all_read(j - 1, FAR, 1)
                    add_outer(FAR, FAR + 1)

                @pl.when(j > 3)
                def _():
                    stored(j - 4).wait()

                @pl.when(two_before)
                def _():
                    finish(H, j - 2)

        pl.run_scoped(
            phase2h,
            pltpu.VMEM((dc, fc), BF16),
            pltpu.VMEM((fc, 2 * mc), BF16),
            pltpu.VMEM((two, nc, ny, ROWS, dp), BF16),
            sem((two,)), sem((two,)), sem((two,)),
        )

        def phase2d(wc, dv, kv, kt, wsem, dsem, ksem):
            loads = [cp for w in PAIR for cp in wide_load(wc.at[w], (wg_ref, wu_ref)[w], wmt.at[w], wsem.at[w])]
            _start(loads)
            for w in PAIR:
                _clear(dw.at[w])
            _wait(loads)

            def d_load(j, os, hs=PAIR, us=PAIR):
                return [pltpu.make_async_copy(dda.at[j, kinds[i], cx(STEPS[o]), q, u],
                                              dv.at[q, _row(cx(STEPS[o]) * ft, ft), pl.ds(i * mc + u * hc, hc)],
                                              dsem.at[0])
                        for i in hs for o in os for q in PAIR for u in us]

            def all_read(j):
                pltpu.make_async_copy(dda.at[j], dda.at[j], dsem.at[0]).wait()

            def add_outer():
                n = fc // z.cuts

                @pl.loop(0, z.cuts * two)
                def _(i):
                    q, cols = i // z.cuts, _lane(i % z.cuts * n, n)
                    dw[q, :, cols] += _nt(kt[...], dv[q, cols, :])

            def far(j, us=(None,)):
                for u in us:
                    g_mate_far(D, j, u)
                _start(d_load(j, (FAR,), (1,)))
                _wait(tok_load(X, j, kv, ksem))

                @pl.loop(0, dp // LANES)
                def _(i):
                    v = kv[:, :, :, :, _lane(i * LANES, LANES)].reshape(2 * mc, LANES)
                    kt[_row(i * LANES, LANES), :] = _turned(v)

            def back(j):
                g_last(D, j)
                share_start(D, j, FAR)
                _start(d_load(j, (FAR,), (0,)))

            near = (OWN, RIGHT, LEFT)

            def near_start(j):
                g_mate_near(D, j)
                _start(tok_load(X, j, kv, ksem))
                _start(d_load(j, near))

            @pl.loop(0, last)
            def _(j):
                before, first = j > 0, j == 1

                @pl.when(first)
                def _():
                    sent_tokens()
                    sent_weights()

                @pl.when(before)
                def _():
                    g_pass(D, j)

                @pl.when(before & (j < last - 2))
                def _():
                    g_send(D, j + 2)

                @pl.when(j == last - 1)
                def _():
                    for u in PAIR:
                        g_send(D, last, u)
                    for i in range(nj):
                        g_sent(H, i)

                @pl.when(before)
                def _():
                    near_start(j - 1)

                front(D, j, wc)

                @pl.when(before)
                def _():
                    back(j - 1)

                share_start(D, j + 1, OWN)

                @pl.when(before)
                def _():
                    shares(D, j - 1, wc, FAR, FAR + 1)
                    send_up(D, j - 1)

                @pl.when(first)
                def _():
                    finish_start(H, last)

                @pl.when(j > 1)
                def _():
                    finish_start(D, j - 2)

                @pl.when(before)
                def _():
                    far(j - 1)
                    all_read(j - 1)
                    add_outer()

                @pl.when(before)
                def _():
                    stored(nj + j - 4).wait()

                @pl.when(first)
                def _():
                    finish(H, last)

                @pl.when(j > 1)
                def _():
                    finish(D, j - 2)

            m = last - 1
            near_start(m)
            back(m)
            _clear(pt.at[at_of(D, last) % 2])
            shares(D, m, wc, FAR, FAR + 1)
            send_up(D, m)
            far(m)
            shares(D, last, wc, OWN, RIGHT)
            g_pass(D, last, 0)
            all_read(m)
            add_outer()
            finish_start(D, m - 1)
            stored(nj + m - 3).wait()
            finish(D, m - 1)
            for i in range(m):
                g_sent(D, i)
            _start(tok_load(X, last, kv, ksem))
            g_pass(D, last, 1)
            share_start(D, last, RIGHT)
            share_start(D, last, LEFT)
            _start(d_load(last, near, (0,)))
            share(D, last, RIGHT, wc)
            share_blank(D, FAR % 2)
            rs_free(at_of(D, last) - 2)
            share(D, last, LEFT, wc)
            g_last(D, last, 0)
            _start(share_load(D, last, FAR, 0), True)

            @pl.loop(0, two)
            def _(u):
                @pl.when(u == 1)
                def _():
                    g_last(D, last, 1)
                    _start(share_load(D, last, FAR, 1), True)
                    for i in PAIR:
                        stored(nj + m - 2 + i).wait()

                    @pl.loop(0, nj)
                    def _(i):
                        out_send(H, i)

                    @pl.loop(0, m)
                    def _(i):
                        out_send(D, i)
                share(D, last, FAR, wc, u)
                upright(D, last, u)
                rs_send(at_of(D, last), u, rsv)

                @pl.when(u == 0)
                def _():
                    finish_start(D, m)
            for u in PAIR:
                g_mate_near(D, last, u)
            _start(d_load(last, near, (1,)))
            _start(d_load(last, (FAR,), (0,)))
            finish(D, m)
            far(last, PAIR)
            g_sent(D, m)
            for u in PAIR:
                g_sent(D, last, u)
            all_read(last)
            _start([residual(D, last, u) for u in PAIR], True)
            add_outer()
            stored(nj + m).wait()
            out_send(D, m)
            finish(D, last, rsv)
            for i in PAIR:
                rs_free(nj + last - i)

            v = ovh.at[:, _head(nc - 1)]
            left_for(v, a2s.at[0])

            @pl.loop(0, 2 * nj)
            def _(i):
                out_done(i)
            arrived(v, a2r, 0, mate)

        pl.run_scoped(
            phase2d,
            pltpu.VMEM((two, dc, fc), BF16),
            pltpu.VMEM((two, fc, 2 * mc), BF16),
            pltpu.VMEM((two, nc, ny, ROWS, dp), BF16),
            pltpu.VMEM((dp, 2 * mc), BF16),
            sem((two, two)), sem((1,)), sem((two,)),
        )

    pl.run_scoped(
        phase2,
        pltpu.VMEM((two, dc, mc), F32),
        pltpu.VMEM((two, nc, ny, ROWS, dc), F32),
        pltpu.VMEM((two, ny - 1, hn, ROWS, dc), F32),
        pltpu.VMEM((nc, ROWS, dc), BF16),
        pltpu.VMEM((two, nc, ROWS, dc), BF16),
        pltpu.VMEM((two, two, z.cover, mc), BF16),
        sem((two, two, two)), sem((two, two)), sem((2 * nj,)), sem((two,)),
    )


def _move(cuts, y, dx, dw, dwd, y_out, dx_out, dwg_out, dwu_out, dwd_out, bufs, sems):
    rows = [(y, bufs.at[0], y_out), (dx, bufs.at[1], dx_out)]
    grads = [(dwd, dwd_out)] + [(dw.at[q], o) for q, o in enumerate((dwg_out, dwu_out))]
    read = [pltpu.make_async_copy(a, b, sems.at[i]) for i, (a, b, _) in enumerate(rows)]
    write = [pltpu.make_async_copy(b, o, sems.at[i]) for i, (_, b, o) in enumerate(rows)]
    out = []
    for r in range(cuts):
        for a, o in grads:
            n = a.shape[0] // cuts
            out.append(pltpu.make_async_copy(a.at[_half(r, n)], o.at[_half(r, n)], sems.at[len(rows) + len(out)]))
    _start(read, True)
    for i in PAIR:
        _start(out[i::2], i == 1)
    for a, b in zip(read, write):
        a.wait()
        _start([b], True)
    _wait(write + out)


def _results(y, dx, dw, dwd, like, cuts):
    hbm, vmem = pltpu.HBM, pltpu.VMEM
    spaces = (hbm, hbm, vmem, vmem)
    like = jax.ShapeDtypeStruct(like.shape, F32)
    rows = [jax.ShapeDtypeStruct(a.shape, a.dtype) for a in (y, dx)]
    outs = rows + [like, like, jax.ShapeDtypeStruct(dwd.shape, F32)]
    return pl.pallas_call(
        functools.partial(_move, cuts),
        out_shape=outs,
        in_specs=[pl.BlockSpec(memory_space=m) for m in spaces],
        out_specs=[pl.BlockSpec(memory_space=hbm)] * len(outs),
        scratch_shapes=[vmem((len(rows), *y.shape), y.dtype), pltpu.SemaphoreType.DMA((len(rows) + 3 * cuts,))],
        name="results",
        compiler_params=pltpu.CompilerParams(vmem_limit_bytes=VMEM_LIMIT // 10),
    )(*(pltpu.with_memory_space_constraint(v, m) for v, m in zip((y, dx, dw, dwd), spaces)))


def solution(mesh):
    nx, ny = mesh.shape["dp"], mesh.shape["tp"]
    axes = mesh.axis_names
    row_spec = P(("part", "dp", "tp"), None)
    win_spec = P(("part", "dp"), "tp")
    wout_spec = P(("part", "tp"), "dp")

    def f(x, wg, wu, wd, dy):
        z = Sizes(axes, nx, ny, x, wg)
        steps, two, kinds = 2 * z.nj, len(PAIR), len(WEIGHTS)
        hbm = pl.BlockSpec(memory_space=pltpu.HBM)
        vmem = pl.BlockSpec(memory_space=pltpu.VMEM)
        bf16 = functools.partial(jax.ShapeDtypeStruct, dtype=BF16)
        f32 = functools.partial(jax.ShapeDtypeStruct, dtype=F32)
        outs = [
            bf16(x.shape), bf16(x.shape), pltpu.VMEM((two, z.dp, z.fc), F32), pltpu.VMEM(wd.shape, F32),
            bf16((two, z.nc, ny, z.td, z.d)),
            bf16((two, z.nc, ny, z.td, z.dp)),
            bf16((two, z.fc, z.dp)),
            bf16((z.dp, z.fc)),
            bf16((kinds, z.nc, two, z.ft, z.dp)),
            bf16((kinds, z.dp, z.fc)),
            bf16((z.nj, two, z.nc, two, z.ft, z.hc)),
            bf16((z.nj, two, z.nc, two, two, z.ft, z.hc)),
            f32((steps, two, ny - 1, z.nc // 2, ROWS, z.dc)),
            bf16((steps, z.nc, ROWS, z.dc)),
        ]
        specs = [hbm] * len(outs)
        specs[2:4] = [vmem] * 2
        sem = pltpu.SemaphoreType.DMA
        chips = len(CHIPS)
        shapes = ((two,), (two, 3), (two,), (two, chips, 3), (kinds,), (kinds, chips), (kinds,), (kinds, chips),
                  (two,), (two + kinds,), (steps + 1, two), (steps + 1, 5), (two,), (steps, two), (1,), (1,))
        r = pl.pallas_call(
            functools.partial(_kernel, z),
            out_shape=outs,
            in_specs=[hbm] * 5,
            out_specs=specs,
            scratch_shapes=[sem(shape) for shape in shapes]
            + [pltpu.VMEM((two, ny - 1, z.nc // 2, ROWS, z.dc), F32)],
            name="mlp",
            compiler_params=pltpu.CompilerParams(
                collective_id=0, has_side_effects=True, vmem_limit_bytes=VMEM_LIMIT),
        )(x, wg, wu, wd, dy)
        return tuple(_results(*r[:4], wg, 4))

    return jax.shard_map(f, mesh=mesh, in_specs=(row_spec, win_spec, win_spec, wout_spec, row_spec),
                         out_specs=(row_spec, row_spec, win_spec, win_spec, wout_spec), check_vma=False)
```
